128 devices in a mesh: gx: 8 (over z_lo, y), gy: 16 (over x, z_hi, core).
Axes of the slice: x: 4, y: 4, z: 4 (z_hi: 2, z_lo: 2; z = z_hi * 2 + z_lo), core: 2. Of those that a mesh axis runs over, the one named last changes fastest.
Arguments:
- cotangent: float32 [256, 1024, 128], P('gx', 'gy'), may hold values from -6 to 6
- speed: float32 [3, 256, 1024, 128], P(None, 'gx', 'gy'), may hold values from 0.05 to 0.45
- coeff: float32 [3, 256, 1024, 128], P(None, 'gx', 'gy'), may hold values from 0.3 to 3
- dirs: int32 [3, 256, 1024], P(None, 'gx', 'gy'), may hold values from 0 to 1
Outputs:
- grad: float32 [256, 1024, 128], P('gx', 'gy')
The draws below stay inside these ranges and needn't reach their ends.
Inputs may be any that keep to these rules, and one draw needn't show every extreme that they name: `dirs`: 0 means the lower cell of a face is upwind, 1 the upper cell.
All inputs are finite; a program needn't handle non-finite values.
Results may differ from the reference program's by a relative error of at most 0.0003.
Values sent between devices are 32-bit elements; how exact they have to be, the bound alone decides.
No kernel may reach another device: no remote copies, remote signals or barrier semaphores. Data moves between devices by JAX's collectives and lax.ppermute only.
A program may use at most 128 MiB of HBM per device.

```python
import math
import jax
import jax.numpy as jnp
from jax import lax

NZ = 128
ITERS = 2
NX = 256
NY = 1024


def plant(array, rng, smallest, top_value):
    index_at = [jax.random.randint(jax.random.fold_in(rng, axis), (), 0, length) for axis, length in enumerate(array.shape)]
    main_axis = array.shape.index(max(array.shape))
    next_to = index_at[:main_axis] + [(index_at[main_axis] + 1) % array.shape[main_axis]] + index_at[main_axis + 1:]
    return array.at[tuple(index_at)].set(smallest).at[tuple(next_to)].set(top_value)


def shard_levels(own_key, shape, pieces, smallest, top_value):
    gain = 1.0
    for dim, parts in pieces:
        steps = jax.random.uniform(jax.random.fold_in(jax.random.fold_in(own_key, 6), dim), (parts,), jnp.float32, smallest / len(pieces), top_value / len(pieces))
        gain = gain * jnp.repeat(jnp.exp(steps), shape[dim] // parts).reshape((-1,) + (1,) * (len(shape) - 1 - dim))
    return gain


def scatter_about(rng, dims, width, limit, shards=(), held_as=jnp.bfloat16):
    drawn = width * jax.random.normal(rng, dims, jnp.float32)
    if shards:
        drawn = drawn * shard_levels(rng, dims, shards, -0.22, 0.18)
    return jnp.clip(drawn, -limit, limit).astype(held_as)


def setup_inputs(seed: int = 0) -> dict:
    seeds = jax.random.split(jax.random.key(seed), 5)
    return {
        "cotangent": scatter_about(seeds[0], (NX, NY, NZ), 1.0, 6.0, ((0, 8), (1, 16)), jnp.float32),
        "speed": jnp.clip(jnp.exp(math.log(0.45) - 2.1972245 * jax.random.uniform(seeds[1], (3, NX, NY, NZ), jnp.float32) ** shard_levels(seeds[1], (3, NX, NY, NZ), ((1, 8), (2, 16)), -0.2, 0.2)), 0.05, 0.45),
        "coeff": jnp.clip(jnp.exp(math.log(3.0) - 2.3025851 * jax.random.uniform(seeds[2], (3, NX, NY, NZ), jnp.float32) ** shard_levels(seeds[2], (3, NX, NY, NZ), ((1, 8), (2, 16)), -0.2, 0.2)), 0.3, 3.0),
        "dirs": plant(jax.random.randint(seeds[3], (3, NX, NY), 0, 2), jax.random.fold_in(seeds[3], 1), 0, 1).astype(jnp.int32),
    }


explicit_table = ((0.0, 0.0, 0.0, 0.0), (0.5, 0.0, 0.0, 0.0), (0.25, 0.5, 0.0, 0.0), (0.2, 0.3, 0.5, 0.0))
implicit_table = ((0.0, 0.0, 0.0, 0.0), (0.25, 0.25, 0.0, 0.0), (0.25, 0.25, 0.25, 0.0), (0.15, 0.35, 0.25, 0.25))
section_weights = (0.15, 0.35, 0.25, 0.25)
implicit_diagonal = 0.25
step_length = 1.0


def local_ahead(values, dimension):
    tail = lax.slice_in_dim(values, 1, values.shape[dimension], axis=dimension)
    return jnp.concatenate([tail, jnp.zeros_like(lax.slice_in_dim(values, 0, 1, axis=dimension))], dimension)


def local_behind(values, dimension):
    head = lax.slice_in_dim(values, 0, values.shape[dimension] - 1, axis=dimension)
    return jnp.concatenate([jnp.zeros_like(lax.slice_in_dim(values, 0, 1, axis=dimension)), head], dimension)


def transposed(advected, diffused, velocity, coeff):
    total = jnp.zeros_like(diffused)
    for dimension in range(3):
        flux = coeff[dimension] * (local_ahead(diffused, dimension) - diffused)
        total = total + flux - local_behind(flux, dimension)
        if advected is not None:
            moved = velocity[dimension] * (local_ahead(advected, dimension) - advected)
            upwind_here = velocity[dimension] > 0
            total = total + jnp.where(upwind_here, moved, 0.0)
            total = total + local_behind(jnp.where(upwind_here, 0.0, moved), dimension)
    return total


def solve_section(rhs, velocity, coeff):
    solution = jnp.zeros_like(rhs)
    residual = rhs
    direction = rhs
    norm_now = jnp.sum(residual * residual)
    for iteration in range(ITERS):
        image = direction - implicit_diagonal * step_length * transposed(None, direction, velocity, coeff)
        alpha = norm_now / jnp.sum(direction * image)
        solution = solution + alpha * direction
        residual = residual - alpha * image
        norm_next = jnp.sum(residual * residual)
        direction = residual + (norm_next / norm_now) * direction
        norm_now = norm_next
    return solution


def reference(cotangent, speed, coeff, dirs):
    signs = (1 - 2 * dirs).astype(jnp.float32)
    velocity = speed * signs[..., None]
    section_adjoints = [None, None, None, None]
    for section_index in (3, 2, 1, 0):
        advected = step_length * section_weights[section_index] * cotangent
        diffused = step_length * section_weights[section_index] * cotangent
        for later in range(section_index + 1, 4):
            advected = advected + step_length * explicit_table[later][section_index] * section_adjoints[later]
            diffused = diffused + step_length * implicit_table[later][section_index] * section_adjoints[later]
        source = transposed(advected, diffused, velocity, coeff)
        if section_index > 0:
            section_adjoints[section_index] = solve_section(source, velocity, coeff)
        else:
            section_adjoints[section_index] = source
    return cotangent + section_adjoints[0] + section_adjoints[1] + section_adjoints[2] + section_adjoints[3]
```

```python
import jax
import jax.numpy as jnp
from jax import lax
from jax.experimental import pallas as pl
from jax.experimental.pallas import tpu as pltpu
from jax.sharding import PartitionSpec as P


NX, NY, NZ = 32, 64, 128
H = 7
T = 8
EX, EY = NX + 2 * H, NY + 2 * T
TILES = EY // T
F32 = jnp.float32

LOW = ((0, 7), (1, 7), (4, 7), (2, 6), (3, 6), (5, 6), (6, 6))
HIGH = ((0, 7), (1, 6), (4, 6), (2, 6), (3, 6), (5, 6), (6, 6))
NLOW = sum(n for _, n in LOW)
NHIGH = sum(n for _, n in HIGH)


def lane_row():
    return (
        lax.broadcasted_iota(jnp.int32, (T, NZ), 1),
        lax.broadcasted_iota(jnp.int32, (T, NZ), 0),
    )


def tile(ref, x, t):
    return ref[x, t * T : (t + 1) * T, :]


def loops(x0, x1, body, carry):
    for part, lo, hi in ((0, x0, min(H, x1)), (1, max(x0, H), min(x1, H + NX)), (2, H + NX, x1)):
        if hi > lo:
            carry = lax.fori_loop(lo, hi, lambda x, c, part=part: body(x, c, part), carry)
    return carry


class Shifts:
    def __init__(self):
        lane, self.row = lane_row()
        self.first, self.last = (lane == 0, lane == NZ - 1)
        self.top = self.row == 0

    def z_ahead(self, v):
        return jnp.where(self.last, 0.0, pltpu.roll(v, NZ - 1, 1))

    def z_behind(self, flux):
        return jnp.where(self.first, 0.0, pltpu.roll(flux, 1, 1))

    def y_behind(self, flux, rolled_before):
        rolled = pltpu.roll(flux, 1, 0)
        return jnp.where(self.top, rolled_before, rolled), rolled


def y_ahead(ref, x, t, v):
    if t + 1 < TILES:
        return ref[x, t * T + 1 : (t + 1) * T + 1, :]
    return pltpu.roll(v, T - 1, 0)


def diffusion_flux(kref, ahead, v):
    return kref * (ahead - v)


def masked(value, t, part, mx, my):
    if part == 2:
        value = value * mx
    if t == TILES - 1:
        value = value * my
    return value


def m_pass(e, v_ref, out_ref, x0, x1, tiles, mx, my, sh, energy=False):
    def plane_flux(x):
        return [e[1, x, t * T : (t + 1) * T, :] * (tile(v_ref, x + 1, t) - tile(v_ref, x, t)) for t in tiles]

    zero = jnp.zeros((T, NZ), F32)
    accs = (zero,) * (1 if energy else 3)

    def body(x, carry, part):
        flux_x, accs = carry
        accs = list(accs)
        new_flux = []
        before = zero
        if tiles[0] > 0:
            t = tiles[0] - 1
            v = tile(v_ref, x, t)
            before = pltpu.roll(e[2, x, t * T : (t + 1) * T, :] * (y_ahead(v_ref, x, t, v) - v), 1, 0)
        for i, t in enumerate(tiles):
            rows = slice(t * T, (t + 1) * T)
            v = tile(v_ref, x, t)
            fx = e[1, x, rows, :] * (tile(v_ref, x + 1, t) - v)
            fy = e[2, x, rows, :] * (y_ahead(v_ref, x, t, v) - v)
            fz = e[3, x, rows, :] * (sh.z_ahead(v) - v)
            fy_low, before = sh.y_behind(fy, before)
            total = (fx - flux_x[i]) + (fy - fy_low) + (fz - sh.z_behind(fz))
            w = v - 0.25 * total
            new_flux.append(fx)
            if energy:
                accs[0] = accs[0] + v * w
            else:
                out_ref[x, rows, :] = masked(w, t, part, mx, my)
                if part == 1 and 0 < t < TILES - 1:
                    accs[0] = accs[0] + v * v
                    accs[1] = accs[1] + v * w
                    accs[2] = accs[2] + w * w
        return new_flux, tuple(accs)

    return loops(x0, x1, body, (plane_flux(x0 - 1), accs))[1]


def s_pass(e, out_ref, weight, x0, x1, mx, my, sh):
    tiles = range(TILES)

    def parts(k, u, delta):
        return (k + jnp.maximum(u, 0.0)) * delta, (k - jnp.minimum(u, 0.0)) * delta

    def get(f, x, t):
        return e[f, x, t * T : (t + 1) * T, :]

    low = [parts(get(1, x0 - 1, t), get(4, x0 - 1, t), get(0, x0, t) - get(0, x0 - 1, t))[1] for t in tiles]
    zero = jnp.zeros((T, NZ), F32)

    def body(x, flux_x, part):
        new_flux = []
        before = zero
        for t in tiles:
            v = get(0, x, t)
            if t + 1 < TILES:
                vy = e[0, x, t * T + 1 : (t + 1) * T + 1, :]
            else:
                vy = pltpu.roll(v, T - 1, 0)
            up_x, low_x = parts(get(1, x, t), get(4, x, t), get(0, x + 1, t) - v)
            up_y, low_y = parts(get(2, x, t), get(5, x, t), vy - v)
            up_z, low_z = parts(get(3, x, t), get(6, x, t), sh.z_ahead(v) - v)
            low_y, before = sh.y_behind(low_y, before)
            total = (up_x - flux_x[t]) + (up_y - low_y) + (up_z - sh.z_behind(low_z))
            new_flux.append(low_x)
            out_ref[x, t * T : (t + 1) * T, :] = masked(weight * total, t, part, mx, my)
        return new_flux

    loops(x0, x1, body, low)


def fd_pass(e, a_ref, d_ref, emit, x0, x1, tiles, mx, my, sh):
    def parts(k, u, da, dd):
        flux = k * dd
        return flux + jnp.maximum(u, 0.0) * da, flux - jnp.minimum(u, 0.0) * da

    def get(f, x, t):
        return e[f, x, t * T : (t + 1) * T, :]

    def y_parts(x, t, a, d):
        return parts(get(2, x, t), get(5, x, t), y_ahead(a_ref, x, t, a) - a, y_ahead(d_ref, x, t, d) - d)

    def x_parts(x, t, a, d):
        return parts(get(1, x, t), get(4, x, t), tile(a_ref, x + 1, t) - a, tile(d_ref, x + 1, t) - d)

    low = [x_parts(x0 - 1, t, tile(a_ref, x0 - 1, t), tile(d_ref, x0 - 1, t))[1] for t in tiles]
    zero = jnp.zeros((T, NZ), F32)

    def body(x, flux_x, part):
        new_flux = []
        before = zero
        if tiles[0] > 0:
            t = tiles[0] - 1
            before = pltpu.roll(y_parts(x, t, tile(a_ref, x, t), tile(d_ref, x, t))[1], 1, 0)
        for i, t in enumerate(tiles):
            a, d = tile(a_ref, x, t), tile(d_ref, x, t)
            up_x, low_x = x_parts(x, t, a, d)
            up_y, low_y = y_parts(x, t, a, d)
            up_z, low_z = parts(get(3, x, t), get(6, x, t), sh.z_ahead(a) - a, sh.z_ahead(d) - d)
            low_y, before = sh.y_behind(low_y, before)
            total = (up_x - flux_x[i]) + (up_y - low_y) + (up_z - sh.z_behind(low_z))
            new_flux.append(low_x)
            emit(x, t, masked(total, t, part, mx, my))
        return new_flux

    loops(x0, x1, body, low)


def write_moments(out_ref, accs):
    lane = lax.broadcasted_iota(jnp.int32, (1, NZ), 1)
    row = jnp.zeros((1, NZ), F32)
    for i, acc in enumerate(accs):
        total = jnp.sum(jnp.sum(acc, axis=0, keepdims=True), axis=1, keepdims=True)
        row = jnp.where(lane // 32 == i, total, row)
    out_ref[...] = jnp.broadcast_to(row, out_ref.shape)


def coefficients(moments_ref):
    sums = jnp.sum(moments_ref[...], axis=0, keepdims=True)
    lane = lax.broadcasted_iota(jnp.int32, (1, NZ), 1)
    m0, m1, m2, m3 = (
        jnp.sum(jnp.where(lane == 32 * i, sums, 0.0), axis=1, keepdims=True) for i in range(4)
    )
    alpha0 = m0 / m1
    rr = alpha0 * alpha0 * m2 - m0
    product = m1 - 2.0 * alpha0 * m2 + alpha0 * alpha0 * m3
    ratio = rr / m0
    alpha1 = rr / (product - ratio * rr / alpha0)
    a = alpha0 + alpha1 * (1.0 + ratio)
    b = -(alpha1 * alpha0)
    return jnp.broadcast_to(a, (T, NZ)), jnp.broadcast_to(b, (T, NZ))


def pack_kernel(cot, coeff, vel, low, high, ylow, yhigh, cll, clh, chl, chh):
    def get(f, planes, rows):
        if f == 0:
            return cot[planes, rows, :]
        return (coeff if f < 4 else vel)[(f - 1) % 3, planes, rows, :]

    bottom, top, full = slice(0, T), slice(NY - T, NY), slice(0, NY)
    at = 0
    for f, n in LOW:
        planes = slice(NX - n, NX)
        low[at : at + n] = get(f, planes, full)
        cll[at : at + n] = get(f, planes, top)
        clh[at : at + n] = get(f, planes, bottom)
        at += n
    at = 0
    for f, n in HIGH:
        planes = slice(0, n)
        high[at : at + n] = get(f, planes, full)
        chl[at : at + n] = get(f, planes, top)
        chh[at : at + n] = get(f, planes, bottom)
        at += n
    for f in range(7):
        ylow[f * NX : (f + 1) * NX] = get(f, slice(0, NX), top)
        yhigh[f * NX : (f + 1) * NX] = get(f, slice(0, NX), bottom)


def center_kernel(cot, coeff, vel, e):
    def body(x, _):
        e[0, H + x, T : T + NY, :] = cot[x]
        for d in range(3):
            e[1 + d, H + x, T : T + NY, :] = coeff[d, x]
            e[4 + d, H + x, T : T + NY, :] = vel[d, x]
        return _

    lax.fori_loop(0, NX, body, 0)


def first_kernel(mask, e_in, low, high, ylow, yhigh, cll, clh, chl, chh, e, y, w, moments):
    mx, my = mask[0], mask[1]
    sh = Shifts()
    at = 0
    for f, n in LOW:
        planes = slice(H - n, H)
        e[f, planes, T : T + NY, :] = low[at : at + n]
        e[f, planes, 0:T, :] = cll[at : at + n]
        e[f, planes, T + NY :, :] = clh[at : at + n]
        at += n
    at = 0
    for f, n in HIGH:
        planes = slice(H + NX, H + NX + n)
        e[f, planes, T : T + NY, :] = high[at : at + n]
        e[f, planes, 0:T, :] = chl[at : at + n]
        e[f, planes, T + NY :, :] = chh[at : at + n]
        at += n
    for f in range(7):
        e[f, H : H + NX, 0:T, :] = ylow[f * NX : (f + 1) * NX]
        e[f, H : H + NX, T + NY :, :] = yhigh[f * NX : (f + 1) * NX]
    s_pass(e, y, 0.25, 1, EX - 1, mx, my, sh)
    finish(e, y, w, moments, 5, mx, my, sh)


def finish(e, y, w, moments, depth, mx, my, sh):
    dots = m_pass(e, y, w, H - depth, H + NX + depth, range(TILES), mx, my, sh)
    energy = m_pass(e, w, None, H, H + NX, range(1, TILES - 1), mx, my, sh, energy=True)
    write_moments(moments, dots + energy)


def combine(x0, x1, emit):
    def body(x, _):
        for t in range(TILES):
            emit(x, t)
        return _

    lax.fori_loop(x0, x1, body, 0)


def put(ref):
    def emit(x, t, value):
        ref[x, t * T : (t + 1) * T, :] = value

    return emit


def third_kernel(mask, e, y4, w4, sums, nu4, y, w, moments, adv, dif):
    mx, my = mask[0], mask[1]
    sh = Shifts()
    a, b = coefficients(sums)

    def emit(x, t):
        nu = a * tile(y4, x, t) + b * tile(w4, x, t)
        c = 0.25 * e[0, x, t * T : (t + 1) * T, :]
        put(nu4)(x, t, nu)
        put(adv)(x, t, c + 0.5 * nu)
        put(dif)(x, t, c + 0.25 * nu)

    combine(H - 5, H + NX + 5, emit)
    fd_pass(e, adv, dif, put(y), H - 4, H + NX + 4, range(TILES), mx, my, sh)
    finish(e, y, w, moments, 3, mx, my, sh)


def second_kernel(mask, e, nu4, y3, w3, sums, nu3, y, w, moments, adv, dif):
    mx, my = mask[0], mask[1]
    sh = Shifts()
    a, b = coefficients(sums)

    def emit(x, t):
        nu = a * tile(y3, x, t) + b * tile(w3, x, t)
        c = 0.35 * e[0, x, t * T : (t + 1) * T, :]
        four = tile(nu4, x, t)
        put(nu3)(x, t, nu)
        put(adv)(x, t, c + 0.3 * four + 0.5 * nu)
        put(dif)(x, t, c + 0.35 * four + 0.25 * nu)

    combine(H - 3, H + NX + 3, emit)
    fd_pass(e, adv, dif, put(y), H - 2, H + NX + 2, range(TILES), mx, my, sh)
    finish(e, y, w, moments, 1, mx, my, sh)


def last_kernel(mask, e, nu4, nu3, y2, w2, sums, out, adv, dif, base):
    mx, my = mask[0], mask[1]
    sh = Shifts()
    a, b = coefficients(sums)

    def emit(x, t):
        nu = a * tile(y2, x, t) + b * tile(w2, x, t)
        cot = e[0, x, t * T : (t + 1) * T, :]
        c = 0.15 * cot
        four, three = tile(nu4, x, t), tile(nu3, x, t)
        put(adv)(x, t, c + 0.2 * four + 0.25 * three + 0.5 * nu)
        put(dif)(x, t, c + 0.15 * four + 0.25 * three + 0.25 * nu)
        put(base)(x, t, cot + four + three + nu)

    def result(x, t, value):
        out[x - H, (t - 1) * T : t * T, :] = tile(base, x, t) + value

    combine(H - 1, H + NX + 1, emit)
    fd_pass(e, adv, dif, result, H, H + NX, range(1, TILES - 1), mx, my, sh)


def shape(*dims):
    return jax.ShapeDtypeStruct(dims, F32)


FIELD = shape(EX, EY, NZ)
EXT = shape(7, EX, EY, NZ)
ROWS = shape(128, NZ)
VMEM = pl.BlockSpec(memory_space=pltpu.VMEM)
SMEM = pl.BlockSpec(memory_space=pltpu.SMEM)
LIMIT = 24 * 1024 * 1024


def call(kernel, outs, ins, scratch=(), aliases=None, smem=True, name=None, limit=LIMIT):
    return pl.pallas_call(
        kernel,
        out_shape=outs,
        in_specs=[SMEM if smem and i == 0 else VMEM for i in range(len(ins))],
        out_specs=jax.tree.map(lambda _: VMEM, outs),
        scratch_shapes=[pltpu.VMEM(s.shape, F32) for s in scratch],
        input_output_aliases=aliases or {},
        compiler_params=pltpu.CompilerParams(vmem_limit_bytes=limit),
        name=name,
    )(*ins)


def local(cotangent, speed, coeff, dirs):
    nx, ny = lax.axis_size("gx"), lax.axis_size("gy")
    ix, iy = lax.axis_index("gx"), lax.axis_index("gy")
    mask = jnp.stack([(ix < nx - 1).astype(F32), (iy < ny - 1).astype(F32)])
    velocity = speed * (1 - 2 * dirs).astype(F32)[..., None]

    strips = call(
        pack_kernel,
        [shape(NLOW, NY, NZ), shape(NHIGH, NY, NZ), shape(7 * NX, T, NZ), shape(7 * NX, T, NZ)]
        + [shape(NLOW, T, NZ)] * 2 + [shape(NHIGH, T, NZ)] * 2,
        [cotangent, coeff, velocity],
        smem=False,
        name="pack",
    )

    def shifted(value, dx, dy):
        perm = []
        for i in range(nx):
            for j in range(ny):
                if 0 <= i + dx < nx and 0 <= j + dy < ny:
                    perm.append((i * ny + j, (i + dx) * ny + j + dy))
        return lax.ppermute(value, ("gx", "gy"), perm)

    moves = ((1, 0), (-1, 0), (0, 1), (0, -1), (1, 1), (1, -1), (-1, 1), (-1, -1))
    received = [shifted(s, dx, dy) for s, (dx, dy) in zip(strips, moves)]
    e = call(center_kernel, EXT, [cotangent, coeff, velocity], smem=False, name="center")

    def reduced(moments):
        return lax.all_to_all(moments, ("gx", "gy"), 0, 0, tiled=True)

    e, y4, w4, moments = call(
        first_kernel, [EXT, FIELD, FIELD, ROWS], [mask, e, *received], aliases={1: 0}, name="first"
    )
    nu4, y3, w3, moments = call(
        third_kernel, [FIELD, FIELD, FIELD, ROWS], [mask, e, y4, w4, reduced(moments)], [FIELD] * 2, name="third"
    )
    nu3, y2, w2, moments = call(
        second_kernel, [FIELD, FIELD, FIELD, ROWS], [mask, e, nu4, y3, w3, reduced(moments)], [FIELD] * 2, name="second"
    )
    return call(
        last_kernel, shape(NX, NY, NZ), [mask, e, nu4, nu3, y2, w2, reduced(moments)], [FIELD] * 3, name="last"
    )


def solution(mesh):
    placed = (P("gx", "gy", None), P(None, "gx", "gy", None), P(None, "gx", "gy", None), P(None, "gx", "gy"))
    return jax.shard_map(local, mesh=mesh, in_specs=placed, out_specs=P("gx", "gy", None), check_vma=False)
```

```python
import jax
import jax.numpy as jnp
from jax import lax
from jax.experimental import pallas as pl
from jax.experimental.pallas import tpu as pltpu
from jax.sharding import PartitionSpec as P


NX, NY, NZ = 32, 64, 128
H = 3
T = 8
EX, EY = NX + 2 * H, NY + 2 * T
TILES = EY // T
INNER = range(1, TILES - 1)
F32 = jnp.float32

C, K, U, K2B, U2B = 0, 1, 4, 7, 8
LOW = ((0, 3), (1, 3), (4, 3), (2, 2), (3, 2), (5, 2), (6, 2))
HIGH = ((0, 3), (1, 2), (4, 2), (2, 2), (3, 2), (5, 2), (6, 2))
NLOW = sum(n for _, n in LOW)
NHIGH = sum(n for _, n in HIGH)
STEP = 4


def rows(t):
    return slice(t * T, (t + 1) * T)


class Masks:
    def __init__(self):
        lane = lax.broadcasted_iota(jnp.int32, (T, NZ), 1)
        row = lax.broadcasted_iota(jnp.int32, (T, NZ), 0)
        self.first, self.last, self.top = lane == 0, lane == NZ - 1, row == 0


def back(v):
    return pltpu.roll(v, 1, 1)


class Tiles:
    def __init__(self, ref, masks):
        self.ref, self.masks, self.seen = ref, masks, {}

    def at(self, x, i, t):
        key = (i, t)
        if key not in self.seen:
            self.seen[key] = self.ref[x + i, rows(t), :]
        return self.seen[key]

    def dx(self, x, i, t):
        return self.at(x, i + 1, t) - self.at(x, i, t)

    def dy(self, x, i, t):
        v = self.at(x, i, t)
        if t + 1 < TILES:
            return self.ref[x + i, t * T + 1 : (t + 1) * T + 1, :] - v
        return pltpu.roll(v, T - 1, 0) - v

    def dz(self, x, i, t):
        v = self.at(x, i, t)
        return jnp.where(self.masks.last, 0.0, pltpu.roll(v, NZ - 1, 1)) - v

    def dz_below(self, x, i, t):
        v = self.at(x, i, t)
        return v - back(v)


def sweep(x0, x1, step, body, carry):
    count = -(-(x1 - x0) // step)
    return lax.fori_loop(0, count, lambda n, c: body(x0 + n * step, c), carry)


def fluxes(x0, tiles, masks, parts, emit):
    def plane(x, low_x, i, fetch):
        new_low = []
        before = jnp.zeros((T, NZ), F32)
        if tiles[0] > 0:
            before = pltpu.roll(parts(fetch, 1, x, i, tiles[0] - 1)[1], 1, 0)
        for n, t in enumerate(tiles):
            up_x, down_x = parts(fetch, 0, x, i, t)
            up_y, down_y = parts(fetch, 1, x, i, t)
            up_z, down_z = parts(fetch, 2, x, i, t)
            rolled = pltpu.roll(down_y, 1, 0)
            down_y = jnp.where(masks.top, before, rolled)
            before = rolled
            total = (up_x - low_x[n]) + (up_y - down_y) + (up_z - down_z)
            new_low.append(down_x)
            emit(fetch, x, i, t, total)
        return new_low

    return plane


def run(x0, x1, step, tiles, masks, fetch_of, parts, emit):
    plane = fluxes(x0, tiles, masks, parts, emit)
    fetch = fetch_of()
    low = [parts(fetch, 0, x0 - 1, 0, t)[1] for t in tiles]

    def body(x, low):
        fetch = fetch_of()
        for i in range(step):
            low = plane(x, low, i, fetch)
        return low

    sweep(x0, x1, step, body, low)


def m_pass(e, v_ref, w_ref, masks):
    def parts(v, d, x, i, t):
        if d == 2:
            return e[K + 2, x + i, rows(t), :] * v.dz(x, i, t), e[K2B, x + i, rows(t), :] * v.dz_below(x, i, t)
        flux = e[K + d, x + i, rows(t), :] * (v.dx, v.dy)[d](x, i, t)
        return flux, flux

    def emit(v, x, i, t, total):
        w_ref[x + i, rows(t), :] = v.at(x, i, t) - total

    run(1, EX - 1, STEP, range(TILES), masks, lambda: Tiles(v_ref, masks), parts, emit)


def s_pass(e, y_ref, masks):
    cot = e.at[C]

    def parts(v, d, x, i, t):
        k, u = e[K + d, x + i, rows(t), :], e[U + d, x + i, rows(t), :]
        delta = (v.dx, v.dy, v.dz)[d](x, i, t)
        up = (k + jnp.maximum(u, 0.0)) * delta
        if d == 2:
            k, u = e[K2B, x + i, rows(t), :], e[U2B, x + i, rows(t), :]
            delta = v.dz_below(x, i, t)
        return up, (k - jnp.minimum(u, 0.0)) * delta

    def emit(v, x, i, t, total):
        y_ref[x + i, rows(t), :] = total

    run(1, EX - 1, STEP, range(TILES), masks, lambda: Tiles(cot, masks), parts, emit)


def fd_pass(e, a_ref, d_ref, put, x0, x1, tiles, masks):
    def parts(both, d, x, i, t):
        a, b = both
        k, u = e[K + d, x + i, rows(t), :], e[U + d, x + i, rows(t), :]
        da, db = ((v.dx, v.dy, v.dz)[d](x, i, t) for v in (a, b))
        flux = k * db
        up = flux + jnp.maximum(u, 0.0) * da
        if d == 2:
            u = e[U2B, x + i, rows(t), :]
            flux = e[K2B, x + i, rows(t), :] * b.dz_below(x, i, t)
            da = a.dz_below(x, i, t)
        return up, flux - jnp.minimum(u, 0.0) * da

    def emit(both, x, i, t, total):
        put(x + i, t, total)

    run(x0, x1, STEP, tiles, masks, lambda: (Tiles(a_ref, masks), Tiles(d_ref, masks)), parts, emit)


def products(e, y_ref, w_ref, masks):
    zero = jnp.zeros((T, NZ), F32)

    def body(x, accs):
        yy, yw, ww, energy = accs
        w = Tiles(w_ref, masks)
        for i in range(STEP):
            for t in INNER:
                v, y = w.at(x, i, t), y_ref[x + i, rows(t), :]
                yy, yw, ww = yy + y * y, yw + y * v, ww + v * v
                for d, delta in enumerate((w.dx, w.dy, w.dz)):
                    difference = delta(x, i, t)
                    energy = energy + e[K + d, x + i, rows(t), :] * (difference * difference)
        return yy, yw, ww, energy

    return sweep(H, H + NX, STEP, body, (zero,) * 4)


def outside_is_zero(edge, ref):
    @pl.when(edge[0] == 0)
    def _():
        ref[H + NX : EX - 1] = jnp.zeros((H - 1, EY, NZ), F32)

    @pl.when(edge[1] == 0)
    def _():
        ref[:, EY - T :, :] = jnp.zeros((EX, T, NZ), F32)


def finish(edge, e, y, w, up, down, moments, masks):
    outside_is_zero(edge, y)
    m_pass(e, y, w, masks)
    outside_is_zero(edge, w)
    if up is not None:
        for n, ref in enumerate((y, w)):
            up[n * H : (n + 1) * H] = ref[NX : NX + H]
            down[n * H : (n + 1) * H] = ref[H : 2 * H]
    yy, yw, ww, energy = products(e, y, w, masks)
    lane = lax.broadcasted_iota(jnp.int32, (1, NZ), 1)
    row = jnp.zeros((1, NZ), F32)
    for i, acc in enumerate((yy, yw, ww, ww + energy)):
        total = jnp.sum(jnp.sum(acc, axis=0, keepdims=True), axis=1, keepdims=True)
        row = jnp.where(lane // 32 == i, total, row)
    moments[...] = jnp.broadcast_to(row, moments.shape)


def coefficients(moments_ref):
    sums = jnp.sum(moments_ref[...], axis=0, keepdims=True)
    lane = lax.broadcasted_iota(jnp.int32, (1, NZ), 1)
    m0, m1, m2, m3 = (jnp.sum(jnp.where(lane == 32 * i, sums, 0.0), axis=1, keepdims=True) for i in range(4))
    alpha0 = m0 / m1
    rr = alpha0 * alpha0 * m2 - m0
    product = m1 - 2.0 * alpha0 * m2 + alpha0 * alpha0 * m3
    ratio = rr / m0
    alpha1 = rr / (product - ratio * rr / alpha0)
    a = alpha0 + alpha1 * (1.0 + ratio)
    b = -(alpha1 * alpha0)
    return jnp.broadcast_to(a, (T, NZ)), jnp.broadcast_to(b, (T, NZ))


def pack_kernel(cot, coeff, vel, low, high, ylow, yhigh, cll, clh, chl, chh):
    def get(f, planes, rows):
        if f == 0:
            return cot[planes, rows, :]
        return (coeff if f < 4 else vel)[(f - 1) % 3, planes, rows, :]

    bottom, top, full = slice(0, T), slice(NY - T, NY), slice(0, NY)
    at = 0
    for f, n in LOW:
        planes = slice(NX - n, NX)
        low[at : at + n] = get(f, planes, full)
        cll[at : at + n] = get(f, planes, top)
        clh[at : at + n] = get(f, planes, bottom)
        at += n
    at = 0
    for f, n in HIGH:
        planes = slice(0, n)
        high[at : at + n] = get(f, planes, full)
        chl[at : at + n] = get(f, planes, top)
        chh[at : at + n] = get(f, planes, bottom)
        at += n
    for f in range(7):
        ylow[f * NX : (f + 1) * NX] = get(f, slice(0, NX), top)
        yhigh[f * NX : (f + 1) * NX] = get(f, slice(0, NX), bottom)


def place(e, f, x, rows, value, masks):
    if f > 0:
        value = 0.25 * value
    e[f, x, rows, :] = value
    if f in (K + 2, U + 2):
        n = value.shape[0]
        first = lax.broadcasted_iota(jnp.int32, (n, NZ), 1) == 0
        e[K2B if f == K + 2 else U2B, x, rows, :] = jnp.where(first, 0.0, back(value))


def first_kernel(edge, cot, coeff, vel, low, high, ylow, yhigh, cll, clh, chl, chh, e, y, w, up, down, moments):
    masks = Masks()
    middle, below, above = slice(T, T + NY), slice(0, T), slice(T + NY, EY)
    for fields, base, middles, lows, highs in (
        (LOW, None, low, cll, clh),
        (HIGH, H + NX, high, chl, chh),
    ):
        at = 0
        for f, n in fields:
            for i in range(n):
                x = (H - n if base is None else base) + i
                place(e, f, x, middle, middles[at + i], masks)
                place(e, f, x, below, lows[at + i], masks)
                place(e, f, x, above, highs[at + i], masks)
            at += n

    def body(x, _):
        for f in range(7):
            value = cot[x] if f == 0 else (coeff if f < 4 else vel)[(f - 1) % 3, x]
            place(e, f, H + x, middle, value, masks)
            place(e, f, H + x, below, ylow[f * NX + x], masks)
            place(e, f, H + x, above, yhigh[f * NX + x], masks)
        return _

    lax.fori_loop(0, NX, body, 0)
    s_pass(e, y, masks)
    finish(edge, e, y, w, up, down, moments, masks)


def combine(x0, x1, emit):
    def body(x, _):
        for t in range(TILES):
            emit(x, t)
        return _

    lax.fori_loop(x0, x1, body, 0)


def nu_of(a, b, y, w, low, high, emit):
    combine(H, H + NX, lambda x, t: emit(x, t, a * y[x, rows(t), :] + b * w[x, rows(t), :]))
    for base, strip in ((0, low), (H + NX, high)):
        for i in range(H):
            for t in range(TILES):
                emit(base + i, t, a * strip[i, rows(t), :] + b * strip[H + i, rows(t), :])


def third_kernel(edge, e, y4, w4, low, high, sums, nu4, y, w, up, down, moments, adv, dif):
    masks = Masks()
    a, b = coefficients(sums)

    def emit(x, t, nu):
        c = e[C, x, rows(t), :]
        nu4[x, rows(t), :] = nu
        adv[x, rows(t), :] = c + 2.0 * nu
        dif[x, rows(t), :] = c + nu

    nu_of(a, b, y4, w4, low, high, emit)

    def put(x, t, value):
        y[x, rows(t), :] = value

    fd_pass(e, adv, dif, put, 1, EX - 1, range(TILES), masks)
    finish(edge, e, y, w, up, down, moments, masks)


def second_kernel(edge, e, nu4, y3, w3, low, high, sums, nu3, y, w, moments, adv, dif):
    masks = Masks()
    a, b = coefficients(sums)

    def emit(x, t, nu):
        c = 1.4 * e[C, x, rows(t), :]
        four = nu4[x, rows(t), :]
        nu3[x, rows(t), :] = nu
        adv[x, rows(t), :] = c + 1.2 * four + 2.0 * nu
        dif[x, rows(t), :] = c + 1.4 * four + nu

    nu_of(a, b, y3, w3, low, high, emit)

    def put(x, t, value):
        y[x, rows(t), :] = value

    fd_pass(e, adv, dif, put, 1, EX - 1, range(TILES), masks)
    finish(edge, e, y, w, None, None, moments, masks)


def last_kernel(e, nu4, nu3, y2, w2, sums, out, adv, dif, base):
    masks = Masks()
    a, b = coefficients(sums)

    def emit(x, t):
        nu = a * y2[x, rows(t), :] + b * w2[x, rows(t), :]
        cot = e[C, x, rows(t), :]
        four, three = nu4[x, rows(t), :], nu3[x, rows(t), :]
        adv[x, rows(t), :] = 0.6 * cot + 0.8 * four + three + 2.0 * nu
        dif[x, rows(t), :] = 0.6 * (cot + four) + three + nu
        base[x, rows(t), :] = cot + four + three + nu

    combine(H - 1, H + NX + 1, emit)

    def put(x, t, value):
        out[x - H, rows(t - 1), :] = base[x, rows(t), :] + value

    fd_pass(e, adv, dif, put, H, H + NX, INNER, masks)


def shape(*dims):
    return jax.ShapeDtypeStruct(dims, F32)


FIELD = shape(EX, EY, NZ)
EXT = shape(9, EX, EY, NZ)
STRIP = shape(2 * H, EY, NZ)
ROWS = shape(128, NZ)
VMEM = pl.BlockSpec(memory_space=pltpu.VMEM)
SMEM = pl.BlockSpec(memory_space=pltpu.SMEM)
LIMIT = 24 * 1024 * 1024


def call(kernel, outs, ins, scratch=0, smem=True, name=None):
    return pl.pallas_call(
        kernel,
        out_shape=outs,
        in_specs=[SMEM if smem and i == 0 else VMEM for i in range(len(ins))],
        out_specs=jax.tree.map(lambda _: VMEM, outs),
        scratch_shapes=[pltpu.VMEM(FIELD.shape, F32)] * scratch,
        compiler_params=pltpu.CompilerParams(vmem_limit_bytes=LIMIT),
        name=name,
    )(*ins)


def local(cotangent, speed, coeff, dirs):
    nx, ny = lax.axis_size("gx"), lax.axis_size("gy")
    ix, iy = lax.axis_index("gx"), lax.axis_index("gy")
    edge = jnp.stack([(ix < nx - 1).astype(jnp.int32), (iy < ny - 1).astype(jnp.int32)])
    velocity = speed * (1 - 2 * dirs).astype(F32)[..., None]

    strips = call(
        pack_kernel,
        [shape(NLOW, NY, NZ), shape(NHIGH, NY, NZ), shape(7 * NX, T, NZ), shape(7 * NX, T, NZ)]
        + [shape(NLOW, T, NZ)] * 2 + [shape(NHIGH, T, NZ)] * 2,
        [cotangent, coeff, velocity],
        smem=False,
        name="pack",
    )

    def shifted(value, dx, dy):
        perm = []
        for i in range(nx):
            for j in range(ny):
                if 0 <= i + dx < nx and 0 <= j + dy < ny:
                    perm.append((i * ny + j, (i + dx) * ny + j + dy))
        return lax.ppermute(value, ("gx", "gy"), perm)

    def along_x(up, down):
        return shifted(up, 1, 0), shifted(down, -1, 0)

    def reduced(moments):
        return lax.all_to_all(moments, ("gx", "gy"), 0, 0, tiled=True)

    moves = ((1, 0), (-1, 0), (0, 1), (0, -1), (1, 1), (1, -1), (-1, 1), (-1, -1))
    received = [shifted(s, dx, dy) for s, (dx, dy) in zip(strips, moves)]
    e, y4, w4, up, down, moments = call(
        first_kernel,
        [EXT, FIELD, FIELD, STRIP, STRIP, ROWS],
        [edge, cotangent, coeff, velocity, *received],
        name="first",
    )
    low, high = along_x(up, down)
    nu4, y3, w3, up, down, moments = call(
        third_kernel,
        [FIELD, FIELD, FIELD, STRIP, STRIP, ROWS],
        [edge, e, y4, w4, low, high, reduced(moments)],
        scratch=2,
        name="third",
    )
    low, high = along_x(up, down)
    nu3, y2, w2, moments = call(
        second_kernel,
        [FIELD, FIELD, FIELD, ROWS],
        [edge, e, nu4, y3, w3, low, high, reduced(moments)],
        scratch=2,
        name="second",
    )
    return call(
        last_kernel, shape(NX, NY, NZ), [e, nu4, nu3, y2, w2, reduced(moments)], scratch=3, smem=False, name="last"
    )


def solution(mesh):
    placed = (P("gx", "gy", None), P(None, "gx", "gy", None), P(None, "gx", "gy", None), P(None, "gx", "gy"))
    return jax.shard_map(local, mesh=mesh, in_specs=placed, out_specs=P("gx", "gy", None), check_vma=False)
```

```python
import jax
import jax.numpy as jnp
from jax import lax
from jax.experimental import pallas as pl
from jax.experimental.pallas import tpu as pltpu
from jax.sharding import PartitionSpec as P


NX, NY, NZ = 32, 64, 128
H = 3
T = 8
EX, EY = NX + 2 * H, NY + 2 * T
TILES = EY // T
INNER = range(1, TILES - 1)
F32 = jnp.float32

C, K, U, K2B, U2B = 0, 1, 4, 7, 8
LOW = ((0, 3), (1, 3), (4, 3), (2, 2), (3, 2), (5, 2), (6, 2))
HIGH = ((0, 3), (1, 2), (4, 2), (2, 2), (3, 2), (5, 2), (6, 2))
NLOW = sum(n for _, n in LOW)
NHIGH = sum(n for _, n in HIGH)
STEP = 9
BLOCK_STEP = 8


def rows(t):
    return slice(t * T, (t + 1) * T)


class Masks:
    def __init__(self):
        lane = lax.broadcasted_iota(jnp.int32, (T, NZ), 1)
        row = lax.broadcasted_iota(jnp.int32, (T, NZ), 0)
        self.first, self.last, self.top = lane == 0, lane == NZ - 1, row == 0


def back(v):
    return pltpu.roll(v, 1, 1)


class Tiles:
    def __init__(self, ref, masks):
        self.ref, self.masks, self.seen = ref, masks, {}

    def at(self, x, i, t):
        key = (i, t)
        if key not in self.seen:
            self.seen[key] = self.ref[x + i, rows(t), :]
        return self.seen[key]

    def dx(self, x, i, t):
        return self.at(x, i + 1, t) - self.at(x, i, t)

    def dy(self, x, i, t):
        v = self.at(x, i, t)
        if t + 1 < TILES:
            return self.ref[x + i, t * T + 1 : (t + 1) * T + 1, :] - v
        return pltpu.roll(v, T - 1, 0) - v

    def dz(self, x, i, t):
        v = self.at(x, i, t)
        return jnp.where(self.masks.last, 0.0, pltpu.roll(v, NZ - 1, 1)) - v

    def dz_below(self, x, i, t):
        v = self.at(x, i, t)
        return v - back(v)


def sweep(x0, x1, step, body, carry):
    count = (x1 - x0) // step
    assert count * step == x1 - x0
    return lax.fori_loop(0, count, lambda n, c: body(x0 + n * step, c), carry)


def fluxes(x0, tiles, masks, parts, emit):
    def plane(x, low_x, i, fetch):
        new_low = []
        before = jnp.zeros((T, NZ), F32)
        if tiles[0] > 0:
            before = pltpu.roll(parts(fetch, 1, x, i, tiles[0] - 1)[1], 1, 0)
        for n, t in enumerate(tiles):
            up_x, down_x = parts(fetch, 0, x, i, t)
            up_y, down_y = parts(fetch, 1, x, i, t)
            up_z, down_z = parts(fetch, 2, x, i, t)
            rolled = pltpu.roll(down_y, 1, 0)
            down_y = jnp.where(masks.top, before, rolled)
            before = rolled
            total = (up_x - low_x[n]) + (up_y - down_y) + (up_z - down_z)
            new_low.append(down_x)
            emit(fetch, x, i, t, total)
        return new_low

    return plane


def run(x0, x1, step, tiles, masks, fetch_of, parts, emit):
    plane = fluxes(x0, tiles, masks, parts, emit)
    fetch = fetch_of()
    low = [parts(fetch, 0, x0 - 1, 0, t)[1] for t in tiles]

    def body(x, low):
        fetch = fetch_of()
        for i in range(step):
            low = plane(x, low, i, fetch)
        return low

    sweep(x0, x1, step, body, low)


def m_pass(e, v_ref, w_ref, masks):
    def parts(v, d, x, i, t):
        if d == 2:
            return e[K + 2, x + i, rows(t), :] * v.dz(x, i, t), e[K2B, x + i, rows(t), :] * v.dz_below(x, i, t)
        flux = e[K + d, x + i, rows(t), :] * (v.dx, v.dy)[d](x, i, t)
        return flux, flux

    def emit(v, x, i, t, total):
        w_ref[x + i, rows(t), :] = v.at(x, i, t) - total

    run(1, EX - 1, STEP, range(TILES), masks, lambda: Tiles(v_ref, masks), parts, emit)


def s_pass(e, y_ref, masks):
    cot = e.at[C]

    def parts(v, d, x, i, t):
        k, u = e[K + d, x + i, rows(t), :], e[U + d, x + i, rows(t), :]
        delta = (v.dx, v.dy, v.dz)[d](x, i, t)
        up = (k + jnp.maximum(u, 0.0)) * delta
        if d == 2:
            k, u = e[K2B, x + i, rows(t), :], e[U2B, x + i, rows(t), :]
            delta = v.dz_below(x, i, t)
        return up, (k - jnp.minimum(u, 0.0)) * delta

    def emit(v, x, i, t, total):
        y_ref[x + i, rows(t), :] = total

    run(1, EX - 1, STEP, range(TILES), masks, lambda: Tiles(cot, masks), parts, emit)


def fd_pass(e, a_ref, d_ref, put, x0, x1, step, tiles, masks):
    def parts(both, d, x, i, t):
        a, b = both
        k, u = e[K + d, x + i, rows(t), :], e[U + d, x + i, rows(t), :]
        da, db = ((v.dx, v.dy, v.dz)[d](x, i, t) for v in (a, b))
        flux = k * db
        up = flux + jnp.maximum(u, 0.0) * da
        if d == 2:
            u = e[U2B, x + i, rows(t), :]
            flux = e[K2B, x + i, rows(t), :] * b.dz_below(x, i, t)
            da = a.dz_below(x, i, t)
        return up, flux - jnp.minimum(u, 0.0) * da

    def emit(both, x, i, t, total):
        put(x + i, t, total)

    run(x0, x1, step, tiles, masks, lambda: (Tiles(a_ref, masks), Tiles(d_ref, masks)), parts, emit)


def products(e, y_ref, w_ref, masks):
    zero = jnp.zeros((T, NZ), F32)

    def body(x, accs):
        yy, yw, ww, *energy = accs
        w = Tiles(w_ref, masks)
        for i in range(BLOCK_STEP):
            for t in INNER:
                v, y = w.at(x, i, t), y_ref[x + i, rows(t), :]
                yy, yw, ww = yy + y * y, yw + y * v, ww + v * v
                for d, delta in enumerate((w.dx, w.dy, w.dz)):
                    difference = delta(x, i, t)
                    energy[d] = energy[d] + e[K + d, x + i, rows(t), :] * (difference * difference)
        return yy, yw, ww, *energy

    yy, yw, ww, *energy = sweep(H, H + NX, BLOCK_STEP, body, (zero,) * 6)
    return yy, yw, ww, ww + (energy[0] + energy[1] + energy[2])


def outside_is_zero(edge, ref):
    @pl.when(edge[0] == 0)
    def _():
        ref[H + NX : EX - 1] = jnp.zeros((H - 1, EY, NZ), F32)

    @pl.when(edge[1] == 0)
    def _():
        ref[:, EY - T :, :] = jnp.zeros((EX, T, NZ), F32)


def finish(edge, e, y, w, up, down, moments, masks):
    outside_is_zero(edge, y)
    m_pass(e, y, w, masks)
    outside_is_zero(edge, w)
    if up is not None:
        for n, ref in enumerate((y, w)):
            up[n * H : (n + 1) * H] = ref[NX : NX + H]
            down[n * H : (n + 1) * H] = ref[H : 2 * H]
    sums = products(e, y, w, masks)
    lane = lax.broadcasted_iota(jnp.int32, (1, NZ), 1)
    row = jnp.zeros((1, NZ), F32)
    for i, acc in enumerate(sums):
        total = jnp.sum(jnp.sum(acc, axis=0, keepdims=True), axis=1, keepdims=True)
        row = jnp.where(lane // 32 == i, total, row)
    moments[...] = jnp.broadcast_to(row, moments.shape)


def coefficients(moments_ref):
    sums = jnp.sum(moments_ref[...], axis=0, keepdims=True)
    lane = lax.broadcasted_iota(jnp.int32, (1, NZ), 1)
    m0, m1, m2, m3 = (jnp.sum(jnp.where(lane == 32 * i, sums, 0.0), axis=1, keepdims=True) for i in range(4))
    alpha0 = m0 / m1
    rr = alpha0 * alpha0 * m2 - m0
    product = m1 - 2.0 * alpha0 * m2 + alpha0 * alpha0 * m3
    ratio = rr / m0
    alpha1 = rr / (product - ratio * rr / alpha0)
    a = alpha0 + alpha1 * (1.0 + ratio)
    b = -(alpha1 * alpha0)
    return jnp.broadcast_to(a, (T, NZ)), jnp.broadcast_to(b, (T, NZ))


def signs(dirs, d, x, first_rows):
    sign = (1 - 2 * dirs[d, pl.ds(x, 1), :]).astype(F32)
    count = T * len(first_rows)
    row = lax.broadcasted_iota(jnp.int32, (count, NY), 0)
    column = lax.broadcasted_iota(jnp.int32, (count, NY), 1)
    at = row
    for n, first in enumerate(first_rows):
        at = jnp.where(row // T == n, row - n * T + first, at)
    picked = jnp.where(at == column, jnp.broadcast_to(sign, (count, NY)), 0.0)
    ones = jnp.ones((NY, NZ), jnp.bfloat16)
    return jnp.dot(picked.astype(jnp.bfloat16), ones, preferred_element_type=F32)


def pack_kernel(edge, cot, speed, coeff, dirs, low, high, ylow, yhigh, cll, clh, chl, chh, sems):
    bottom, top, full = slice(0, T), slice(NY - T, NY), slice(0, NY)
    copies = []

    def fetch(f, planes, rows, target):
        source = cot.at[planes, rows] if f == 0 else (coeff if f < 4 else speed).at[(f - 1) % 3, planes, rows]
        copy = pltpu.make_async_copy(source, target, sems.at[len(copies)])
        copy.start()
        copies.append(copy)

    for f in range(7):
        fetch(f, slice(0, NX), top, ylow.at[f * NX : (f + 1) * NX])
        fetch(f, slice(0, NX), bottom, yhigh.at[f * NX : (f + 1) * NX])
    signed = []
    for fields, strip in ((LOW, low), (HIGH, high)):
        at = 0
        for f, n in fields:
            start = NX - n if fields is LOW else 0
            fetch(f, slice(start, start + n), full, strip.at[at : at + n])
            if f >= 4:
                signed += [(strip, at + i, f - 4, start + i) for i in range(n)]
            at += n
    for copy in copies:
        copy.wait()
    for d in range(3):
        for x in range(NX):
            sign = signs(dirs, d, x, (NY - T, 0))
            at = (4 + d) * NX + x
            ylow[at] = ylow[at] * sign[:T]
            yhigh[at] = yhigh[at] * sign[T:]
    for strip, at, d, x in signed:
        strip[at] = strip[at] * signs(dirs, d, x, tuple(range(0, NY, T)))
    cll[...] = low[:, top, :]
    clh[...] = low[:, bottom, :]
    chl[...] = high[:, top, :]
    chh[...] = high[:, bottom, :]


def place(e, f, x, rows, value):
    if f > 0:
        value = 0.25 * value
    e[f, x, rows, :] = value
    if f in (K + 2, U + 2):
        first = lax.broadcasted_iota(jnp.int32, value.shape, 1) == 0
        e[K2B if f == K + 2 else U2B, x, rows, :] = jnp.where(first, 0.0, back(value))


def center_kernel(cot, speed, coeff, dirs, e, sems):
    every = tuple(range(0, NY, T))
    middle = slice(T, T + NY)
    copies = []
    for f in range(7):
        source = cot if f == 0 else (coeff if f < 4 else speed).at[(f - 1) % 3]
        copies.append(pltpu.make_async_copy(source, e.at[f, H : H + NX, middle], sems.at[f]))
    for copy in copies:
        copy.start()
    for copy in copies:
        copy.wait()

    def body(n, _):
        for i in range(2):
            x = H + 2 * n + i
            for d in range(3):
                place(e, K + d, x, middle, e[K + d, x, middle, :])
                place(e, U + d, x, middle, e[U + d, x, middle, :] * signs(dirs, d, x - H, every))
        return _

    lax.fori_loop(0, NX // 2, body, 0)


def first_kernel(edge, e_in, low, high, ylow, yhigh, cll, clh, chl, chh, e, y, w, up, down, moments):
    masks = Masks()
    middle, below, above = slice(T, T + NY), slice(0, T), slice(T + NY, EY)
    for fields, base, middles, lows, highs in (
        (LOW, None, low, cll, clh),
        (HIGH, H + NX, high, chl, chh),
    ):
        at = 0
        for f, n in fields:
            for i in range(n):
                x = (H - n if base is None else base) + i
                place(e, f, x, middle, middles[at + i])
                place(e, f, x, below, lows[at + i])
                place(e, f, x, above, highs[at + i])
            at += n

    def body(n, _):
        for i in range(4):
            x = 4 * n + i
            for f in range(7):
                place(e, f, H + x, below, ylow[f * NX + x])
                place(e, f, H + x, above, yhigh[f * NX + x])
        return _

    lax.fori_loop(0, NX // 4, body, 0)
    s_pass(e, y, masks)
    finish(edge, e, y, w, up, down, moments, masks)


def combine(x0, x1, emit):
    def body(x, _):
        for t in range(TILES):
            emit(x, t)
        return _

    lax.fori_loop(x0, x1, body, 0)


def nu_of(a, b, y, w, low, high, emit):
    combine(H, H + NX, lambda x, t: emit(x, t, a * y[x, rows(t), :] + b * w[x, rows(t), :]))
    for base, strip in ((0, low), (H + NX, high)):
        for i in range(H):
            for t in range(TILES):
                emit(base + i, t, a * strip[i, rows(t), :] + b * strip[H + i, rows(t), :])


def third_kernel(edge, e, y4, w4, low, high, sums, nu4, y, w, up, down, moments, adv, dif):
    masks = Masks()
    a, b = coefficients(sums)

    def emit(x, t, nu):
        c = e[C, x, rows(t), :]
        nu4[x, rows(t), :] = nu
        adv[x, rows(t), :] = c + 2.0 * nu
        dif[x, rows(t), :] = c + nu

    nu_of(a, b, y4, w4, low, high, emit)

    def put(x, t, value):
        y[x, rows(t), :] = value

    fd_pass(e, adv, dif, put, 1, EX - 1, STEP, range(TILES), masks)
    finish(edge, e, y, w, up, down, moments, masks)


def second_kernel(edge, e, nu4, y3, w3, low, high, sums, nu3, y, w, moments, adv, dif):
    masks = Masks()
    a, b = coefficients(sums)

    def emit(x, t, nu):
        c = 1.4 * e[C, x, rows(t), :]
        four = nu4[x, rows(t), :]
        nu3[x, rows(t), :] = nu
        adv[x, rows(t), :] = c + 1.2 * four + 2.0 * nu
        dif[x, rows(t), :] = c + 1.4 * four + nu

    nu_of(a, b, y3, w3, low, high, emit)

    def put(x, t, value):
        y[x, rows(t), :] = value

    fd_pass(e, adv, dif, put, 1, EX - 1, STEP, range(TILES), masks)
    finish(edge, e, y, w, None, None, moments, masks)


def last_kernel(e, nu4, nu3, y2, w2, sums, out, adv, dif, base):
    masks = Masks()
    a, b = coefficients(sums)

    def emit(x, t):
        nu = a * y2[x, rows(t), :] + b * w2[x, rows(t), :]
        cot = e[C, x, rows(t), :]
        four, three = nu4[x, rows(t), :], nu3[x, rows(t), :]
        adv[x, rows(t), :] = 0.6 * cot + 0.8 * four + three + 2.0 * nu
        dif[x, rows(t), :] = 0.6 * (cot + four) + three + nu
        base[x, rows(t), :] = cot + four + three + nu

    combine(H - 1, H + NX + 1, emit)

    def put(x, t, value):
        out[x - H, rows(t - 1), :] = base[x, rows(t), :] + value

    fd_pass(e, adv, dif, put, H, H + NX, BLOCK_STEP, INNER, masks)


def shape(*dims):
    return jax.ShapeDtypeStruct(dims, F32)


FIELD = shape(EX, EY, NZ)
EXT = shape(9, EX, EY, NZ)
STRIP = shape(2 * H, EY, NZ)
ROWS = shape(128, NZ)
VMEM = pl.BlockSpec(memory_space=pltpu.VMEM)
SMEM = pl.BlockSpec(memory_space=pltpu.SMEM)
HBM = pl.BlockSpec(memory_space=pltpu.HBM)
LIMIT = 8 * 1024 * 1024


def call(kernel, outs, ins, scratch=0, name=None, specs=None, sems=0, aliases=None):
    return pl.pallas_call(
        kernel,
        out_shape=outs,
        in_specs=specs or [SMEM] + [VMEM] * (len(ins) - 1),
        out_specs=jax.tree.map(lambda _: VMEM, outs),
        scratch_shapes=[pltpu.VMEM(FIELD.shape, F32)] * scratch + ([pltpu.SemaphoreType.DMA((sems,))] if sems else []),
        input_output_aliases=aliases or {},
        compiler_params=pltpu.CompilerParams(vmem_limit_bytes=LIMIT),
        name=name,
    )(*ins)


def local(cotangent, speed, coeff, dirs):
    nx, ny = lax.axis_size("gx"), lax.axis_size("gy")
    ix, iy = lax.axis_index("gx"), lax.axis_index("gy")
    hbm = [pltpu.with_memory_space_constraint(v, pltpu.HBM) for v in (cotangent, speed, coeff)]
    edge = jnp.stack([(ix < nx - 1).astype(jnp.int32), (iy < ny - 1).astype(jnp.int32)])

    strips = call(
        pack_kernel,
        [shape(NLOW, NY, NZ), shape(NHIGH, NY, NZ), shape(7 * NX, T, NZ), shape(7 * NX, T, NZ)]
        + [shape(NLOW, T, NZ)] * 2 + [shape(NHIGH, T, NZ)] * 2,
        [edge, *hbm, dirs],
        specs=[SMEM, HBM, HBM, HBM, VMEM],
        sems=28,
        name="pack",
    )

    def shifted(value, dx, dy):
        perm = []
        for i in range(nx):
            for j in range(ny):
                if 0 <= i + dx < nx and 0 <= j + dy < ny:
                    perm.append((i * ny + j, (i + dx) * ny + j + dy))
        return lax.ppermute(value, ("gx", "gy"), perm)

    def along_x(up, down):
        return shifted(up, 1, 0), shifted(down, -1, 0)

    def reduced(moments):
        return lax.all_to_all(moments, ("gx", "gy"), 0, 0, tiled=True)

    moves = ((1, 0), (-1, 0), (0, 1), (0, -1), (1, 1), (1, -1), (-1, 1), (-1, -1))
    received = [shifted(s, dx, dy) for s, (dx, dy) in zip(strips, moves)]
    e = call(center_kernel, EXT, [*hbm, dirs], specs=[HBM] * 3 + [VMEM], sems=7, name="center")
    e, y4, w4, up, down, moments = call(
        first_kernel,
        [EXT, FIELD, FIELD, STRIP, STRIP, ROWS],
        [edge, e, *received],
        aliases={1: 0},
        name="first",
    )
    low, high = along_x(up, down)
    nu4, y3, w3, up, down, moments = call(
        third_kernel,
        [FIELD, FIELD, FIELD, STRIP, STRIP, ROWS],
        [edge, e, y4, w4, low, high, reduced(moments)],
        scratch=2,
        name="third",
    )
    low, high = along_x(up, down)
    nu3, y2, w2, moments = call(
        second_kernel,
        [FIELD, FIELD, FIELD, ROWS],
        [edge, e, nu4, y3, w3, low, high, reduced(moments)],
        scratch=2,
        name="second",
    )
    return call(
        last_kernel, shape(NX, NY, NZ), [e, nu4, nu3, y2, w2, reduced(moments)], scratch=3, specs=[VMEM] * 6, name="last"
    )


def solution(mesh):
    placed = (P("gx", "gy", None), P(None, "gx", "gy", None), P(None, "gx", "gy", None), P(None, "gx", "gy"))
    return jax.shard_map(local, mesh=mesh, in_specs=placed, out_specs=P("gx", "gy", None), check_vma=False)
```

```python
import jax
import jax.numpy as jnp
from jax import lax
from jax.experimental import pallas as pl
from jax.experimental.pallas import tpu as pltpu
from jax.sharding import PartitionSpec as P


NX, NY, NZ = 32, 64, 128
H = 3
T = 8
EX, EY = NX + 2 * H, NY + 2 * T
TILES = EY // T
INNER = range(1, TILES - 1)
F32 = jnp.float32

C, K, U, K2B, U2B = 0, 1, 4, 7, 8
LOW = ((0, 3), (1, 3), (4, 3), (2, 2), (3, 2), (5, 2), (6, 2))
HIGH = ((0, 3), (1, 2), (4, 2), (2, 2), (3, 2), (5, 2), (6, 2))
NLOW = sum(n for _, n in LOW)
NHIGH = sum(n for _, n in HIGH)
YLOW = ((0, 7), (1, 6), (4, 6), (2, 7), (3, 6), (5, 7), (6, 6))
YHIGH = ((0, 7), (1, 6), (4, 6), (2, 6), (3, 6), (5, 6), (6, 6))
GROUP = 8
YROWS_LOW = GROUP * sum(n for _, n in YLOW)
YROWS_HIGH = GROUP * sum(n for _, n in YHIGH)
STEP = 9
CENTER_STEP = 8
BLOCK_STEP = 8


def rows(t):
    return slice(t * T, (t + 1) * T)


class Masks:
    def __init__(self):
        lane = lax.broadcasted_iota(jnp.int32, (T, NZ), 1)
        row = lax.broadcasted_iota(jnp.int32, (T, NZ), 0)
        self.first, self.last, self.top = lane == 0, lane == NZ - 1, row == 0


def back(v):
    return pltpu.roll(v, 1, 1)


class Tiles:
    def __init__(self, ref, masks):
        self.ref, self.masks, self.seen = ref, masks, {}

    def at(self, x, i, t):
        key = (i, t)
        if key not in self.seen:
            self.seen[key] = self.ref[x + i, rows(t), :]
        return self.seen[key]

    def dx(self, x, i, t):
        return self.at(x, i + 1, t) - self.at(x, i, t)

    def dy(self, x, i, t):
        v = self.at(x, i, t)
        if t + 1 < TILES:
            return self.ref[x + i, t * T + 1 : (t + 1) * T + 1, :] - v
        return pltpu.roll(v, T - 1, 0) - v

    def dz(self, x, i, t):
        v = self.at(x, i, t)
        return jnp.where(self.masks.last, 0.0, pltpu.roll(v, NZ - 1, 1)) - v

    def dz_below(self, x, i, t):
        v = self.at(x, i, t)
        return v - back(v)


def sweep(x0, x1, step, body, carry):
    count = (x1 - x0) // step
    assert count * step == x1 - x0
    return lax.fori_loop(0, count, lambda n, c: body(x0 + n * step, c), carry)


def fluxes(x0, tiles, masks, parts, emit):
    def plane(x, low_x, i, fetch):
        new_low = []
        before = jnp.zeros((T, NZ), F32)
        if tiles[0] > 0:
            before = pltpu.roll(parts(fetch, 1, x, i, tiles[0] - 1)[1], 1, 0)
        for n, t in enumerate(tiles):
            up_x, down_x = parts(fetch, 0, x, i, t)
            up_y, down_y = parts(fetch, 1, x, i, t)
            up_z, down_z = parts(fetch, 2, x, i, t)
            rolled = pltpu.roll(down_y, 1, 0)
            down_y = jnp.where(masks.top, before, rolled)
            before = rolled
            total = (up_x - low_x[n]) + (up_y - down_y) + (up_z - down_z)
            new_low.append(down_x)
            emit(fetch, x, i, t, total)
        return new_low

    return plane


def run(x0, x1, step, tiles, masks, fetch_of, parts, emit):
    plane = fluxes(x0, tiles, masks, parts, emit)
    fetch = fetch_of()
    low = [parts(fetch, 0, x0 - 1, 0, t)[1] for t in tiles]

    def body(x, low):
        fetch = fetch_of()
        for i in range(step):
            low = plane(x, low, i, fetch)
        return low

    sweep(x0, x1, step, body, low)


def m_pass(e, v_ref, w_ref, masks):
    def parts(v, d, x, i, t):
        if d == 2:
            return e[K + 2, x + i, rows(t), :] * v.dz(x, i, t), e[K2B, x + i, rows(t), :] * v.dz_below(x, i, t)
        flux = e[K + d, x + i, rows(t), :] * (v.dx, v.dy)[d](x, i, t)
        return flux, flux

    def emit(v, x, i, t, total):
        w_ref[x + i, rows(t), :] = v.at(x, i, t) - total

    run(1, EX - 1, STEP, range(TILES), masks, lambda: Tiles(v_ref, masks), parts, emit)


def s_pass(e, y_ref, masks):
    cot = e.at[C]

    def parts(v, d, x, i, t):
        k, u = e[K + d, x + i, rows(t), :], e[U + d, x + i, rows(t), :]
        delta = (v.dx, v.dy, v.dz)[d](x, i, t)
        up = (k + jnp.maximum(u, 0.0)) * delta
        if d == 2:
            k, u = e[K2B, x + i, rows(t), :], e[U2B, x + i, rows(t), :]
            delta = v.dz_below(x, i, t)
        return up, (k - jnp.minimum(u, 0.0)) * delta

    def emit(v, x, i, t, total):
        y_ref[x + i, rows(t), :] = total

    run(1, EX - 1, STEP, range(TILES), masks, lambda: Tiles(cot, masks), parts, emit)


def fd_pass(e, a_ref, d_ref, put, x0, x1, step, tiles, masks):
    def parts(both, d, x, i, t):
        a, b = both
        k, u = e[K + d, x + i, rows(t), :], e[U + d, x + i, rows(t), :]
        da, db = ((v.dx, v.dy, v.dz)[d](x, i, t) for v in (a, b))
        flux = k * db
        up = flux + jnp.maximum(u, 0.0) * da
        if d == 2:
            u = e[U2B, x + i, rows(t), :]
            flux = e[K2B, x + i, rows(t), :] * b.dz_below(x, i, t)
            da = a.dz_below(x, i, t)
        return up, flux - jnp.minimum(u, 0.0) * da

    def emit(both, x, i, t, total):
        put(x + i, t, total)

    run(x0, x1, step, tiles, masks, lambda: (Tiles(a_ref, masks), Tiles(d_ref, masks)), parts, emit)


def products(e, y_ref, w_ref, masks):
    zero = jnp.zeros((T, NZ), F32)

    def body(x, accs):
        yy, yw, ww, *energy = accs
        w = Tiles(w_ref, masks)
        for i in range(BLOCK_STEP):
            for t in INNER:
                v, y = w.at(x, i, t), y_ref[x + i, rows(t), :]
                yy, yw, ww = yy + y * y, yw + y * v, ww + v * v
                for d, delta in enumerate((w.dx, w.dy, w.dz)):
                    difference = delta(x, i, t)
                    energy[d] = energy[d] + e[K + d, x + i, rows(t), :] * (difference * difference)
        return yy, yw, ww, *energy

    yy, yw, ww, *energy = sweep(H, H + NX, BLOCK_STEP, body, (zero,) * 6)
    return yy, yw, ww, ww + (energy[0] + energy[1] + energy[2])


def outside_is_zero(edge, ref):
    @pl.when(edge[0] == 0)
    def _():
        ref[H + NX : EX - 1] = jnp.zeros((H - 1, EY, NZ), F32)

    @pl.when(edge[1] == 0)
    def _():
        ref[:, EY - T :, :] = jnp.zeros((EX, T, NZ), F32)


def finish(edge, e, y, w, up, down, moments, masks):
    outside_is_zero(edge, y)
    m_pass(e, y, w, masks)
    outside_is_zero(edge, w)
    if up is not None:
        for n, ref in enumerate((y, w)):
            up[n * H : (n + 1) * H] = ref[NX : NX + H]
            down[n * H : (n + 1) * H] = ref[H : 2 * H]
    sums = products(e, y, w, masks)
    lane = lax.broadcasted_iota(jnp.int32, (1, NZ), 1)
    row = jnp.zeros((1, NZ), F32)
    for i, acc in enumerate(sums):
        total = jnp.sum(jnp.sum(acc, axis=0, keepdims=True), axis=1, keepdims=True)
        row = jnp.where(lane // 32 == i, total, row)
    moments[...] = jnp.broadcast_to(row, moments.shape)


def coefficients(moments_ref):
    sums = jnp.sum(moments_ref[...], axis=0, keepdims=True)
    lane = lax.broadcasted_iota(jnp.int32, (1, NZ), 1)
    m0, m1, m2, m3 = (jnp.sum(jnp.where(lane == 32 * i, sums, 0.0), axis=1, keepdims=True) for i in range(4))
    alpha0 = m0 / m1
    rr = alpha0 * alpha0 * m2 - m0
    product = m1 - 2.0 * alpha0 * m2 + alpha0 * alpha0 * m3
    ratio = rr / m0
    alpha1 = rr / (product - ratio * rr / alpha0)
    a = alpha0 + alpha1 * (1.0 + ratio)
    b = -(alpha1 * alpha0)
    return jnp.broadcast_to(a, (T, NZ)), jnp.broadcast_to(b, (T, NZ))


def signs(dirs, d, x, first_rows):
    sign = (1 - 2 * dirs[d, pl.ds(x, 1), :]).astype(F32)
    count = T * len(first_rows)
    row = lax.broadcasted_iota(jnp.int32, (count, NY), 0)
    column = lax.broadcasted_iota(jnp.int32, (count, NY), 1)
    at = row
    for n, first in enumerate(first_rows):
        at = jnp.where(row // T == n, row - n * T + first, at)
    picked = jnp.where(at == column, jnp.broadcast_to(sign, (count, NY)), 0.0)
    ones = jnp.ones((NY, NZ), jnp.bfloat16)
    return jnp.dot(picked.astype(jnp.bfloat16), ones, preferred_element_type=F32)


def pack_kernel(edge, cot, speed, coeff, all_dirs, low, high, ylow, yhigh, cll, clh, chl, chh, dirs, tops, bottoms, sems):
    bottom, top, full = slice(0, T), slice(NY - T, NY), slice(0, NY)
    copies = [pltpu.make_async_copy(all_dirs, dirs, sems.at[0])]
    copies[0].start()

    def fetch(f, planes, rows, target):
        source = cot.at[planes, rows] if f == 0 else (coeff if f < 4 else speed).at[(f - 1) % 3, planes, rows]
        copy = pltpu.make_async_copy(source, target, sems.at[len(copies)])
        copy.start()
        copies.append(copy)

    for f in range(7):
        fetch(f, slice(0, NX), top, tops.at[f])
        fetch(f, slice(0, NX), bottom, bottoms.at[f])
    signed = []
    for fields, strip in ((LOW, low), (HIGH, high)):
        at = 0
        for f, n in fields:
            start = NX - n if fields is LOW else 0
            fetch(f, slice(start, start + n), full, strip.at[at : at + n])
            if f >= 4:
                signed += [(strip, at + i, f - 4, start + i) for i in range(n)]
            at += n
    for copy in copies:
        copy.wait()
    for group in range(NX // GROUP):
        at_low = at_high = 0
        for x in range(group * GROUP, (group + 1) * GROUP):
            sign = [signs(dirs, d, x, (NY - T, 0)) for d in range(3)]
            for (f, n), (_, m) in zip(YLOW, YHIGH):
                upper, lower = tops[f, x], bottoms[f, x]
                if f >= 4:
                    upper, lower = upper * sign[f - 4][:T], lower * sign[f - 4][T:]
                ylow[group, at_low : at_low + n, :] = upper[T - n :]
                yhigh[group, at_high : at_high + m, :] = lower[:m]
                at_low += n
                at_high += m
    for strip, at, d, x in signed:
        strip[at] = strip[at] * signs(dirs, d, x, tuple(range(0, NY, T)))
    cll[...] = low[:, top, :]
    clh[...] = low[:, bottom, :]
    chl[...] = high[:, top, :]
    chh[...] = high[:, bottom, :]


def place(e, f, x, rows, value):
    if f > 0:
        value = 0.25 * value
    e[f, x, rows, :] = value
    if f in (K + 2, U + 2):
        first = lax.broadcasted_iota(jnp.int32, value.shape, 1) == 0
        e[K2B if f == K + 2 else U2B, x, rows, :] = jnp.where(first, 0.0, back(value))


def shifted_tile(ref, group, start):
    inside = min(max(start, 0), ref.shape[1] - T)
    value = ref[group, inside : inside + T, :]
    return value if inside == start else pltpu.roll(value, (inside - start) % T, 0)


def center_kernel(cot, speed, coeff, dirs, e):
    every = tuple(range(0, NY, T))
    middle = slice(T, T + NY)

    def body(n, _):
        for i in range(CENTER_STEP):
            x = CENTER_STEP * n + i
            place(e, C, H + x, middle, cot[x])
            for d in range(3):
                place(e, K + d, H + x, middle, coeff[d, x])
                place(e, U + d, H + x, middle, speed[d, x] * signs(dirs, d, x, every))
        return _

    lax.fori_loop(0, NX // CENTER_STEP, body, 0)


def first_kernel(edge, e_in, low, high, ylow, yhigh, cll, clh, chl, chh, e, y, w, up, down, moments):
    masks = Masks()
    middle, below, above = slice(T, T + NY), slice(0, T), slice(T + NY, EY)
    for fields, base, middles, lows, highs in (
        (LOW, None, low, cll, clh),
        (HIGH, H + NX, high, chl, chh),
    ):
        at = 0
        for f, n in fields:
            for i in range(n):
                x = (H - n if base is None else base) + i
                place(e, f, x, middle, middles[at + i])
                place(e, f, x, below, lows[at + i])
                place(e, f, x, above, highs[at + i])
            at += n

    def body(group, _):
        at_low = at_high = 0
        for i in range(GROUP):
            x = H + group * GROUP + i
            for (f, n), (_, m) in zip(YLOW, YHIGH):
                place(e, f, x, below, shifted_tile(ylow, group, at_low + n - T))
                place(e, f, x, above, shifted_tile(yhigh, group, at_high))
                at_low += n
                at_high += m
        return _

    lax.fori_loop(0, NX // GROUP, body, 0)
    s_pass(e, y, masks)
    finish(edge, e, y, w, up, down, moments, masks)


def combine(x0, x1, emit):
    def body(x, _):
        for t in range(TILES):
            emit(x, t)
        return _

    lax.fori_loop(x0, x1, body, 0)


def nu_of(a, b, y, w, low, high, emit):
    combine(H, H + NX, lambda x, t: emit(x, t, a * y[x, rows(t), :] + b * w[x, rows(t), :]))
    for base, strip in ((0, low), (H + NX, high)):
        for i in range(H):
            for t in range(TILES):
                emit(base + i, t, a * strip[i, rows(t), :] + b * strip[H + i, rows(t), :])


def third_kernel(edge, e, y4, w4, low, high, sums, nu4, y, w, up, down, moments, adv, dif):
    masks = Masks()
    a, b = coefficients(sums)

    def emit(x, t, nu):
        c = e[C, x, rows(t), :]
        nu4[x, rows(t), :] = nu
        adv[x, rows(t), :] = c + 2.0 * nu
        dif[x, rows(t), :] = c + nu

    nu_of(a, b, y4, w4, low, high, emit)

    def put(x, t, value):
        y[x, rows(t), :] = value

    fd_pass(e, adv, dif, put, 1, EX - 1, STEP, range(TILES), masks)
    finish(edge, e, y, w, up, down, moments, masks)


def second_kernel(edge, e, nu4, y3, w3, low, high, sums, nu3, y, w, moments, adv, dif):
    masks = Masks()
    a, b = coefficients(sums)

    def emit(x, t, nu):
        c = 1.4 * e[C, x, rows(t), :]
        four = nu4[x, rows(t), :]
        nu3[x, rows(t), :] = nu
        adv[x, rows(t), :] = c + 1.2 * four + 2.0 * nu
        dif[x, rows(t), :] = c + 1.4 * four + nu

    nu_of(a, b, y3, w3, low, high, emit)

    def put(x, t, value):
        y[x, rows(t), :] = value

    fd_pass(e, adv, dif, put, 1, EX - 1, STEP, range(TILES), masks)
    finish(edge, e, y, w, None, None, moments, masks)


def last_kernel(e, nu4, nu3, y2, w2, sums, out, adv, dif, base):
    masks = Masks()
    a, b = coefficients(sums)

    def emit(x, t):
        nu = a * y2[x, rows(t), :] + b * w2[x, rows(t), :]
        cot = e[C, x, rows(t), :]
        four, three = nu4[x, rows(t), :], nu3[x, rows(t), :]
        adv[x, rows(t), :] = 0.6 * cot + 0.8 * four + three + 2.0 * nu
        dif[x, rows(t), :] = 0.6 * (cot + four) + three + nu
        base[x, rows(t), :] = cot + four + three + nu

    combine(H - 1, H + NX + 1, emit)

    def put(x, t, value):
        out[x - H, rows(t - 1), :] = base[x, rows(t), :] + value

    fd_pass(e, adv, dif, put, H, H + NX, BLOCK_STEP, INNER, masks)


def shape(*dims):
    return jax.ShapeDtypeStruct(dims, F32)


FIELD = shape(EX, EY, NZ)
EXT = shape(9, EX, EY, NZ)
SCRATCH = [pltpu.VMEM((EX, EY, NZ), F32)]
STRIP = shape(2 * H, EY, NZ)
ROWS = shape(128, NZ)
VMEM = pl.BlockSpec(memory_space=pltpu.VMEM)
SMEM = pl.BlockSpec(memory_space=pltpu.SMEM)
HBM = pl.BlockSpec(memory_space=pltpu.HBM)
LIMIT = 8 * 1024 * 1024


def call(kernel, outs, ins, scratch=(), name=None, specs=None, sems=0, aliases=None):
    return pl.pallas_call(
        kernel,
        out_shape=outs,
        in_specs=specs or [SMEM] + [VMEM] * (len(ins) - 1),
        out_specs=jax.tree.map(lambda _: VMEM, outs),
        scratch_shapes=list(scratch) + ([pltpu.SemaphoreType.DMA((sems,))] if sems else []),
        input_output_aliases=aliases or {},
        compiler_params=pltpu.CompilerParams(vmem_limit_bytes=LIMIT),
        name=name,
    )(*ins)


def local(cotangent, speed, coeff, dirs):
    nx, ny = lax.axis_size("gx"), lax.axis_size("gy")
    ix, iy = lax.axis_index("gx"), lax.axis_index("gy")
    hbm = [pltpu.with_memory_space_constraint(v, pltpu.HBM) for v in (cotangent, speed, coeff, dirs)]
    edge = jnp.stack([(ix < nx - 1).astype(jnp.int32), (iy < ny - 1).astype(jnp.int32)])

    strips = call(
        pack_kernel,
        [shape(NLOW, NY, NZ), shape(NHIGH, NY, NZ), shape(NX // GROUP, YROWS_LOW, NZ), shape(NX // GROUP, YROWS_HIGH, NZ)]
        + [shape(NLOW, T, NZ)] * 2 + [shape(NHIGH, T, NZ)] * 2,
        [edge, *hbm],
        specs=[SMEM] + [HBM] * 4,
        scratch=[pltpu.VMEM((3, NX, NY), jnp.int32)] + [pltpu.VMEM((7, NX, T, NZ), F32)] * 2,
        sems=29,
        name="pack",
    )

    def shifted(value, dx, dy):
        perm = []
        for i in range(nx):
            for j in range(ny):
                if 0 <= i + dx < nx and 0 <= j + dy < ny:
                    perm.append((i * ny + j, (i + dx) * ny + j + dy))
        return lax.ppermute(value, ("gx", "gy"), perm)

    def along_x(up, down):
        return shifted(up, 1, 0), shifted(down, -1, 0)

    def reduced(moments):
        return lax.all_to_all(moments, ("gx", "gy"), 0, 0, tiled=True)

    moves = ((1, 0), (-1, 0), (0, 1), (0, -1), (1, 1), (1, -1), (-1, 1), (-1, -1))
    received = [shifted(s, dx, dy) for s, (dx, dy) in zip(strips, moves)]
    e = call(center_kernel, EXT, [cotangent, speed, coeff, dirs], specs=[VMEM] * 4, name="center")
    e, y4, w4, up, down, moments = call(
        first_kernel,
        [EXT, FIELD, FIELD, STRIP, STRIP, ROWS],
        [edge, e, *received],
        aliases={1: 0},
        name="first",
    )
    low, high = along_x(up, down)
    nu4, y3, w3, up, down, moments = call(
        third_kernel,
        [FIELD, FIELD, FIELD, STRIP, STRIP, ROWS],
        [edge, e, y4, w4, low, high, reduced(moments)],
        scratch=SCRATCH * 2,
        name="third",
    )
    low, high = along_x(up, down)
    nu3, y2, w2, moments = call(
        second_kernel,
        [FIELD, FIELD, FIELD, ROWS],
        [edge, e, nu4, y3, w3, low, high, reduced(moments)],
        scratch=SCRATCH * 2,
        name="second",
    )
    return call(
        last_kernel, shape(NX, NY, NZ), [e, nu4, nu3, y2, w2, reduced(moments)], scratch=SCRATCH * 3, specs=[VMEM] * 6, name="last"
    )


def solution(mesh):
    placed = (P("gx", "gy", None), P(None, "gx", "gy", None), P(None, "gx", "gy", None), P(None, "gx", "gy"))
    return jax.shard_map(local, mesh=mesh, in_specs=placed, out_specs=P("gx", "gy", None), check_vma=False)
```

```python
import jax
import jax.numpy as jnp
from jax import lax
from jax.experimental import pallas as pl
from jax.experimental.pallas import tpu as pltpu
from jax.sharding import PartitionSpec as P


NX, NY, NZ = 32, 64, 128
H = 3
T = 8
EX, EY = NX + 2 * H, NY + 2 * T
TILES = EY // T
INNER = range(1, TILES - 1)
F32 = jnp.float32

C, K, U, K2B, U2B = 0, 1, 4, 7, 8
LOW = ((0, 3), (1, 3), (4, 3), (2, 2), (3, 2), (5, 2), (6, 2))
HIGH = ((0, 3), (1, 2), (4, 2), (2, 2), (3, 2), (5, 2), (6, 2))
NLOW = sum(n for _, n in LOW)
NHIGH = sum(n for _, n in HIGH)
YLOW = ((0, 7), (1, 6), (4, 6), (2, 7), (3, 6), (5, 7), (6, 6))
YHIGH = ((0, 7), (1, 6), (4, 6), (2, 6), (3, 6), (5, 6), (6, 6))
GROUP = 8
YROWS_LOW = GROUP * sum(n for _, n in YLOW)
YROWS_HIGH = GROUP * sum(n for _, n in YHIGH)
STEP = 9
CENTER_STEP = 8
THREE_STEP = 4
PAIRS = ((0, 0), (0, 1), (0, 2), (1, 1), (1, 2), (2, 2))
BLOCK_STEP = 8


def rows(t):
    return slice(t * T, (t + 1) * T)


class Masks:
    def __init__(self):
        lane = lax.broadcasted_iota(jnp.int32, (T, NZ), 1)
        row = lax.broadcasted_iota(jnp.int32, (T, NZ), 0)
        self.first, self.last, self.top = lane == 0, lane == NZ - 1, row == 0


def back(v):
    return pltpu.roll(v, 1, 1)


class Tiles:
    def __init__(self, ref, masks):
        self.ref, self.masks, self.seen = ref, masks, {}

    def at(self, x, i, t):
        key = (i, t)
        if key not in self.seen:
            self.seen[key] = self.ref[x + i, rows(t), :]
        return self.seen[key]

    def dx(self, x, i, t):
        return self.at(x, i + 1, t) - self.at(x, i, t)

    def dy(self, x, i, t):
        v = self.at(x, i, t)
        if t + 1 < TILES:
            return self.ref[x + i, t * T + 1 : (t + 1) * T + 1, :] - v
        return pltpu.roll(v, T - 1, 0) - v

    def dz(self, x, i, t):
        v = self.at(x, i, t)
        return jnp.where(self.masks.last, 0.0, pltpu.roll(v, NZ - 1, 1)) - v

    def dz_below(self, x, i, t):
        v = self.at(x, i, t)
        return v - back(v)


def sweep(x0, x1, step, body, carry):
    count = (x1 - x0) // step
    assert count * step == x1 - x0
    return lax.fori_loop(0, count, lambda n, c: body(x0 + n * step, c), carry)


def fluxes(x0, tiles, masks, parts, emit):
    def plane(x, low_x, i, fetch):
        new_low = []
        before = jnp.zeros((T, NZ), F32)
        if tiles[0] > 0:
            before = pltpu.roll(parts(fetch, 1, x, i, tiles[0] - 1)[1], 1, 0)
        for n, t in enumerate(tiles):
            up_x, down_x = parts(fetch, 0, x, i, t)
            up_y, down_y = parts(fetch, 1, x, i, t)
            up_z, down_z = parts(fetch, 2, x, i, t)
            rolled = pltpu.roll(down_y, 1, 0)
            down_y = jnp.where(masks.top, before, rolled)
            before = rolled
            total = (up_x - low_x[n]) + (up_y - down_y) + (up_z - down_z)
            new_low.append(down_x)
            emit(fetch, x, i, t, total)
        return new_low

    return plane


def run(x0, x1, step, tiles, masks, fetch_of, parts, emit):
    plane = fluxes(x0, tiles, masks, parts, emit)
    fetch = fetch_of()
    low = [parts(fetch, 0, x0 - 1, 0, t)[1] for t in tiles]

    def body(x, low):
        fetch = fetch_of()
        for i in range(step):
            low = plane(x, low, i, fetch)
        return low

    sweep(x0, x1, step, body, low)


def m_pass(e, v_ref, w_ref, masks):
    def parts(v, d, x, i, t):
        if d == 2:
            return e[K + 2, x + i, rows(t), :] * v.dz(x, i, t), e[K2B, x + i, rows(t), :] * v.dz_below(x, i, t)
        flux = e[K + d, x + i, rows(t), :] * (v.dx, v.dy)[d](x, i, t)
        return flux, flux

    def emit(v, x, i, t, total):
        w_ref[x + i, rows(t), :] = v.at(x, i, t) - total

    run(1, EX - 1, STEP, range(TILES), masks, lambda: Tiles(v_ref, masks), parts, emit)


def s_pass(e, y_ref, masks):
    cot = e.at[C]

    def parts(v, d, x, i, t):
        k, u = e[K + d, x + i, rows(t), :], e[U + d, x + i, rows(t), :]
        delta = (v.dx, v.dy, v.dz)[d](x, i, t)
        up = (k + jnp.maximum(u, 0.0)) * delta
        if d == 2:
            k, u = e[K2B, x + i, rows(t), :], e[U2B, x + i, rows(t), :]
            delta = v.dz_below(x, i, t)
        return up, (k - jnp.minimum(u, 0.0)) * delta

    def emit(v, x, i, t, total):
        y_ref[x + i, rows(t), :] = total

    run(1, EX - 1, STEP, range(TILES), masks, lambda: Tiles(cot, masks), parts, emit)


def fd_pass(e, a_ref, d_ref, put, x0, x1, step, tiles, masks):
    def parts(both, d, x, i, t):
        a, b = both
        k, u = e[K + d, x + i, rows(t), :], e[U + d, x + i, rows(t), :]
        da, db = ((v.dx, v.dy, v.dz)[d](x, i, t) for v in (a, b))
        flux = k * db
        up = flux + jnp.maximum(u, 0.0) * da
        if d == 2:
            u = e[U2B, x + i, rows(t), :]
            flux = e[K2B, x + i, rows(t), :] * b.dz_below(x, i, t)
            da = a.dz_below(x, i, t)
        return up, flux - jnp.minimum(u, 0.0) * da

    def emit(both, x, i, t, total):
        put(x + i, t, total)

    run(x0, x1, step, tiles, masks, lambda: (Tiles(a_ref, masks), Tiles(d_ref, masks)), parts, emit)


def products(e, y_ref, w_ref, masks):
    zero = jnp.zeros((T, NZ), F32)

    def body(x, accs):
        yy, yw, ww, *energy = accs
        w = Tiles(w_ref, masks)
        for i in range(BLOCK_STEP):
            for t in INNER:
                v, y = w.at(x, i, t), y_ref[x + i, rows(t), :]
                yy, yw, ww = yy + y * y, yw + y * v, ww + v * v
                for d, delta in enumerate((w.dx, w.dy, w.dz)):
                    difference = delta(x, i, t)
                    energy[d] = energy[d] + e[K + d, x + i, rows(t), :] * (difference * difference)
        return yy, yw, ww, *energy

    yy, yw, ww, *energy = sweep(H, H + NX, BLOCK_STEP, body, (zero,) * 6)
    return yy, yw, ww, ww + (energy[0] + energy[1] + energy[2])


def outside_is_zero(edge, ref):
    @pl.when(edge[0] == 0)
    def _():
        ref[H + NX : EX - 1] = jnp.zeros((H - 1, EY, NZ), F32)

    @pl.when(edge[1] == 0)
    def _():
        ref[:, EY - T :, :] = jnp.zeros((EX, T, NZ), F32)


def finish(edge, e, y, w, up, down, moments, masks):
    outside_is_zero(edge, y)
    m_pass(e, y, w, masks)
    outside_is_zero(edge, w)
    if up is not None:
        for n, ref in enumerate((y, w)):
            up[n * H : (n + 1) * H] = ref[NX : NX + H]
            down[n * H : (n + 1) * H] = ref[H : 2 * H]
    if moments is None:
        return
    write_sums(moments, products(e, y, w, masks))


def write_sums(moments, sums):
    lane = lax.broadcasted_iota(jnp.int32, (1, NZ), 1)
    row = jnp.zeros((1, NZ), F32)
    for i, acc in enumerate(sums):
        total = jnp.sum(jnp.sum(acc, axis=0, keepdims=True), axis=1, keepdims=True)
        row = jnp.where(lane // 4 == i, total, row)
    moments[...] = jnp.broadcast_to(row, moments.shape)


def read_sums(moments_ref, count):
    sums = jnp.sum(moments_ref[...], axis=0, keepdims=True)
    lane = lax.broadcasted_iota(jnp.int32, (1, NZ), 1)
    return [jnp.sum(jnp.where(lane == 4 * i, sums, 0.0), axis=1, keepdims=True) for i in range(count)]


def coefficients(m0, m1, m2, m3):
    alpha0 = m0 / m1
    rr = alpha0 * alpha0 * m2 - m0
    product = m1 - 2.0 * alpha0 * m2 + alpha0 * alpha0 * m3
    ratio = rr / m0
    alpha1 = rr / (product - ratio * rr / alpha0)
    a = alpha0 + alpha1 * (1.0 + ratio)
    b = -(alpha1 * alpha0)
    return a, b


def full(*scalars):
    return tuple(jnp.broadcast_to(v, (T, NZ)) for v in scalars)


def two_sections(moments_ref):
    sums = read_sums(moments_ref, 4 * len(PAIRS))
    grams = [dict(zip(PAIRS, sums[len(PAIRS) * k : len(PAIRS) * (k + 1)])) for k in range(4)]
    a, b = coefficients(*(g[0, 0] for g in grams))
    moments = [
        g[0, 0]
        + 2.0 * (a * g[0, 1] + b * g[0, 2])
        + (a * a * g[1, 1] + 2.0 * a * b * g[1, 2] + b * b * g[2, 2])
        for g in grams
    ]
    return full(a, b, *coefficients(*moments))


def signs(dirs, d, x, first_rows):
    sign = (1 - 2 * dirs[d, pl.ds(x, 1), :]).astype(F32)
    count = T * len(first_rows)
    row = lax.broadcasted_iota(jnp.int32, (count, NY), 0)
    column = lax.broadcasted_iota(jnp.int32, (count, NY), 1)
    at = row
    for n, first in enumerate(first_rows):
        at = jnp.where(row // T == n, row - n * T + first, at)
    picked = jnp.where(at == column, jnp.broadcast_to(sign, (count, NY)), 0.0)
    ones = jnp.ones((NY, NZ), jnp.bfloat16)
    return jnp.dot(picked.astype(jnp.bfloat16), ones, preferred_element_type=F32)


def pack_kernel(edge, cot, speed, coeff, all_dirs, low, high, ylow, yhigh, cll, clh, chl, chh, dirs, tops, bottoms, sems):
    bottom, top, full = slice(0, T), slice(NY - T, NY), slice(0, NY)
    copies = [pltpu.make_async_copy(all_dirs, dirs, sems.at[0])]
    copies[0].start()

    def fetch(f, planes, rows, target):
        source = cot.at[planes, rows] if f == 0 else (coeff if f < 4 else speed).at[(f - 1) % 3, planes, rows]
        copy = pltpu.make_async_copy(source, target, sems.at[len(copies)])
        copy.start()
        copies.append(copy)

    for f in range(7):
        fetch(f, slice(0, NX), top, tops.at[f])
        fetch(f, slice(0, NX), bottom, bottoms.at[f])
    signed = []
    for fields, strip in ((LOW, low), (HIGH, high)):
        at = 0
        for f, n in fields:
            start = NX - n if fields is LOW else 0
            fetch(f, slice(start, start + n), full, strip.at[at : at + n])
            if f >= 4:
                signed += [(strip, at + i, f - 4, start + i) for i in range(n)]
            at += n
    for copy in copies:
        copy.wait()
    for group in range(NX // GROUP):
        at_low = at_high = 0
        for x in range(group * GROUP, (group + 1) * GROUP):
            sign = [signs(dirs, d, x, (NY - T, 0)) for d in range(3)]
            for (f, n), (_, m) in zip(YLOW, YHIGH):
                upper, lower = tops[f, x], bottoms[f, x]
                if f >= 4:
                    upper, lower = upper * sign[f - 4][:T], lower * sign[f - 4][T:]
                ylow[group, at_low : at_low + n, :] = upper[T - n :]
                yhigh[group, at_high : at_high + m, :] = lower[:m]
                at_low += n
                at_high += m
    for strip, at, d, x in signed:
        strip[at] = strip[at] * signs(dirs, d, x, tuple(range(0, NY, T)))
    cll[...] = low[:, top, :]
    clh[...] = low[:, bottom, :]
    chl[...] = high[:, top, :]
    chh[...] = high[:, bottom, :]


def place(e, f, x, rows, value):
    if f > 0:
        value = 0.25 * value
    e[f, x, rows, :] = value
    if f in (K + 2, U + 2):
        first = lax.broadcasted_iota(jnp.int32, value.shape, 1) == 0
        e[K2B if f == K + 2 else U2B, x, rows, :] = jnp.where(first, 0.0, back(value))


def shifted_tile(ref, group, start):
    inside = min(max(start, 0), ref.shape[1] - T)
    value = ref[group, inside : inside + T, :]
    return value if inside == start else pltpu.roll(value, (inside - start) % T, 0)


def center_kernel(cot, speed, coeff, dirs, e):
    every = tuple(range(0, NY, T))
    middle = slice(T, T + NY)

    def body(n, _):
        for i in range(CENTER_STEP):
            x = CENTER_STEP * n + i
            place(e, C, H + x, middle, cot[x])
            for d in range(3):
                place(e, K + d, H + x, middle, coeff[d, x])
                place(e, U + d, H + x, middle, speed[d, x] * signs(dirs, d, x, every))
        return _

    lax.fori_loop(0, NX // CENTER_STEP, body, 0)


def first_kernel(edge, e_in, low, high, ylow, yhigh, cll, clh, chl, chh, e, y, w, up, down):
    masks = Masks()
    middle, below, above = slice(T, T + NY), slice(0, T), slice(T + NY, EY)
    for fields, base, middles, lows, highs in (
        (LOW, None, low, cll, clh),
        (HIGH, H + NX, high, chl, chh),
    ):
        at = 0
        for f, n in fields:
            for i in range(n):
                x = (H - n if base is None else base) + i
                place(e, f, x, middle, middles[at + i])
                place(e, f, x, below, lows[at + i])
                place(e, f, x, above, highs[at + i])
            at += n

    def body(group, _):
        at_low = at_high = 0
        for i in range(GROUP):
            x = H + group * GROUP + i
            for (f, n), (_, m) in zip(YLOW, YHIGH):
                place(e, f, x, below, shifted_tile(ylow, group, at_low + n - T))
                place(e, f, x, above, shifted_tile(yhigh, group, at_high))
                at_low += n
                at_high += m
        return _

    lax.fori_loop(0, NX // GROUP, body, 0)
    s_pass(e, y, masks)
    finish(edge, e, y, w, up, down, None, masks)


def combine(x0, x1, emit):
    def body(x, _):
        for t in range(TILES):
            emit(x, t)
        return _

    lax.fori_loop(x0, x1, body, 0)


def parts_pass(e, y_ref, w_ref, p1, p2, x0, x1, step, masks):
    zero = jnp.zeros((T, NZ), F32)
    tiles = range(TILES)

    def faces(both, d, x, i, t):
        y, w = both
        k, u = e[K + d, x + i, rows(t), :], e[U + d, x + i, rows(t), :]
        dy, dw = ((v.dx, v.dy, v.dz)[d](x, i, t) for v in both)
        ahead = 2.0 * jnp.maximum(u, 0.0)
        flux = k * dw
        up = (ahead * dy, ahead * dw + flux)
        if d == 2:
            k, u = e[K2B, x + i, rows(t), :], e[U2B, x + i, rows(t), :]
            dy, dw = y.dz_below(x, i, t), w.dz_below(x, i, t)
            flux = k * dw
        behind = 2.0 * jnp.minimum(u, 0.0)
        return up, (behind * dy, behind * dw - flux)

    first = (Tiles(y_ref, masks), Tiles(w_ref, masks))
    low_x = [faces(first, 0, x0 - 1, 0, t)[1] for t in tiles]

    def body(x, low_x):
        both = (Tiles(y_ref, masks), Tiles(w_ref, masks))
        for i in range(step):
            before = (zero, zero)
            next_low = []
            for t in tiles:
                (x_up, x_low), (y_up, y_low), (z_up, z_low) = (faces(both, d, x, i, t) for d in range(3))
                next_low.append(x_low)
                rolled = tuple(pltpu.roll(v, 1, 0) for v in y_low)
                y_below = [jnp.where(masks.top, old, new) for old, new in zip(before, rolled)]
                before = rolled
                totals = [
                    (x_up[j] + low_x[t][j]) + (y_up[j] + y_below[j]) + (z_up[j] + z_low[j]) for j in range(2)
                ]
                p1[x + i, rows(t), :] = totals[0] + (both[0].at(x, i, t) - both[1].at(x, i, t))
                p2[x + i, rows(t), :] = totals[1]
            low_x = next_low
        return low_x

    sweep(x0, x1, step, body, low_x)


def products_of_three(e, fields, images, masks):
    zero = jnp.zeros((T, NZ), F32)
    count = len(PAIRS)

    def body(x, accs):
        accs = list(accs)
        readers = [Tiles(ref, masks) for ref in images]
        for i in range(THREE_STEP):
            for t in INNER:
                q = [ref[x + i, rows(t), :] for ref in fields]
                m = [v.at(x, i, t) for v in readers]
                for n, (j, k) in enumerate(PAIRS):
                    accs[n] = accs[n] + q[j] * q[k]
                    accs[count + n] = accs[count + n] + q[j] * m[k]
                    accs[2 * count + n] = accs[2 * count + n] + m[j] * m[k]
                for d in range(3):
                    delta = [(v.dx, v.dy, v.dz)[d](x, i, t) for v in readers]
                    scaled = [e[K + d, x + i, rows(t), :] * v for v in delta]
                    for n, (j, k) in enumerate(PAIRS):
                        accs[3 * count + n] = accs[3 * count + n] + scaled[j] * delta[k]
        return tuple(accs)

    accs = sweep(H, H + NX, THREE_STEP, body, (zero,) * (4 * count))
    return accs[: 3 * count] + tuple(accs[3 * count + n] + accs[2 * count + n] for n in range(count))


def basis_kernel(edge, e, y, w, low, high, y4, w4, p1, p2, m1, m2, up, down, moments):
    masks = Masks()

    def body(n, _):
        for i in range(4):
            y4[H + 4 * n + i] = y[H + 4 * n + i]
            w4[H + 4 * n + i] = w[H + 4 * n + i]
        return _

    lax.fori_loop(0, NX // 4, body, 0)
    for base, strip in ((0, low), (H + NX, high)):
        y4[base : base + H] = strip[0:H]
        w4[base : base + H] = strip[H:]
    parts_pass(e, y4, w4, p1, p2, 1, EX - 1, STEP, masks)
    for p, m in ((p1, m1), (p2, m2)):
        outside_is_zero(edge, p)
        m_pass(e, p, m, masks)
        outside_is_zero(edge, m)
    for n, ref in enumerate((p1, p2, m1, m2)):
        up[n * H : (n + 1) * H] = ref[NX : NX + H]
        down[n * H : (n + 1) * H] = ref[H : 2 * H]
    write_sums(moments, products_of_three(e, (y4, p1, p2), (w4, m1, m2), masks))


def second_kernel(edge, e, y4, w4, p1, p2, m1, m2, low, high, sums, nu4, nu3, y, w, moments, adv, dif):
    masks = Masks()
    a4, b4, a3, b3 = two_sections(sums)

    def emit(x, t, parts):
        v, m = y4[x, rows(t), :], w4[x, rows(t), :]
        q1, q2, n1, n2 = parts
        c = 1.4 * e[C, x, rows(t), :]
        four = a4 * v + b4 * m
        three = a3 * (v + a4 * q1 + b4 * q2) + b3 * (m + a4 * n1 + b4 * n2)
        nu4[x, rows(t), :] = four
        nu3[x, rows(t), :] = three
        adv[x, rows(t), :] = c + 1.2 * four + 2.0 * three
        dif[x, rows(t), :] = c + 1.4 * four + three

    combine(H, H + NX, lambda x, t: emit(x, t, [ref[x, rows(t), :] for ref in (p1, p2, m1, m2)]))
    for base, strip in ((0, low), (H + NX, high)):
        for i in range(H):
            for t in range(TILES):
                emit(base + i, t, [strip[n * H + i, rows(t), :] for n in range(4)])

    def put(x, t, value):
        y[x, rows(t), :] = value

    fd_pass(e, adv, dif, put, 1, EX - 1, STEP, range(TILES), masks)
    finish(edge, e, y, w, None, None, moments, masks)


def last_kernel(e, nu4, nu3, y2, w2, sums, out, adv, dif, base):
    masks = Masks()
    a, b = full(*coefficients(*read_sums(sums, 4)))

    def emit(x, t):
        nu = a * y2[x, rows(t), :] + b * w2[x, rows(t), :]
        cot = e[C, x, rows(t), :]
        four, three = nu4[x, rows(t), :], nu3[x, rows(t), :]
        adv[x, rows(t), :] = 0.6 * cot + 0.8 * four + three + 2.0 * nu
        dif[x, rows(t), :] = 0.6 * (cot + four) + three + nu
        base[x, rows(t), :] = cot + four + three + nu

    combine(H - 1, H + NX + 1, emit)

    def put(x, t, value):
        out[x - H, rows(t - 1), :] = base[x, rows(t), :] + value

    fd_pass(e, adv, dif, put, H, H + NX, BLOCK_STEP, INNER, masks)


def shape(*dims):
    return jax.ShapeDtypeStruct(dims, F32)


FIELD = shape(EX, EY, NZ)
EXT = shape(9, EX, EY, NZ)
SCRATCH = [pltpu.VMEM((EX, EY, NZ), F32)]
STRIP = shape(2 * H, EY, NZ)
STRIPS = shape(4 * H, EY, NZ)
ROWS = shape(128, NZ)
VMEM = pl.BlockSpec(memory_space=pltpu.VMEM)
SMEM = pl.BlockSpec(memory_space=pltpu.SMEM)
HBM = pl.BlockSpec(memory_space=pltpu.HBM)
LIMIT = 8 * 1024 * 1024


def call(kernel, outs, ins, scratch=(), name=None, specs=None, sems=0, aliases=None):
    return pl.pallas_call(
        kernel,
        out_shape=outs,
        in_specs=specs or [SMEM] + [VMEM] * (len(ins) - 1),
        out_specs=jax.tree.map(lambda _: VMEM, outs),
        scratch_shapes=list(scratch) + ([pltpu.SemaphoreType.DMA((sems,))] if sems else []),
        input_output_aliases=aliases or {},
        compiler_params=pltpu.CompilerParams(vmem_limit_bytes=LIMIT),
        name=name,
    )(*ins)


def local(cotangent, speed, coeff, dirs):
    nx, ny = lax.axis_size("gx"), lax.axis_size("gy")
    ix, iy = lax.axis_index("gx"), lax.axis_index("gy")
    hbm = [pltpu.with_memory_space_constraint(v, pltpu.HBM) for v in (cotangent, speed, coeff, dirs)]
    edge = jnp.stack([(ix < nx - 1).astype(jnp.int32), (iy < ny - 1).astype(jnp.int32)])

    strips = call(
        pack_kernel,
        [shape(NLOW, NY, NZ), shape(NHIGH, NY, NZ), shape(NX // GROUP, YROWS_LOW, NZ), shape(NX // GROUP, YROWS_HIGH, NZ)]
        + [shape(NLOW, T, NZ)] * 2 + [shape(NHIGH, T, NZ)] * 2,
        [edge, *hbm],
        specs=[SMEM] + [HBM] * 4,
        scratch=[pltpu.VMEM((3, NX, NY), jnp.int32)] + [pltpu.VMEM((7, NX, T, NZ), F32)] * 2,
        sems=29,
        name="pack",
    )

    def shifted(value, dx, dy):
        perm = []
        for i in range(nx):
            for j in range(ny):
                if 0 <= i + dx < nx and 0 <= j + dy < ny:
                    perm.append((i * ny + j, (i + dx) * ny + j + dy))
        return lax.ppermute(value, ("gx", "gy"), perm)

    def along_x(up, down):
        return shifted(up, 1, 0), shifted(down, -1, 0)

    def reduced(moments):
        return lax.all_to_all(moments, ("gx", "gy"), 0, 0, tiled=True)

    moves = ((1, 0), (-1, 0), (0, 1), (0, -1), (1, 1), (1, -1), (-1, 1), (-1, -1))
    received = [shifted(s, dx, dy) for s, (dx, dy) in zip(strips, moves)]
    e = call(center_kernel, EXT, [cotangent, speed, coeff, dirs], specs=[VMEM] * 4, name="center")
    e, y, w, up, down = call(
        first_kernel, [EXT, FIELD, FIELD, STRIP, STRIP], [edge, e, *received], aliases={1: 0}, name="first"
    )
    *basis, up, down, moments = call(
        basis_kernel,
        [FIELD] * 6 + [STRIPS, STRIPS, ROWS],
        [edge, e, y, w, *along_x(up, down)],
        name="basis",
    )
    low, high = along_x(up, down)
    nu4, nu3, y2, w2, moments = call(
        second_kernel,
        [FIELD] * 4 + [ROWS],
        [edge, e, *basis, low, high, reduced(moments)],
        scratch=SCRATCH * 2,
        name="second",
    )
    return call(
        last_kernel, shape(NX, NY, NZ), [e, nu4, nu3, y2, w2, reduced(moments)], scratch=SCRATCH * 3, specs=[VMEM] * 6, name="last"
    )


def solution(mesh):
    placed = (P("gx", "gy", None), P(None, "gx", "gy", None), P(None, "gx", "gy", None), P(None, "gx", "gy"))
    return jax.shard_map(local, mesh=mesh, in_specs=placed, out_specs=P("gx", "gy", None), check_vma=False)
```

```python
import jax
import jax.numpy as jnp
from jax import lax
from jax.experimental import pallas as pl
from jax.experimental.pallas import tpu as pltpu
from jax.sharding import PartitionSpec as P


NX, NY, NZ = 32, 64, 128
H = 3
T = 8
EX, EY = NX + 2 * H, NY + 2 * T
TILES = EY // T
INNER = range(1, TILES - 1)
F32 = jnp.float32

C, K, U, K2B, U2B = 0, 1, 4, 7, 8
LOW = ((0, 3), (1, 3), (4, 3), (2, 2), (3, 2), (5, 2), (6, 2))
HIGH = ((0, 3), (1, 2), (4, 2), (2, 2), (3, 2), (5, 2), (6, 2))
NLOW = sum(n for _, n in LOW)
NHIGH = sum(n for _, n in HIGH)
YLOW = ((0, 7), (1, 6), (4, 6), (2, 7), (3, 6), (5, 7), (6, 6))
YHIGH = ((0, 7), (1, 6), (4, 6), (2, 6), (3, 6), (5, 6), (6, 6))
GROUP = 8
YROWS_LOW = GROUP * sum(n for _, n in YLOW)
YROWS_HIGH = GROUP * sum(n for _, n in YHIGH)
STEP = 9
CENTER_STEP = 8
THREE_STEP = 4
A0, B0 = 0.6, -0.083
PAIRS = ((0, 0), (0, 1), (0, 2), (1, 1), (1, 2), (2, 2))
BLOCK_STEP = 8


def rows(t):
    return slice(t * T, (t + 1) * T)


class Masks:
    def __init__(self):
        lane = lax.broadcasted_iota(jnp.int32, (T, NZ), 1)
        row = lax.broadcasted_iota(jnp.int32, (T, NZ), 0)
        self.first, self.last, self.top = lane == 0, lane == NZ - 1, row == 0


def back(v):
    return pltpu.roll(v, 1, 1)


class Tiles:
    def __init__(self, ref, masks):
        self.ref, self.masks, self.seen = ref, masks, {}

    def at(self, x, i, t):
        key = (i, t)
        if key not in self.seen:
            self.seen[key] = self.ref[x + i, rows(t), :]
        return self.seen[key]

    def dx(self, x, i, t):
        return self.at(x, i + 1, t) - self.at(x, i, t)

    def dy(self, x, i, t):
        v = self.at(x, i, t)
        if t + 1 < TILES:
            return self.ref[x + i, t * T + 1 : (t + 1) * T + 1, :] - v
        return pltpu.roll(v, T - 1, 0) - v

    def dz(self, x, i, t):
        v = self.at(x, i, t)
        return jnp.where(self.masks.last, 0.0, pltpu.roll(v, NZ - 1, 1)) - v

    def dz_below(self, x, i, t):
        v = self.at(x, i, t)
        return v - back(v)


def sweep(x0, x1, step, body, carry):
    count = (x1 - x0) // step
    assert count * step == x1 - x0
    return lax.fori_loop(0, count, lambda n, c: body(x0 + n * step, c), carry)


def fluxes(x0, tiles, masks, parts, emit):
    def plane(x, low_x, i, fetch):
        new_low = []
        before = jnp.zeros((T, NZ), F32)
        if tiles[0] > 0:
            before = pltpu.roll(parts(fetch, 1, x, i, tiles[0] - 1)[1], 1, 0)
        for n, t in enumerate(tiles):
            up_x, down_x = parts(fetch, 0, x, i, t)
            up_y, down_y = parts(fetch, 1, x, i, t)
            up_z, down_z = parts(fetch, 2, x, i, t)
            rolled = pltpu.roll(down_y, 1, 0)
            down_y = jnp.where(masks.top, before, rolled)
            before = rolled
            total = (up_x - low_x[n]) + (up_y - down_y) + (up_z - down_z)
            new_low.append(down_x)
            emit(fetch, x, i, t, total)
        return new_low

    return plane


def run(x0, x1, step, tiles, masks, fetch_of, parts, emit):
    plane = fluxes(x0, tiles, masks, parts, emit)
    fetch = fetch_of()
    low = [parts(fetch, 0, x0 - 1, 0, t)[1] for t in tiles]

    def body(x, low):
        fetch = fetch_of()
        for i in range(step):
            low = plane(x, low, i, fetch)
        return low

    sweep(x0, x1, step, body, low)


def m_pass(e, v_ref, w_ref, masks, x0=1, x1=NX + 2 * H - 1, step=None):
    def parts(v, d, x, i, t):
        if d == 2:
            return e[K + 2, x + i, rows(t), :] * v.dz(x, i, t), e[K2B, x + i, rows(t), :] * v.dz_below(x, i, t)
        flux = e[K + d, x + i, rows(t), :] * (v.dx, v.dy)[d](x, i, t)
        return flux, flux

    def emit(v, x, i, t, total):
        w_ref[x + i, rows(t), :] = v.at(x, i, t) - total

    run(x0, x1, step or STEP, range(TILES), masks, lambda: Tiles(v_ref, masks), parts, emit)


def s_pass(e, y_ref, masks):
    cot = e.at[C]

    def parts(v, d, x, i, t):
        k, u = e[K + d, x + i, rows(t), :], e[U + d, x + i, rows(t), :]
        delta = (v.dx, v.dy, v.dz)[d](x, i, t)
        up = (k + jnp.maximum(u, 0.0)) * delta
        if d == 2:
            k, u = e[K2B, x + i, rows(t), :], e[U2B, x + i, rows(t), :]
            delta = v.dz_below(x, i, t)
        return up, (k - jnp.minimum(u, 0.0)) * delta

    def emit(v, x, i, t, total):
        y_ref[x + i, rows(t), :] = total

    run(1, EX - 1, STEP, range(TILES), masks, lambda: Tiles(cot, masks), parts, emit)


def fd_pass(e, a_ref, d_ref, put, x0, x1, step, tiles, masks):
    def parts(both, d, x, i, t):
        a, b = both
        k, u = e[K + d, x + i, rows(t), :], e[U + d, x + i, rows(t), :]
        da, db = ((v.dx, v.dy, v.dz)[d](x, i, t) for v in (a, b))
        flux = k * db
        up = flux + jnp.maximum(u, 0.0) * da
        if d == 2:
            u = e[U2B, x + i, rows(t), :]
            flux = e[K2B, x + i, rows(t), :] * b.dz_below(x, i, t)
            da = a.dz_below(x, i, t)
        return up, flux - jnp.minimum(u, 0.0) * da

    def emit(both, x, i, t, total):
        put(x + i, t, total)

    run(x0, x1, step, tiles, masks, lambda: (Tiles(a_ref, masks), Tiles(d_ref, masks)), parts, emit)


def products(e, y_ref, w_ref, masks):
    zero = jnp.zeros((T, NZ), F32)

    def body(x, accs):
        yy, yw, ww, *energy = accs
        w = Tiles(w_ref, masks)
        for i in range(BLOCK_STEP):
            for t in INNER:
                v, y = w.at(x, i, t), y_ref[x + i, rows(t), :]
                yy, yw, ww = yy + y * y, yw + y * v, ww + v * v
                for d, delta in enumerate((w.dx, w.dy, w.dz)):
                    difference = delta(x, i, t)
                    energy[d] = energy[d] + e[K + d, x + i, rows(t), :] * (difference * difference)
        return yy, yw, ww, *energy

    yy, yw, ww, *energy = sweep(H, H + NX, BLOCK_STEP, body, (zero,) * 6)
    return yy, yw, ww, ww + (energy[0] + energy[1] + energy[2])


def outside_is_zero(edge, ref):
    @pl.when(edge[0] == 0)
    def _():
        ref[H + NX : EX - 1] = jnp.zeros((H - 1, EY, NZ), F32)

    @pl.when(edge[1] == 0)
    def _():
        ref[:, EY - T :, :] = jnp.zeros((EX, T, NZ), F32)


def finish(edge, e, y, w, up, down, moments, masks):
    outside_is_zero(edge, y)
    m_pass(e, y, w, masks)
    outside_is_zero(edge, w)
    if up is not None:
        for n, ref in enumerate((y, w)):
            up[n * H : (n + 1) * H] = ref[NX : NX + H]
            down[n * H : (n + 1) * H] = ref[H : 2 * H]
    if moments is None:
        return
    write_sums(moments, products(e, y, w, masks))


def write_sums(moments, sums):
    lane = lax.broadcasted_iota(jnp.int32, (1, NZ), 1)
    row = jnp.zeros((1, NZ), F32)
    for i, acc in enumerate(sums):
        total = jnp.sum(jnp.sum(acc, axis=0, keepdims=True), axis=1, keepdims=True)
        row = jnp.where(lane // 4 == i, total, row)
    moments[...] = jnp.broadcast_to(row, moments.shape)


def read_sums(moments_ref, count):
    sums = jnp.sum(moments_ref[...], axis=0, keepdims=True)
    lane = lax.broadcasted_iota(jnp.int32, (1, NZ), 1)
    return [jnp.sum(jnp.where(lane == 4 * i, sums, 0.0), axis=1, keepdims=True) for i in range(count)]


def coefficients(m0, m1, m2, m3):
    alpha0 = m0 / m1
    rr = alpha0 * alpha0 * m2 - m0
    product = m1 - 2.0 * alpha0 * m2 + alpha0 * alpha0 * m3
    ratio = rr / m0
    alpha1 = rr / (product - ratio * rr / alpha0)
    a = alpha0 + alpha1 * (1.0 + ratio)
    b = -(alpha1 * alpha0)
    return a, b


def full(*scalars):
    return tuple(jnp.broadcast_to(v, (T, NZ)) for v in scalars)


def two_sections(moments_ref):
    sums = read_sums(moments_ref, 4 * len(PAIRS))
    grams = [dict(zip(PAIRS, sums[len(PAIRS) * k : len(PAIRS) * (k + 1)])) for k in range(4)]

    def moments(a, b):
        return [
            g[0, 0]
            + 2.0 * (a * g[0, 1] + b * g[0, 2])
            + (a * a * g[1, 1] + 2.0 * a * b * g[1, 2] + b * b * g[2, 2])
            for g in grams
        ]

    a, b = coefficients(*moments(-A0, -B0))
    return full(a, b, *coefficients(*moments(a - A0, b - B0)))


def signs(dirs, d, x, first_rows):
    sign = (1 - 2 * dirs[d, pl.ds(x, 1), :]).astype(F32)
    count = T * len(first_rows)
    row = lax.broadcasted_iota(jnp.int32, (count, NY), 0)
    column = lax.broadcasted_iota(jnp.int32, (count, NY), 1)
    at = row
    for n, first in enumerate(first_rows):
        at = jnp.where(row // T == n, row - n * T + first, at)
    picked = jnp.where(at == column, jnp.broadcast_to(sign, (count, NY)), 0.0)
    ones = jnp.ones((NY, NZ), jnp.bfloat16)
    return jnp.dot(picked.astype(jnp.bfloat16), ones, preferred_element_type=F32)


def pack_kernel(edge, cot, speed, coeff, all_dirs, low, high, ylow, yhigh, cll, clh, chl, chh, dirs, tops, bottoms, sems):
    bottom, top, full = slice(0, T), slice(NY - T, NY), slice(0, NY)
    copies = [pltpu.make_async_copy(all_dirs, dirs, sems.at[0])]
    copies[0].start()

    def fetch(f, planes, rows, target):
        source = cot.at[planes, rows] if f == 0 else (coeff if f < 4 else speed).at[(f - 1) % 3, planes, rows]
        copy = pltpu.make_async_copy(source, target, sems.at[len(copies)])
        copy.start()
        copies.append(copy)

    for f in range(7):
        fetch(f, slice(0, NX), top, tops.at[f])
        fetch(f, slice(0, NX), bottom, bottoms.at[f])
    signed = []
    for fields, strip in ((LOW, low), (HIGH, high)):
        at = 0
        for f, n in fields:
            start = NX - n if fields is LOW else 0
            fetch(f, slice(start, start + n), full, strip.at[at : at + n])
            if f >= 4:
                signed += [(strip, at + i, f - 4, start + i) for i in range(n)]
            at += n
    for copy in copies:
        copy.wait()
    for group in range(NX // GROUP):
        at_low = at_high = 0
        for x in range(group * GROUP, (group + 1) * GROUP):
            sign = [signs(dirs, d, x, (NY - T, 0)) for d in range(3)]
            for (f, n), (_, m) in zip(YLOW, YHIGH):
                upper, lower = tops[f, x], bottoms[f, x]
                if f >= 4:
                    upper, lower = upper * sign[f - 4][:T], lower * sign[f - 4][T:]
                ylow[group, at_low : at_low + n, :] = upper[T - n :]
                yhigh[group, at_high : at_high + m, :] = lower[:m]
                at_low += n
                at_high += m
    for strip, at, d, x in signed:
        strip[at] = strip[at] * signs(dirs, d, x, tuple(range(0, NY, T)))
    cll[...] = low[:, top, :]
    clh[...] = low[:, bottom, :]
    chl[...] = high[:, top, :]
    chh[...] = high[:, bottom, :]


def place(e, f, x, rows, value):
    if f > 0:
        value = 0.25 * value
    e[f, x, rows, :] = value
    if f in (K + 2, U + 2):
        first = lax.broadcasted_iota(jnp.int32, value.shape, 1) == 0
        e[K2B if f == K + 2 else U2B, x, rows, :] = jnp.where(first, 0.0, back(value))


def shifted_tile(ref, group, start):
    inside = min(max(start, 0), ref.shape[1] - T)
    value = ref[group, inside : inside + T, :]
    return value if inside == start else pltpu.roll(value, (inside - start) % T, 0)


def center_kernel(cot, speed, coeff, dirs, e):
    every = tuple(range(0, NY, T))
    middle = slice(T, T + NY)

    def body(n, _):
        for i in range(CENTER_STEP):
            x = CENTER_STEP * n + i
            place(e, C, H + x, middle, cot[x])
            for d in range(3):
                place(e, K + d, H + x, middle, coeff[d, x])
                place(e, U + d, H + x, middle, speed[d, x] * signs(dirs, d, x, every))
        return _

    lax.fori_loop(0, NX // CENTER_STEP, body, 0)


def first_kernel(edge, e_in, low, high, ylow, yhigh, cll, clh, chl, chh, e, y, w, up, down):
    masks = Masks()
    middle, below, above = slice(T, T + NY), slice(0, T), slice(T + NY, EY)
    for fields, base, middles, lows, highs in (
        (LOW, None, low, cll, clh),
        (HIGH, H + NX, high, chl, chh),
    ):
        at = 0
        for f, n in fields:
            for i in range(n):
                x = (H - n if base is None else base) + i
                place(e, f, x, middle, middles[at + i])
                place(e, f, x, below, lows[at + i])
                place(e, f, x, above, highs[at + i])
            at += n

    def body(group, _):
        at_low = at_high = 0
        for i in range(GROUP):
            x = H + group * GROUP + i
            for (f, n), (_, m) in zip(YLOW, YHIGH):
                place(e, f, x, below, shifted_tile(ylow, group, at_low + n - T))
                place(e, f, x, above, shifted_tile(yhigh, group, at_high))
                at_low += n
                at_high += m
        return _

    lax.fori_loop(0, NX // GROUP, body, 0)
    s_pass(e, y, masks)
    finish(edge, e, y, w, up, down, None, masks)


def combine(x0, x1, emit, tiles=range(TILES)):
    def body(n, _):
        for i in range(2):
            for t in tiles:
                emit(x0 + 2 * n + i, t)
        return _

    lax.fori_loop(0, (x1 - x0) // 2, body, 0)


def parts_pass(e, y_ref, w_ref, p1, p2, x0, x1, step, masks):
    zero = jnp.zeros((T, NZ), F32)
    tiles = range(TILES)

    def faces(both, d, x, i, t):
        y, w = both
        k, u = e[K + d, x + i, rows(t), :], e[U + d, x + i, rows(t), :]
        dy, dw = ((v.dx, v.dy, v.dz)[d](x, i, t) for v in both)
        ahead = 2.0 * jnp.maximum(u, 0.0)
        flux = k * dw
        up = (ahead * dy, ahead * dw + flux)
        if d == 2:
            k, u = e[K2B, x + i, rows(t), :], e[U2B, x + i, rows(t), :]
            dy, dw = y.dz_below(x, i, t), w.dz_below(x, i, t)
            flux = k * dw
        behind = 2.0 * jnp.minimum(u, 0.0)
        return up, (behind * dy, behind * dw - flux)

    first = (Tiles(y_ref, masks), Tiles(w_ref, masks))
    low_x = [faces(first, 0, x0 - 1, 0, t)[1] for t in tiles]

    def body(x, low_x):
        both = (Tiles(y_ref, masks), Tiles(w_ref, masks))
        for i in range(step):
            before = (zero, zero)
            next_low = []
            for t in tiles:
                (x_up, x_low), (y_up, y_low), (z_up, z_low) = (faces(both, d, x, i, t) for d in range(3))
                next_low.append(x_low)
                rolled = tuple(pltpu.roll(v, 1, 0) for v in y_low)
                y_below = [jnp.where(masks.top, old, new) for old, new in zip(before, rolled)]
                before = rolled
                totals = [
                    (x_up[j] + low_x[t][j]) + (y_up[j] + y_below[j]) + (z_up[j] + z_low[j]) for j in range(2)
                ]
                p1[x + i, rows(t), :] = totals[0] + (both[0].at(x, i, t) - both[1].at(x, i, t))
                p2[x + i, rows(t), :] = totals[1]
            low_x = next_low
        return low_x

    sweep(x0, x1, step, body, low_x)


def products_of_three(e, fields, images, masks):
    zero = jnp.zeros((T, NZ), F32)
    count = len(PAIRS)

    def body(x, accs):
        accs = list(accs)
        readers = [Tiles(ref, masks) for ref in images]
        for i in range(THREE_STEP):
            for t in INNER:
                q = [ref[x + i, rows(t), :] for ref in fields]
                m = [v.at(x, i, t) for v in readers]
                for n, (j, k) in enumerate(PAIRS):
                    accs[n] = accs[n] + q[j] * q[k]
                    accs[count + n] = accs[count + n] + q[j] * m[k]
                    accs[2 * count + n] = accs[2 * count + n] + m[j] * m[k]
                for d in range(3):
                    delta = [(v.dx, v.dy, v.dz)[d](x, i, t) for v in readers]
                    scaled = [e[K + d, x + i, rows(t), :] * v for v in delta]
                    for n, (j, k) in enumerate(PAIRS):
                        accs[3 * count + n] = accs[3 * count + n] + scaled[j] * delta[k]
        return tuple(accs)

    accs = sweep(H, H + NX, THREE_STEP, body, (zero,) * (4 * count))
    return accs[: 3 * count] + tuple(accs[3 * count + n] + accs[2 * count + n] for n in range(count))


def inner_kernel(edge, e, y, w, p1, p2, m1, m2):
    masks = Masks()
    parts_pass(e, y, w, p1, p2, H + 1, H + NX - 1, 10, masks)
    for p, m in ((p1, m1), (p2, m2)):
        outside_is_zero(edge, p)
        m_pass(e, p, m, masks, H + 2, H + NX - 2, 7)


def basis_kernel(
    edge, e, y_in, w_in, p1_in, p2_in, m1_in, m2_in, low, high, y4, w4, p1, p2, m1, m2, up, down, moments, q0, n0
):
    masks = Masks()
    for base, strip in ((0, low), (H + NX, high)):
        y4[base : base + H] = strip[0:H]
        w4[base : base + H] = strip[H:]
    for x0 in (1, H + NX - 1):
        parts_pass(e, y4, w4, p1, p2, x0, x0 + H, H, masks)
    for p, m in ((p1, m1), (p2, m2)):
        outside_is_zero(edge, p)
        m_pass(e, p, m, masks, H, H + 2, 2)
        m_pass(e, p, m, masks, H + NX - 2, H + NX + 1, 3)
        outside_is_zero(edge, m)
    for n, ref in enumerate((p1, p2, m1, m2)):
        up[n * H : (n + 1) * H] = ref[NX : NX + H]
        down[n * H : (n + 1) * H] = ref[H : 2 * H]

    def emit(x, t):
        at = (x, rows(t))
        q0[at] = y4[at] + A0 * p1[at] + B0 * p2[at]
        n0[at] = w4[at] + A0 * m1[at] + B0 * m2[at]

    combine(H, H + NX + 2, emit, range(1, TILES))
    write_sums(moments, products_of_three(e, (q0, p1, p2), (n0, m1, m2), masks))


def second_kernel(edge, e, y4, w4, p1, p2, m1, m2, low, high, sums, nu4, nu3, y, w, moments, adv, dif):
    masks = Masks()
    a4, b4, a3, b3 = two_sections(sums)

    def emit(x, t, parts):
        v, m = y4[x, rows(t), :], w4[x, rows(t), :]
        q1, q2, n1, n2 = parts
        c = 1.4 * e[C, x, rows(t), :]
        four = a4 * v + b4 * m
        three = a3 * (v + a4 * q1 + b4 * q2) + b3 * (m + a4 * n1 + b4 * n2)
        nu4[x, rows(t), :] = four
        nu3[x, rows(t), :] = three
        adv[x, rows(t), :] = c + 1.2 * four + 2.0 * three
        dif[x, rows(t), :] = c + 1.4 * four + three

    combine(H, H + NX, lambda x, t: emit(x, t, [ref[x, rows(t), :] for ref in (p1, p2, m1, m2)]))
    for base, strip in ((0, low), (H + NX, high)):
        for i in range(H):
            for t in range(TILES):
                emit(base + i, t, [strip[n * H + i, rows(t), :] for n in range(4)])

    def put(x, t, value):
        y[x, rows(t), :] = value

    fd_pass(e, adv, dif, put, 1, EX - 1, STEP, range(TILES), masks)
    finish(edge, e, y, w, None, None, moments, masks)


def last_kernel(e, nu4, nu3, y2, w2, sums, out, adv, dif, base):
    masks = Masks()
    a, b = full(*coefficients(*read_sums(sums, 4)))

    def emit(x, t):
        nu = a * y2[x, rows(t), :] + b * w2[x, rows(t), :]
        cot = e[C, x, rows(t), :]
        four, three = nu4[x, rows(t), :], nu3[x, rows(t), :]
        adv[x, rows(t), :] = 0.6 * cot + 0.8 * four + three + 2.0 * nu
        dif[x, rows(t), :] = 0.6 * (cot + four) + three + nu
        base[x, rows(t), :] = cot + four + three + nu

    combine(H - 1, H + NX + 1, emit)

    def put(x, t, value):
        out[x - H, rows(t - 1), :] = base[x, rows(t), :] + value

    fd_pass(e, adv, dif, put, H, H + NX, BLOCK_STEP, INNER, masks)


def shape(*dims):
    return jax.ShapeDtypeStruct(dims, F32)


FIELD = shape(EX, EY, NZ)
EXT = shape(9, EX, EY, NZ)
SCRATCH = [pltpu.VMEM((EX, EY, NZ), F32)]
STRIP = shape(2 * H, EY, NZ)
STRIPS = shape(4 * H, EY, NZ)
ROWS = shape(128, NZ)
VMEM = pl.BlockSpec(memory_space=pltpu.VMEM)
SMEM = pl.BlockSpec(memory_space=pltpu.SMEM)
HBM = pl.BlockSpec(memory_space=pltpu.HBM)
LIMIT = 8 * 1024 * 1024


def call(kernel, outs, ins, scratch=(), name=None, specs=None, sems=0, aliases=None):
    return pl.pallas_call(
        kernel,
        out_shape=outs,
        in_specs=specs or [SMEM] + [VMEM] * (len(ins) - 1),
        out_specs=jax.tree.map(lambda _: VMEM, outs),
        scratch_shapes=list(scratch) + ([pltpu.SemaphoreType.DMA((sems,))] if sems else []),
        input_output_aliases=aliases or {},
        compiler_params=pltpu.CompilerParams(vmem_limit_bytes=LIMIT),
        name=name,
    )(*ins)


def local(cotangent, speed, coeff, dirs):
    nx, ny = lax.axis_size("gx"), lax.axis_size("gy")
    ix, iy = lax.axis_index("gx"), lax.axis_index("gy")
    hbm = [pltpu.with_memory_space_constraint(v, pltpu.HBM) for v in (cotangent, speed, coeff, dirs)]
    edge = jnp.stack([(ix < nx - 1).astype(jnp.int32), (iy < ny - 1).astype(jnp.int32)])

    strips = call(
        pack_kernel,
        [shape(NLOW, NY, NZ), shape(NHIGH, NY, NZ), shape(NX // GROUP, YROWS_LOW, NZ), shape(NX // GROUP, YROWS_HIGH, NZ)]
        + [shape(NLOW, T, NZ)] * 2 + [shape(NHIGH, T, NZ)] * 2,
        [edge, *hbm],
        specs=[SMEM] + [HBM] * 4,
        scratch=[pltpu.VMEM((3, NX, NY), jnp.int32)] + [pltpu.VMEM((7, NX, T, NZ), F32)] * 2,
        sems=29,
        name="pack",
    )

    def shifted(value, dx, dy):
        perm = []
        for i in range(nx):
            for j in range(ny):
                if 0 <= i + dx < nx and 0 <= j + dy < ny:
                    perm.append((i * ny + j, (i + dx) * ny + j + dy))
        return lax.ppermute(value, ("gx", "gy"), perm)

    def along_x(up, down):
        return shifted(up, 1, 0), shifted(down, -1, 0)

    def reduced(moments):
        return lax.all_to_all(moments, ("gx", "gy"), 0, 0, tiled=True)

    moves = ((1, 0), (-1, 0), (0, 1), (0, -1), (1, 1), (1, -1), (-1, 1), (-1, -1))
    received = [shifted(s, dx, dy) for s, (dx, dy) in zip(strips, moves)]
    e = call(center_kernel, EXT, [cotangent, speed, coeff, dirs], specs=[VMEM] * 4, name="center")
    e, y, w, up, down = call(
        first_kernel, [EXT, FIELD, FIELD, STRIP, STRIP], [edge, e, *received], aliases={1: 0}, name="first"
    )
    inner = call(inner_kernel, [FIELD] * 4, [edge, e, y, w], name="inner")
    *basis, up, down, moments = call(
        basis_kernel,
        [FIELD] * 6 + [STRIPS, STRIPS, ROWS],
        [edge, e, y, w, *inner, *along_x(up, down)],
        scratch=SCRATCH * 2,
        aliases={n + 2: n for n in range(6)},
        name="basis",
    )
    low, high = along_x(up, down)
    nu4, nu3, y2, w2, moments = call(
        second_kernel,
        [FIELD] * 4 + [ROWS],
        [edge, e, *basis, low, high, reduced(moments)],
        scratch=SCRATCH * 2,
        name="second",
    )
    return call(
        last_kernel, shape(NX, NY, NZ), [e, nu4, nu3, y2, w2, reduced(moments)], scratch=SCRATCH * 3, specs=[VMEM] * 6, name="last"
    )


def solution(mesh):
    placed = (P("gx", "gy", None), P(None, "gx", "gy", None), P(None, "gx", "gy", None), P(None, "gx", "gy"))
    return jax.shard_map(local, mesh=mesh, in_specs=placed, out_specs=P("gx", "gy", None), check_vma=False)
```

```python
import jax
import jax.numpy as jnp
from jax import lax
from jax.experimental import pallas as pl
from jax.experimental.pallas import tpu as pltpu
from jax.sharding import PartitionSpec as P


NX, NY, NZ = 32, 64, 128
H = 3
T = 8
EX, EY = NX + 2 * H, NY + 2 * T
TILES = EY // T
INNER = range(1, TILES - 1)
F32 = jnp.float32

C, K, U, K2B, U2B = 0, 1, 4, 7, 8
LOW = ((0, 3), (1, 3), (4, 3), (2, 2), (3, 2), (5, 2), (6, 2))
HIGH = ((0, 3), (1, 2), (4, 2), (2, 2), (3, 2), (5, 2), (6, 2))
NLOW = sum(n for _, n in LOW)
NHIGH = sum(n for _, n in HIGH)
YLOW = ((0, 7), (1, 6), (4, 6), (2, 7), (3, 6), (5, 7), (6, 6))
YHIGH = ((0, 7), (1, 6), (4, 6), (2, 6), (3, 6), (5, 6), (6, 6))
GROUP = 8
YROWS_LOW = GROUP * sum(n for _, n in YLOW)
YROWS_HIGH = GROUP * sum(n for _, n in YHIGH)
STEP = 9
CENTER_STEP = 8
THREE_STEP = 4
A0, B0 = 0.6, -0.083
PAIRS = ((0, 0), (0, 1), (0, 2), (1, 1), (1, 2), (2, 2))
BLOCK_STEP = 8


def rows(t):
    return slice(t * T, (t + 1) * T)


class Masks:
    def __init__(self):
        lane = lax.broadcasted_iota(jnp.int32, (T, NZ), 1)
        row = lax.broadcasted_iota(jnp.int32, (T, NZ), 0)
        self.first, self.last, self.top = lane == 0, lane == NZ - 1, row == 0


def back(v):
    return pltpu.roll(v, 1, 1)


class Tiles:
    def __init__(self, ref, masks):
        self.ref, self.masks, self.seen = ref, masks, {}

    def at(self, x, i, t):
        key = (i, t)
        if key not in self.seen:
            self.seen[key] = self.ref[x + i, rows(t), :]
        return self.seen[key]

    def dx(self, x, i, t):
        return self.at(x, i + 1, t) - self.at(x, i, t)

    def dy(self, x, i, t):
        v = self.at(x, i, t)
        if t + 1 < TILES:
            return self.ref[x + i, t * T + 1 : (t + 1) * T + 1, :] - v
        return pltpu.roll(v, T - 1, 0) - v

    def dz(self, x, i, t):
        v = self.at(x, i, t)
        return jnp.where(self.masks.last, 0.0, pltpu.roll(v, NZ - 1, 1)) - v

    def dz_below(self, x, i, t):
        v = self.at(x, i, t)
        return v - back(v)


def sweep(x0, x1, step, body, carry):
    count = (x1 - x0) // step
    assert count * step == x1 - x0
    return lax.fori_loop(0, count, lambda n, c: body(x0 + n * step, c), carry)


def fluxes(x0, tiles, masks, parts, emit):
    def plane(x, low_x, i, fetch):
        new_low = []
        before = jnp.zeros((T, NZ), F32)
        if tiles[0] > 0:
            before = pltpu.roll(parts(fetch, 1, x, i, tiles[0] - 1)[1], 1, 0)
        for n, t in enumerate(tiles):
            up_x, down_x = parts(fetch, 0, x, i, t)
            up_y, down_y = parts(fetch, 1, x, i, t)
            up_z, down_z = parts(fetch, 2, x, i, t)
            rolled = pltpu.roll(down_y, 1, 0)
            down_y = jnp.where(masks.top, before, rolled)
            before = rolled
            total = (up_x - low_x[n]) + (up_y - down_y) + (up_z - down_z)
            new_low.append(down_x)
            emit(fetch, x, i, t, total)
        return new_low

    return plane


def run(x0, x1, step, tiles, masks, fetch_of, parts, emit):
    plane = fluxes(x0, tiles, masks, parts, emit)
    fetch = fetch_of()
    low = [parts(fetch, 0, x0 - 1, 0, t)[1] for t in tiles]

    def body(x, low):
        fetch = fetch_of()
        for i in range(step):
            low = plane(x, low, i, fetch)
        return low

    sweep(x0, x1, step, body, low)


def m_pass(e, v_ref, w_ref, masks, x0=1, x1=NX + 2 * H - 1, step=None):
    def parts(v, d, x, i, t):
        if d == 2:
            return e[K + 2, x + i, rows(t), :] * v.dz(x, i, t), e[K2B, x + i, rows(t), :] * v.dz_below(x, i, t)
        flux = e[K + d, x + i, rows(t), :] * (v.dx, v.dy)[d](x, i, t)
        return flux, flux

    def emit(v, x, i, t, total):
        w_ref[x + i, rows(t), :] = v.at(x, i, t) - total

    run(x0, x1, step or STEP, range(TILES), masks, lambda: Tiles(v_ref, masks), parts, emit)


def s_pass(e, y_ref, masks):
    cot = e.at[C]

    def parts(v, d, x, i, t):
        k, u = e[K + d, x + i, rows(t), :], e[U + d, x + i, rows(t), :]
        delta = (v.dx, v.dy, v.dz)[d](x, i, t)
        up = (k + jnp.maximum(u, 0.0)) * delta
        if d == 2:
            k, u = e[K2B, x + i, rows(t), :], e[U2B, x + i, rows(t), :]
            delta = v.dz_below(x, i, t)
        return up, (k - jnp.minimum(u, 0.0)) * delta

    def emit(v, x, i, t, total):
        y_ref[x + i, rows(t), :] = total

    run(1, EX - 1, STEP, range(TILES), masks, lambda: Tiles(cot, masks), parts, emit)


def fd_pass(e, a_ref, d_ref, put, x0, x1, step, tiles, masks):
    def parts(both, d, x, i, t):
        a, b = both
        k, u = e[K + d, x + i, rows(t), :], e[U + d, x + i, rows(t), :]
        da, db = ((v.dx, v.dy, v.dz)[d](x, i, t) for v in (a, b))
        flux = k * db
        up = flux + jnp.maximum(u, 0.0) * da
        if d == 2:
            u = e[U2B, x + i, rows(t), :]
            flux = e[K2B, x + i, rows(t), :] * b.dz_below(x, i, t)
            da = a.dz_below(x, i, t)
        return up, flux - jnp.minimum(u, 0.0) * da

    def emit(both, x, i, t, total):
        put(x + i, t, total)

    run(x0, x1, step, tiles, masks, lambda: (Tiles(a_ref, masks), Tiles(d_ref, masks)), parts, emit)


def products(e, y_ref, w_ref, masks):
    zero = jnp.zeros((T, NZ), F32)

    def body(x, accs):
        yy, yw, ww, *energy = accs
        w = Tiles(w_ref, masks)
        for i in range(BLOCK_STEP):
            for t in INNER:
                v, y = w.at(x, i, t), y_ref[x + i, rows(t), :]
                yy, yw, ww = yy + y * y, yw + y * v, ww + v * v
                for d, delta in enumerate((w.dx, w.dy, w.dz)):
                    difference = delta(x, i, t)
                    energy[d] = energy[d] + e[K + d, x + i, rows(t), :] * (difference * difference)
        return yy, yw, ww, *energy

    yy, yw, ww, *energy = sweep(H, H + NX, BLOCK_STEP, body, (zero,) * 6)
    return yy, yw, ww, ww + (energy[0] + energy[1] + energy[2])


def outside_is_zero(edge, ref):
    @pl.when(edge[0] == 0)
    def _():
        ref[H + NX : EX - 1] = jnp.zeros((H - 1, EY, NZ), F32)

    @pl.when(edge[1] == 0)
    def _():
        ref[:, EY - T :, :] = jnp.zeros((EX, T, NZ), F32)


def finish(edge, e, y, w, up, down, moments, masks):
    outside_is_zero(edge, y)
    m_pass(e, y, w, masks)
    outside_is_zero(edge, w)
    if up is not None:
        up[0:1], up[1:3] = y[NX : NX + 1], w[NX : NX + 2]
        down[0:1], down[1:3] = y[H + 2 : H + 3], w[H + 1 : H + 3]
    if moments is None:
        return
    write_sums(moments, products(e, y, w, masks))


def write_sums(moments, sums):
    lane = lax.broadcasted_iota(jnp.int32, (1, NZ), 1)
    row = jnp.zeros((1, NZ), F32)
    for i, acc in enumerate(sums):
        total = jnp.sum(jnp.sum(acc, axis=0, keepdims=True), axis=1, keepdims=True)
        row = jnp.where(lane // 4 == i, total, row)
    moments[...] = jnp.broadcast_to(row, moments.shape)


def read_sums(moments_ref, count):
    sums = jnp.sum(moments_ref[...], axis=0, keepdims=True)
    lane = lax.broadcasted_iota(jnp.int32, (1, NZ), 1)
    return [jnp.sum(jnp.where(lane == 4 * i, sums, 0.0), axis=1, keepdims=True) for i in range(count)]


def coefficients(m0, m1, m2, m3):
    alpha0 = m0 / m1
    rr = alpha0 * alpha0 * m2 - m0
    product = m1 - 2.0 * alpha0 * m2 + alpha0 * alpha0 * m3
    ratio = rr / m0
    alpha1 = rr / (product - ratio * rr / alpha0)
    a = alpha0 + alpha1 * (1.0 + ratio)
    b = -(alpha1 * alpha0)
    return a, b


def full(*scalars):
    return tuple(jnp.broadcast_to(v, (T, NZ)) for v in scalars)


def two_sections(moments_ref):
    sums = read_sums(moments_ref, 4 * len(PAIRS))
    grams = [dict(zip(PAIRS, sums[len(PAIRS) * k : len(PAIRS) * (k + 1)])) for k in range(4)]

    def moments(a, b):
        return [
            g[0, 0]
            + 2.0 * (a * g[0, 1] + b * g[0, 2])
            + (a * a * g[1, 1] + 2.0 * a * b * g[1, 2] + b * b * g[2, 2])
            for g in grams
        ]

    a, b = coefficients(*moments(-A0, -B0))
    return full(a, b, *coefficients(*moments(a - A0, b - B0)))


def signs(dirs, d, x, first_rows):
    sign = (1 - 2 * dirs[d, pl.ds(x, 1), :]).astype(F32)
    count = T * len(first_rows)
    row = lax.broadcasted_iota(jnp.int32, (count, NY), 0)
    column = lax.broadcasted_iota(jnp.int32, (count, NY), 1)
    at = row
    for n, first in enumerate(first_rows):
        at = jnp.where(row // T == n, row - n * T + first, at)
    picked = jnp.where(at == column, jnp.broadcast_to(sign, (count, NY)), 0.0)
    ones = jnp.ones((NY, NZ), jnp.bfloat16)
    return jnp.dot(picked.astype(jnp.bfloat16), ones, preferred_element_type=F32)


def pack_kernel(edge, cot, speed, coeff, all_dirs, low, high, ylow, yhigh, cll, clh, chl, chh, dirs, tops, bottoms, sems):
    bottom, top, full = slice(0, T), slice(NY - T, NY), slice(0, NY)
    copies = [pltpu.make_async_copy(all_dirs, dirs, sems.at[0])]
    copies[0].start()

    def fetch(f, planes, rows, target):
        source = cot.at[planes, rows] if f == 0 else (coeff if f < 4 else speed).at[(f - 1) % 3, planes, rows]
        copy = pltpu.make_async_copy(source, target, sems.at[len(copies)])
        copy.start()
        copies.append(copy)

    for f in range(7):
        fetch(f, slice(0, NX), top, tops.at[f])
        fetch(f, slice(0, NX), bottom, bottoms.at[f])
    signed = []
    for fields, strip in ((LOW, low), (HIGH, high)):
        at = 0
        for f, n in fields:
            start = NX - n if fields is LOW else 0
            fetch(f, slice(start, start + n), full, strip.at[at : at + n])
            if f >= 4:
                signed += [(strip, at + i, f - 4, start + i) for i in range(n)]
            at += n
    for copy in copies:
        copy.wait()
    for group in range(NX // GROUP):
        at_low = at_high = 0
        for x in range(group * GROUP, (group + 1) * GROUP):
            sign = [signs(dirs, d, x, (NY - T, 0)) for d in range(3)]
            for (f, n), (_, m) in zip(YLOW, YHIGH):
                upper, lower = tops[f, x], bottoms[f, x]
                if f >= 4:
                    upper, lower = upper * sign[f - 4][:T], lower * sign[f - 4][T:]
                ylow[group, at_low : at_low + n, :] = upper[T - n :]
                yhigh[group, at_high : at_high + m, :] = lower[:m]
                at_low += n
                at_high += m
    for strip, at, d, x in signed:
        strip[at] = strip[at] * signs(dirs, d, x, tuple(range(0, NY, T)))
    cll[...] = low[:, top, :]
    clh[...] = low[:, bottom, :]
    chl[...] = high[:, top, :]
    chh[...] = high[:, bottom, :]


def place(e, f, x, rows, value):
    if f > 0:
        value = 0.25 * value
    e[f, x, rows, :] = value
    if f in (K + 2, U + 2):
        first = lax.broadcasted_iota(jnp.int32, value.shape, 1) == 0
        e[K2B if f == K + 2 else U2B, x, rows, :] = jnp.where(first, 0.0, back(value))


def shifted_tile(ref, group, start):
    inside = min(max(start, 0), ref.shape[1] - T)
    value = ref[group, inside : inside + T, :]
    return value if inside == start else pltpu.roll(value, (inside - start) % T, 0)


def center_kernel(cot, speed, coeff, dirs, e, sems):
    every = tuple(range(0, NY, T))
    middle = slice(T, T + NY)
    copies = []
    for f in range(7):
        source = cot if f == 0 else (coeff if f < 4 else speed).at[(f - 1) % 3]
        copies.append(pltpu.make_async_copy(source, e.at[f, H : H + NX, middle], sems.at[f]))
    for copy in copies:
        copy.start()
    for copy in copies:
        copy.wait()

    def body(n, _):
        for i in range(CENTER_STEP):
            x = CENTER_STEP * n + i
            for f in range(1, 7):
                value = e[f, H + x, middle, :]
                if f >= 4:
                    value = value * signs(dirs, f - 4, x, every)
                place(e, f, H + x, middle, value)
        return _

    lax.fori_loop(0, NX // CENTER_STEP, body, 0)


def first_kernel(edge, e_in, low, high, ylow, yhigh, cll, clh, chl, chh, e, y, w, up, down):
    masks = Masks()
    middle, below, above = slice(T, T + NY), slice(0, T), slice(T + NY, EY)
    for fields, base, middles, lows, highs in (
        (LOW, None, low, cll, clh),
        (HIGH, H + NX, high, chl, chh),
    ):
        at = 0
        for f, n in fields:
            for i in range(n):
                x = (H - n if base is None else base) + i
                place(e, f, x, middle, middles[at + i])
                place(e, f, x, below, lows[at + i])
                place(e, f, x, above, highs[at + i])
            at += n

    def body(group, _):
        at_low = at_high = 0
        for i in range(GROUP):
            x = H + group * GROUP + i
            for (f, n), (_, m) in zip(YLOW, YHIGH):
                place(e, f, x, below, shifted_tile(ylow, group, at_low + n - T))
                place(e, f, x, above, shifted_tile(yhigh, group, at_high))
                at_low += n
                at_high += m
        return _

    lax.fori_loop(0, NX // GROUP, body, 0)
    s_pass(e, y, masks)
    finish(edge, e, y, w, up, down, None, masks)


def combine(x0, x1, emit, tiles=range(TILES)):
    def body(n, _):
        for i in range(2):
            for t in tiles:
                emit(x0 + 2 * n + i, t)
        return _

    lax.fori_loop(0, (x1 - x0) // 2, body, 0)


def parts_pass(e, y_ref, w_ref, p1, p2, x0, x1, step, masks):
    zero = jnp.zeros((T, NZ), F32)
    tiles = range(TILES)

    def faces(both, d, x, i, t):
        y, w = both
        k, u = e[K + d, x + i, rows(t), :], e[U + d, x + i, rows(t), :]
        dy, dw = ((v.dx, v.dy, v.dz)[d](x, i, t) for v in both)
        ahead = 2.0 * jnp.maximum(u, 0.0)
        flux = k * dw
        up = (ahead * dy, ahead * dw + flux)
        if d == 2:
            k, u = e[K2B, x + i, rows(t), :], e[U2B, x + i, rows(t), :]
            dy, dw = y.dz_below(x, i, t), w.dz_below(x, i, t)
            flux = k * dw
        behind = 2.0 * jnp.minimum(u, 0.0)
        return up, (behind * dy, behind * dw - flux)

    first = (Tiles(y_ref, masks), Tiles(w_ref, masks))
    low_x = [faces(first, 0, x0 - 1, 0, t)[1] for t in tiles]

    def body(x, low_x):
        both = (Tiles(y_ref, masks), Tiles(w_ref, masks))
        for i in range(step):
            before = (zero, zero)
            next_low = []
            for t in tiles:
                (x_up, x_low), (y_up, y_low), (z_up, z_low) = (faces(both, d, x, i, t) for d in range(3))
                next_low.append(x_low)
                rolled = tuple(pltpu.roll(v, 1, 0) for v in y_low)
                y_below = [jnp.where(masks.top, old, new) for old, new in zip(before, rolled)]
                before = rolled
                totals = [
                    (x_up[j] + low_x[t][j]) + (y_up[j] + y_below[j]) + (z_up[j] + z_low[j]) for j in range(2)
                ]
                p1[x + i, rows(t), :] = totals[0] + (both[0].at(x, i, t) - both[1].at(x, i, t))
                p2[x + i, rows(t), :] = totals[1]
            low_x = next_low
        return low_x

    sweep(x0, x1, step, body, low_x)


def products_of_three(e, fields, images, masks):
    zero = jnp.zeros((T, NZ), F32)
    count = len(PAIRS)

    def body(x, accs):
        accs = list(accs)
        readers = [Tiles(ref, masks) for ref in images]
        for i in range(THREE_STEP):
            for t in INNER:
                q = [ref[x + i, rows(t), :] for ref in fields]
                m = [v.at(x, i, t) for v in readers]
                for n, (j, k) in enumerate(PAIRS):
                    accs[n] = accs[n] + q[j] * q[k]
                    accs[count + n] = accs[count + n] + q[j] * m[k]
                    accs[2 * count + n] = accs[2 * count + n] + m[j] * m[k]
                for d in range(3):
                    delta = [(v.dx, v.dy, v.dz)[d](x, i, t) for v in readers]
                    scaled = [e[K + d, x + i, rows(t), :] * v for v in delta]
                    for n, (j, k) in enumerate(PAIRS):
                        accs[3 * count + n] = accs[3 * count + n] + scaled[j] * delta[k]
        return tuple(accs)

    accs = sweep(H, H + NX, THREE_STEP, body, (zero,) * (4 * count))
    return accs[: 3 * count] + tuple(accs[3 * count + n] + accs[2 * count + n] for n in range(count))


def inner_kernel(edge, e, y, w, p1, p2, m1, m2):
    masks = Masks()
    parts_pass(e, y, w, p1, p2, H + 1, H + NX - 1, 10, masks)
    for p, m in ((p1, m1), (p2, m2)):
        outside_is_zero(edge, p)
        m_pass(e, p, m, masks, H + 2, H + NX - 2, 7)


def basis_kernel(
    edge, e, y_in, w_in, p1_in, p2_in, m1_in, m2_in, low, high, y4, w4, p1, p2, m1, m2, up, down, moments, q0, n0
):
    masks = Masks()
    y4[0:1], w4[0:2] = low[0:1], low[1:3]
    y4[EX - 1 :], w4[EX - 2 :] = high[0:1], high[1:3]
    for x0 in (1, H + NX - 1):
        parts_pass(e, y4, w4, p1, p2, x0, x0 + H, H, masks)
    for p, m in ((p1, m1), (p2, m2)):
        outside_is_zero(edge, p)
        m_pass(e, p, m, masks, H - 1, H + 2, 3)
        m_pass(e, p, m, masks, H + NX - 2, H + NX + 1, 3)
        outside_is_zero(edge, m)
    for n, (p, m) in enumerate(((p1, m1), (p2, m2))):
        up[n : n + 1], up[2 * n + 2 : 2 * n + 4] = p[NX : NX + 1], m[NX : NX + 2]
        down[n : n + 1], down[2 * n + 2 : 2 * n + 4] = p[H + 2 : H + 3], m[H + 1 : H + 3]

    def emit(x, t):
        at = (x, rows(t))
        q0[at] = y4[at] + A0 * p1[at] + B0 * p2[at]
        n0[at] = w4[at] + A0 * m1[at] + B0 * m2[at]

    combine(H, H + NX + 2, emit, range(1, TILES))
    write_sums(moments, products_of_three(e, (q0, p1, p2), (n0, m1, m2), masks))


def second_kernel(edge, e, y4, w4, p1, p2, m1, m2, low, high, sums, nu4, nu3, y, w, moments, adv, dif):
    masks = Masks()
    a4, b4, a3, b3 = two_sections(sums)

    def emit(x, t, parts):
        v, m = y4[x, rows(t), :], w4[x, rows(t), :]
        q1, q2, n1, n2 = parts
        c = 1.4 * e[C, x, rows(t), :]
        four = a4 * v + b4 * m
        three = a3 * (v + a4 * q1 + b4 * q2) + b3 * (m + a4 * n1 + b4 * n2)
        nu4[x, rows(t), :] = four
        nu3[x, rows(t), :] = three
        adv[x, rows(t), :] = c + 1.2 * four + 2.0 * three
        dif[x, rows(t), :] = c + 1.4 * four + three

    def read(ref, x, t):
        return ref[x, rows(t), :]

    combine(H - 1, H + NX + 1, lambda x, t: emit(x, t, [read(ref, x, t) for ref in (p1, p2, m1, m2)]))
    for x, strip, p_at, m_at in ((0, low, 0, 0), (1, low, None, 1), (EX - 2, high, None, 0), (EX - 1, high, 0, 1)):
        for t in range(TILES):
            ps = [read(ref, x, t) for ref in (p1, p2)] if p_at is None else [read(strip, n, t) for n in range(2)]
            emit(x, t, ps + [read(strip, 2 + 2 * n + m_at, t) for n in range(2)])

    def put(x, t, value):
        y[x, rows(t), :] = value

    fd_pass(e, adv, dif, put, 1, EX - 1, STEP, range(TILES), masks)
    finish(edge, e, y, w, None, None, moments, masks)


def last_kernel(e, nu4, nu3, y2, w2, sums, out, adv, dif, base):
    masks = Masks()
    a, b = full(*coefficients(*read_sums(sums, 4)))

    def emit(x, t):
        nu = a * y2[x, rows(t), :] + b * w2[x, rows(t), :]
        cot = e[C, x, rows(t), :]
        four, three = nu4[x, rows(t), :], nu3[x, rows(t), :]
        adv[x, rows(t), :] = 0.6 * cot + 0.8 * four + three + 2.0 * nu
        dif[x, rows(t), :] = 0.6 * (cot + four) + three + nu
        base[x, rows(t), :] = cot + four + three + nu

    combine(H - 1, H + NX + 1, emit)

    def put(x, t, value):
        out[x - H, rows(t - 1), :] = base[x, rows(t), :] + value

    fd_pass(e, adv, dif, put, H, H + NX, BLOCK_STEP, INNER, masks)


def shape(*dims):
    return jax.ShapeDtypeStruct(dims, F32)


FIELD = shape(EX, EY, NZ)
EXT = shape(9, EX, EY, NZ)
SCRATCH = [pltpu.VMEM((EX, EY, NZ), F32)]
STRIP = shape(3, EY, NZ)
STRIPS = shape(6, EY, NZ)
ROWS = shape(128, NZ)
VMEM = pl.BlockSpec(memory_space=pltpu.VMEM)
SMEM = pl.BlockSpec(memory_space=pltpu.SMEM)
HBM = pl.BlockSpec(memory_space=pltpu.HBM)
LIMIT = 8 * 1024 * 1024


def call(kernel, outs, ins, scratch=(), name=None, specs=None, sems=0, aliases=None):
    return pl.pallas_call(
        kernel,
        out_shape=outs,
        in_specs=specs or [SMEM] + [VMEM] * (len(ins) - 1),
        out_specs=jax.tree.map(lambda _: VMEM, outs),
        scratch_shapes=list(scratch) + ([pltpu.SemaphoreType.DMA((sems,))] if sems else []),
        input_output_aliases=aliases or {},
        compiler_params=pltpu.CompilerParams(vmem_limit_bytes=LIMIT),
        name=name,
    )(*ins)


def local(cotangent, speed, coeff, dirs):
    nx, ny = lax.axis_size("gx"), lax.axis_size("gy")
    ix, iy = lax.axis_index("gx"), lax.axis_index("gy")
    hbm = [pltpu.with_memory_space_constraint(v, pltpu.HBM) for v in (cotangent, speed, coeff, dirs)]
    edge = jnp.stack([(ix < nx - 1).astype(jnp.int32), (iy < ny - 1).astype(jnp.int32)])

    strips = call(
        pack_kernel,
        [shape(NLOW, NY, NZ), shape(NHIGH, NY, NZ), shape(NX // GROUP, YROWS_LOW, NZ), shape(NX // GROUP, YROWS_HIGH, NZ)]
        + [shape(NLOW, T, NZ)] * 2 + [shape(NHIGH, T, NZ)] * 2,
        [edge, *hbm],
        specs=[SMEM] + [HBM] * 4,
        scratch=[pltpu.VMEM((3, NX, NY), jnp.int32)] + [pltpu.VMEM((7, NX, T, NZ), F32)] * 2,
        sems=29,
        name="pack",
    )

    def shifted(value, dx, dy):
        perm = []
        for i in range(nx):
            for j in range(ny):
                if 0 <= i + dx < nx and 0 <= j + dy < ny:
                    perm.append((i * ny + j, (i + dx) * ny + j + dy))
        return lax.ppermute(value, ("gx", "gy"), perm)

    def along_x(up, down):
        return shifted(up, 1, 0), shifted(down, -1, 0)

    def reduced(moments):
        return lax.all_to_all(moments, ("gx", "gy"), 0, 0, tiled=True)

    moves = ((1, 0), (-1, 0), (0, 1), (0, -1), (1, 1), (1, -1), (-1, 1), (-1, -1))
    received = [shifted(s, dx, dy) for s, (dx, dy) in zip(strips, moves)]
    e = call(center_kernel, EXT, [*hbm[:3], dirs], specs=[HBM] * 3 + [VMEM], sems=7, name="center")
    e, y, w, up, down = call(
        first_kernel, [EXT, FIELD, FIELD, STRIP, STRIP], [edge, e, *received], aliases={1: 0}, name="first"
    )
    inner = call(inner_kernel, [FIELD] * 4, [edge, e, y, w], name="inner")
    *basis, up, down, moments = call(
        basis_kernel,
        [FIELD] * 6 + [STRIPS, STRIPS, ROWS],
        [edge, e, y, w, *inner, *along_x(up, down)],
        scratch=SCRATCH * 2,
        aliases={n + 2: n for n in range(6)},
        name="basis",
    )
    low, high = along_x(up, down)
    nu4, nu3, y2, w2, moments = call(
        second_kernel,
        [FIELD] * 4 + [ROWS],
        [edge, e, *basis, low, high, reduced(moments)],
        scratch=SCRATCH * 2,
        name="second",
    )
    return call(
        last_kernel, shape(NX, NY, NZ), [e, nu4, nu3, y2, w2, reduced(moments)], scratch=SCRATCH * 3, specs=[VMEM] * 6, name="last"
    )


def solution(mesh):
    placed = (P("gx", "gy", None), P(None, "gx", "gy", None), P(None, "gx", "gy", None), P(None, "gx", "gy"))
    return jax.shard_map(local, mesh=mesh, in_specs=placed, out_specs=P("gx", "gy", None), check_vma=False)
```

```python
import jax
import jax.numpy as jnp
from jax import lax
from jax.experimental import pallas as pl
from jax.experimental.pallas import tpu as pltpu
from jax.sharding import PartitionSpec as P


NX, NY, NZ = 32, 64, 128
H = 3
T = 8
EX, EY = NX + 2 * H, NY + 2 * T
TILES = EY // T
INNER = range(1, TILES - 1)
F32 = jnp.float32

C, K, U, K2B, U2B = 0, 1, 4, 7, 8
LOW = ((0, 3), (1, 3), (4, 3), (2, 2), (3, 2), (5, 2), (6, 2))
HIGH = ((0, 3), (1, 2), (4, 2), (2, 2), (3, 2), (5, 2), (6, 2))
NLOW = sum(n for _, n in LOW)
NHIGH = sum(n for _, n in HIGH)
YLOW = ((0, 7), (1, 6), (4, 6), (2, 7), (3, 6), (5, 7), (6, 6))
YHIGH = ((0, 7), (1, 6), (4, 6), (2, 6), (3, 6), (5, 6), (6, 6))
GROUP = 8
YROWS_LOW = GROUP * sum(n for _, n in YLOW)
YROWS_HIGH = GROUP * sum(n for _, n in YHIGH)
STEP = 9
CENTER_STEP = 8
THREE_STEP = 8
A0, B0 = 0.6, -0.083
PAIRS = ((0, 0), (0, 1), (0, 2), (1, 1), (1, 2), (2, 2))
BLOCK_STEP = 8


def rows(t):
    return slice(t * T, (t + 1) * T)


class Masks:
    def __init__(self):
        lane = lax.broadcasted_iota(jnp.int32, (T, NZ), 1)
        row = lax.broadcasted_iota(jnp.int32, (T, NZ), 0)
        self.first, self.last, self.top = lane == 0, lane == NZ - 1, row == 0


def back(v):
    return pltpu.roll(v, 1, 1)


class Tiles:
    def __init__(self, ref, masks):
        self.ref, self.masks, self.seen = ref, masks, {}

    def at(self, x, i, t):
        key = (i, t)
        if key not in self.seen:
            self.seen[key] = self.ref[x + i, rows(t), :]
        return self.seen[key]

    def dx(self, x, i, t):
        return self.at(x, i + 1, t) - self.at(x, i, t)

    def dy(self, x, i, t):
        v = self.at(x, i, t)
        if t + 1 < TILES:
            return self.ref[x + i, t * T + 1 : (t + 1) * T + 1, :] - v
        return pltpu.roll(v, T - 1, 0) - v

    def dz(self, x, i, t):
        v = self.at(x, i, t)
        return jnp.where(self.masks.last, 0.0, pltpu.roll(v, NZ - 1, 1)) - v

    def dz_below(self, x, i, t):
        v = self.at(x, i, t)
        return v - back(v)


def sweep(x0, x1, step, body, carry):
    count = (x1 - x0) // step
    assert count * step == x1 - x0
    return lax.fori_loop(0, count, lambda n, c: body(x0 + n * step, c), carry)


def fluxes(x0, tiles, masks, parts, emit):
    def plane(x, low_x, i, fetch):
        new_low = []
        before = jnp.zeros((T, NZ), F32)
        if tiles[0] > 0:
            before = pltpu.roll(parts(fetch, 1, x, i, tiles[0] - 1)[1], 1, 0)
        for n, t in enumerate(tiles):
            up_x, down_x = parts(fetch, 0, x, i, t)
            up_y, down_y = parts(fetch, 1, x, i, t)
            up_z, down_z = parts(fetch, 2, x, i, t)
            rolled = pltpu.roll(down_y, 1, 0)
            down_y = jnp.where(masks.top, before, rolled)
            before = rolled
            total = (up_x - low_x[n]) + (up_y - down_y) + (up_z - down_z)
            new_low.append(down_x)
            emit(fetch, x, i, t, total)
        return new_low

    return plane


def run(x0, x1, step, tiles, masks, fetch_of, parts, emit):
    plane = fluxes(x0, tiles, masks, parts, emit)
    fetch = fetch_of()
    low = [parts(fetch, 0, x0 - 1, 0, t)[1] for t in tiles]

    def body(x, low):
        fetch = fetch_of()
        for i in range(step):
            low = plane(x, low, i, fetch)
        return low

    sweep(x0, x1, step, body, low)


def m_pass(e, v_ref, w_ref, masks, x0=1, x1=NX + 2 * H - 1, step=None):
    def parts(v, d, x, i, t):
        if d == 2:
            return e[K + 2, x + i, rows(t), :] * v.dz(x, i, t), e[K2B, x + i, rows(t), :] * v.dz_below(x, i, t)
        flux = e[K + d, x + i, rows(t), :] * (v.dx, v.dy)[d](x, i, t)
        return flux, flux

    def emit(v, x, i, t, total):
        w_ref[x + i, rows(t), :] = v.at(x, i, t) - total

    run(x0, x1, step or STEP, range(TILES), masks, lambda: Tiles(v_ref, masks), parts, emit)


def s_pass(e, y_ref, masks):
    cot = e.at[C]

    def parts(v, d, x, i, t):
        k, u = e[K + d, x + i, rows(t), :], e[U + d, x + i, rows(t), :]
        delta = (v.dx, v.dy, v.dz)[d](x, i, t)
        up = (k + jnp.maximum(u, 0.0)) * delta
        if d == 2:
            k, u = e[K2B, x + i, rows(t), :], e[U2B, x + i, rows(t), :]
            delta = v.dz_below(x, i, t)
        return up, (k - jnp.minimum(u, 0.0)) * delta

    def emit(v, x, i, t, total):
        y_ref[x + i, rows(t), :] = total

    run(1, EX - 1, STEP, range(TILES), masks, lambda: Tiles(cot, masks), parts, emit)


def fd_pass(e, a_ref, d_ref, put, x0, x1, step, tiles, masks):
    def parts(both, d, x, i, t):
        a, b = both
        k, u = e[K + d, x + i, rows(t), :], e[U + d, x + i, rows(t), :]
        da, db = ((v.dx, v.dy, v.dz)[d](x, i, t) for v in (a, b))
        flux = k * db
        up = flux + jnp.maximum(u, 0.0) * da
        if d == 2:
            u = e[U2B, x + i, rows(t), :]
            flux = e[K2B, x + i, rows(t), :] * b.dz_below(x, i, t)
            da = a.dz_below(x, i, t)
        return up, flux - jnp.minimum(u, 0.0) * da

    def emit(both, x, i, t, total):
        put(x + i, t, total)

    run(x0, x1, step, tiles, masks, lambda: (Tiles(a_ref, masks), Tiles(d_ref, masks)), parts, emit)


def products(e, y_ref, w_ref, masks):
    zero = jnp.zeros((T, NZ), F32)

    def body(x, accs):
        yy, yw, ww, *energy = accs
        w = Tiles(w_ref, masks)
        for i in range(BLOCK_STEP):
            for t in INNER:
                v, y = w.at(x, i, t), y_ref[x + i, rows(t), :]
                yy, yw, ww = yy + y * y, yw + y * v, ww + v * v
                for d, delta in enumerate((w.dx, w.dy, w.dz)):
                    difference = delta(x, i, t)
                    energy[d] = energy[d] + e[K + d, x + i, rows(t), :] * (difference * difference)
        return yy, yw, ww, *energy

    yy, yw, ww, *energy = sweep(H, H + NX, BLOCK_STEP, body, (zero,) * 6)
    return yy, yw, ww, ww + (energy[0] + energy[1] + energy[2])


def outside_is_zero(edge, ref):
    @pl.when(edge[0] == 0)
    def _():
        ref[H + NX : EX - 1] = jnp.zeros((H - 1, EY, NZ), F32)

    @pl.when(edge[1] == 0)
    def _():
        ref[:, EY - T :, :] = jnp.zeros((EX, T, NZ), F32)


def finish(edge, e, y, w, up, down, moments, masks):
    outside_is_zero(edge, y)
    m_pass(e, y, w, masks)
    outside_is_zero(edge, w)
    if up is not None:
        up[0:1], up[1:3] = y[NX : NX + 1], w[NX : NX + 2]
        down[0:1], down[1:3] = y[H + 2 : H + 3], w[H + 1 : H + 3]
    if moments is None:
        return
    write_sums(moments, products(e, y, w, masks))


def write_sums(moments, sums):
    lane = lax.broadcasted_iota(jnp.int32, (1, NZ), 1)
    row = jnp.zeros((1, NZ), F32)
    for i, acc in enumerate(sums):
        total = jnp.sum(jnp.sum(acc, axis=0, keepdims=True), axis=1, keepdims=True)
        row = jnp.where(lane // 4 == i, total, row)
    moments[...] = jnp.broadcast_to(row, moments.shape)


def read_sums(moments_ref, count):
    sums = jnp.sum(moments_ref[...], axis=0, keepdims=True)
    lane = lax.broadcasted_iota(jnp.int32, (1, NZ), 1)
    return [jnp.sum(jnp.where(lane == 4 * i, sums, 0.0), axis=1, keepdims=True) for i in range(count)]


def coefficients(m0, m1, m2, m3):
    alpha0 = m0 / m1
    rr = alpha0 * alpha0 * m2 - m0
    product = m1 - 2.0 * alpha0 * m2 + alpha0 * alpha0 * m3
    ratio = rr / m0
    alpha1 = rr / (product - ratio * rr / alpha0)
    a = alpha0 + alpha1 * (1.0 + ratio)
    b = -(alpha1 * alpha0)
    return a, b


def full(*scalars):
    return tuple(jnp.broadcast_to(v, (T, NZ)) for v in scalars)


def two_sections(moments_ref):
    sums = read_sums(moments_ref, 4 * len(PAIRS))
    grams = [dict(zip(PAIRS, sums[len(PAIRS) * k : len(PAIRS) * (k + 1)])) for k in range(4)]

    def moments(a, b):
        return [
            g[0, 0]
            + 2.0 * (a * g[0, 1] + b * g[0, 2])
            + (a * a * g[1, 1] + 2.0 * a * b * g[1, 2] + b * b * g[2, 2])
            for g in grams
        ]

    a, b = coefficients(*moments(-A0, -B0))
    return full(a, b, *coefficients(*moments(a - A0, b - B0)))


def signs(dirs, d, x, first_rows):
    sign = (1 - 2 * dirs[d, pl.ds(x, 1), :]).astype(F32)
    count = T * len(first_rows)
    row = lax.broadcasted_iota(jnp.int32, (count, NY), 0)
    column = lax.broadcasted_iota(jnp.int32, (count, NY), 1)
    at = row
    for n, first in enumerate(first_rows):
        at = jnp.where(row // T == n, row - n * T + first, at)
    picked = jnp.where(at == column, jnp.broadcast_to(sign, (count, NY)), 0.0)
    ones = jnp.ones((NY, NZ), jnp.bfloat16)
    return jnp.dot(picked.astype(jnp.bfloat16), ones, preferred_element_type=F32)


def pack_kernel(edge, cot, speed, coeff, all_dirs, low, high, ylow, yhigh, cll, clh, chl, chh, dirs, tops, bottoms, sems):
    bottom, top, full = slice(0, T), slice(NY - T, NY), slice(0, NY)
    copies = [pltpu.make_async_copy(all_dirs, dirs, sems.at[0])]
    copies[0].start()

    def fetch(f, planes, rows, target):
        source = cot.at[planes, rows] if f == 0 else (coeff if f < 4 else speed).at[(f - 1) % 3, planes, rows]
        copy = pltpu.make_async_copy(source, target, sems.at[len(copies)])
        copy.start()
        copies.append(copy)

    for f in range(7):
        fetch(f, slice(0, NX), top, tops.at[f])
        fetch(f, slice(0, NX), bottom, bottoms.at[f])
    signed = []
    for fields, strip in ((LOW, low), (HIGH, high)):
        at = 0
        for f, n in fields:
            start = NX - n if fields is LOW else 0
            fetch(f, slice(start, start + n), full, strip.at[at : at + n])
            if f >= 4:
                signed += [(strip, at + i, f - 4, start + i) for i in range(n)]
            at += n
    for copy in copies:
        copy.wait()
    for group in range(NX // GROUP):
        at_low = at_high = 0
        for x in range(group * GROUP, (group + 1) * GROUP):
            sign = [signs(dirs, d, x, (NY - T, 0)) for d in range(3)]
            for (f, n), (_, m) in zip(YLOW, YHIGH):
                upper, lower = tops[f, x], bottoms[f, x]
                if f >= 4:
                    upper, lower = upper * sign[f - 4][:T], lower * sign[f - 4][T:]
                ylow[group, at_low : at_low + n, :] = upper[T - n :]
                yhigh[group, at_high : at_high + m, :] = lower[:m]
                at_low += n
                at_high += m
    for strip, at, d, x in signed:
        strip[at] = strip[at] * signs(dirs, d, x, tuple(range(0, NY, T)))
    cll[...] = low[:, top, :]
    clh[...] = low[:, bottom, :]
    chl[...] = high[:, top, :]
    chh[...] = high[:, bottom, :]


def place(e, f, x, rows, value):
    if f > 0:
        value = 0.25 * value
    e[f, x, rows, :] = value
    if f in (K + 2, U + 2):
        first = lax.broadcasted_iota(jnp.int32, value.shape, 1) == 0
        e[K2B if f == K + 2 else U2B, x, rows, :] = jnp.where(first, 0.0, back(value))


def shifted_tile(ref, group, start):
    inside = min(max(start, 0), ref.shape[1] - T)
    value = ref[group, inside : inside + T, :]
    return value if inside == start else pltpu.roll(value, (inside - start) % T, 0)


def center_kernel(cot, speed, coeff, dirs, e, sems):
    every = tuple(range(0, NY, T))
    middle = slice(T, T + NY)
    copies = []
    for f in range(7):
        source = cot if f == 0 else (coeff if f < 4 else speed).at[(f - 1) % 3]
        copies.append(pltpu.make_async_copy(source, e.at[f, H : H + NX, middle], sems.at[f]))
    for copy in copies:
        copy.start()
    for copy in copies:
        copy.wait()

    def body(n, _):
        for i in range(CENTER_STEP):
            x = CENTER_STEP * n + i
            for f in range(1, 7):
                value = e[f, H + x, middle, :]
                if f >= 4:
                    value = value * signs(dirs, f - 4, x, every)
                place(e, f, H + x, middle, value)
        return _

    lax.fori_loop(0, NX // CENTER_STEP, body, 0)


def first_kernel(edge, e_in, low, high, ylow, yhigh, cll, clh, chl, chh, e, y, w, up, down):
    masks = Masks()
    middle, below, above = slice(T, T + NY), slice(0, T), slice(T + NY, EY)
    for fields, base, middles, lows, highs in (
        (LOW, None, low, cll, clh),
        (HIGH, H + NX, high, chl, chh),
    ):
        at = 0
        for f, n in fields:
            for i in range(n):
                x = (H - n if base is None else base) + i
                place(e, f, x, middle, middles[at + i])
                place(e, f, x, below, lows[at + i])
                place(e, f, x, above, highs[at + i])
            at += n

    def body(group, _):
        at_low = at_high = 0
        for i in range(GROUP):
            x = H + group * GROUP + i
            for (f, n), (_, m) in zip(YLOW, YHIGH):
                place(e, f, x, below, shifted_tile(ylow, group, at_low + n - T))
                place(e, f, x, above, shifted_tile(yhigh, group, at_high))
                at_low += n
                at_high += m
        return _

    lax.fori_loop(0, NX // GROUP, body, 0)
    s_pass(e, y, masks)
    finish(edge, e, y, w, up, down, None, masks)


def combine(x0, x1, emit, tiles=range(TILES)):
    def body(n, _):
        for i in range(2):
            for t in tiles:
                emit(x0 + 2 * n + i, t)
        return _

    lax.fori_loop(0, (x1 - x0) // 2, body, 0)


def parts_pass(e, y_ref, w_ref, p1, p2, x0, x1, step, masks):
    zero = jnp.zeros((T, NZ), F32)
    tiles = range(TILES)

    def faces(both, d, x, i, t):
        y, w = both
        k, u = e[K + d, x + i, rows(t), :], e[U + d, x + i, rows(t), :]
        dy, dw = ((v.dx, v.dy, v.dz)[d](x, i, t) for v in both)
        ahead = 2.0 * jnp.maximum(u, 0.0)
        flux = k * dw
        up = (ahead * dy, ahead * dw + flux)
        if d == 2:
            k, u = e[K2B, x + i, rows(t), :], e[U2B, x + i, rows(t), :]
            dy, dw = y.dz_below(x, i, t), w.dz_below(x, i, t)
            flux = k * dw
        behind = 2.0 * jnp.minimum(u, 0.0)
        return up, (behind * dy, behind * dw - flux)

    first = (Tiles(y_ref, masks), Tiles(w_ref, masks))
    low_x = [faces(first, 0, x0 - 1, 0, t)[1] for t in tiles]

    def body(x, low_x):
        both = (Tiles(y_ref, masks), Tiles(w_ref, masks))
        for i in range(step):
            before = (zero, zero)
            next_low = []
            for t in tiles:
                (x_up, x_low), (y_up, y_low), (z_up, z_low) = (faces(both, d, x, i, t) for d in range(3))
                next_low.append(x_low)
                rolled = tuple(pltpu.roll(v, 1, 0) for v in y_low)
                y_below = [jnp.where(masks.top, old, new) for old, new in zip(before, rolled)]
                before = rolled
                totals = [
                    (x_up[j] + low_x[t][j]) + (y_up[j] + y_below[j]) + (z_up[j] + z_low[j]) for j in range(2)
                ]
                p1[x + i, rows(t), :] = totals[0] + (both[0].at(x, i, t) - both[1].at(x, i, t))
                p2[x + i, rows(t), :] = totals[1]
            low_x = next_low
        return low_x

    sweep(x0, x1, step, body, low_x)


def products_of_three(e, fields, images, masks):
    zero = jnp.zeros((T, NZ), F32)
    count = len(PAIRS)

    def body(x, accs):
        accs = list(accs)
        readers = [Tiles(ref, masks) for ref in images]
        for i in range(THREE_STEP):
            for t in INNER:
                q = [ref[x + i, rows(t), :] for ref in fields]
                m = [v.at(x, i, t) for v in readers]
                for n, (j, k) in enumerate(PAIRS):
                    accs[n] = accs[n] + q[j] * q[k]
                    accs[count + n] = accs[count + n] + q[j] * m[k]
                    accs[2 * count + n] = accs[2 * count + n] + m[j] * m[k]
                for d in range(3):
                    delta = [(v.dx, v.dy, v.dz)[d](x, i, t) for v in readers]
                    scaled = [e[K + d, x + i, rows(t), :] * v for v in delta]
                    for n, (j, k) in enumerate(PAIRS):
                        accs[3 * count + n] = accs[3 * count + n] + scaled[j] * delta[k]
        return tuple(accs)

    accs = sweep(H, H + NX, THREE_STEP, body, (zero,) * (4 * count))
    return accs[: 3 * count] + tuple(accs[3 * count + n] + accs[2 * count + n] for n in range(count))


def inner_kernel(edge, e, y, w, p1, p2, m1, m2):
    masks = Masks()
    parts_pass(e, y, w, p1, p2, H + 1, H + NX - 1, 10, masks)
    for p, m in ((p1, m1), (p2, m2)):
        outside_is_zero(edge, p)
        m_pass(e, p, m, masks, H + 2, H + NX - 2, 7)


def basis_kernel(
    edge, e, y_in, w_in, p1_in, p2_in, m1_in, m2_in, low, high, y4, w4, p1, p2, m1, m2, up, down, moments, q0, n0
):
    masks = Masks()
    y4[0:1], w4[0:2] = low[0:1], low[1:3]
    y4[EX - 1 :], w4[EX - 2 :] = high[0:1], high[1:3]
    for x0 in (1, H + NX - 1):
        parts_pass(e, y4, w4, p1, p2, x0, x0 + H, H, masks)
    for p, m in ((p1, m1), (p2, m2)):
        outside_is_zero(edge, p)
        m_pass(e, p, m, masks, H - 1, H + 2, 3)
        m_pass(e, p, m, masks, H + NX - 2, H + NX + 1, 3)
        outside_is_zero(edge, m)
    for n, (p, m) in enumerate(((p1, m1), (p2, m2))):
        up[n : n + 1], up[2 * n + 2 : 2 * n + 4] = p[NX : NX + 1], m[NX : NX + 2]
        down[n : n + 1], down[2 * n + 2 : 2 * n + 4] = p[H + 2 : H + 3], m[H + 1 : H + 3]

    def emit(x, t):
        at = (x, rows(t))
        q0[at] = y4[at] + A0 * p1[at] + B0 * p2[at]
        n0[at] = w4[at] + A0 * m1[at] + B0 * m2[at]

    combine(H, H + NX + 2, emit, range(1, TILES))
    write_sums(moments, products_of_three(e, (q0, p1, p2), (n0, m1, m2), masks))


def second_kernel(edge, e, y4, w4, p1, p2, m1, m2, low, high, sums, nu4, nu3, y, w, moments, adv, dif):
    masks = Masks()
    a4, b4, a3, b3 = two_sections(sums)

    def emit(x, t, parts):
        v, m = y4[x, rows(t), :], w4[x, rows(t), :]
        q1, q2, n1, n2 = parts
        c = 1.4 * e[C, x, rows(t), :]
        four = a4 * v + b4 * m
        three = a3 * (v + a4 * q1 + b4 * q2) + b3 * (m + a4 * n1 + b4 * n2)
        nu4[x, rows(t), :] = four
        nu3[x, rows(t), :] = three
        adv[x, rows(t), :] = c + 1.2 * four + 2.0 * three
        dif[x, rows(t), :] = c + 1.4 * four + three

    def read(ref, x, t):
        return ref[x, rows(t), :]

    combine(H - 1, H + NX + 1, lambda x, t: emit(x, t, [read(ref, x, t) for ref in (p1, p2, m1, m2)]))
    for x, strip, p_at, m_at in ((0, low, 0, 0), (1, low, None, 1), (EX - 2, high, None, 0), (EX - 1, high, 0, 1)):
        for t in range(TILES):
            ps = [read(ref, x, t) for ref in (p1, p2)] if p_at is None else [read(strip, n, t) for n in range(2)]
            emit(x, t, ps + [read(strip, 2 + 2 * n + m_at, t) for n in range(2)])

    def put(x, t, value):
        y[x, rows(t), :] = value

    fd_pass(e, adv, dif, put, 1, EX - 1, STEP, range(TILES), masks)
    finish(edge, e, y, w, None, None, moments, masks)


def last_kernel(e, nu4, nu3, y2, w2, sums, out, adv, dif, base):
    masks = Masks()
    a, b = full(*coefficients(*read_sums(sums, 4)))

    def emit(x, t):
        nu = a * y2[x, rows(t), :] + b * w2[x, rows(t), :]
        cot = e[C, x, rows(t), :]
        four, three = nu4[x, rows(t), :], nu3[x, rows(t), :]
        adv[x, rows(t), :] = 0.6 * cot + 0.8 * four + three + 2.0 * nu
        dif[x, rows(t), :] = 0.6 * (cot + four) + three + nu
        base[x, rows(t), :] = cot + four + three + nu

    combine(H - 1, H + NX + 1, emit)

    def put(x, t, value):
        out[x - H, rows(t - 1), :] = base[x, rows(t), :] + value

    fd_pass(e, adv, dif, put, H, H + NX, BLOCK_STEP, INNER, masks)


def shape(*dims):
    return jax.ShapeDtypeStruct(dims, F32)


FIELD = shape(EX, EY, NZ)
EXT = shape(9, EX, EY, NZ)
SCRATCH = [pltpu.VMEM((EX, EY, NZ), F32)]
STRIP = shape(3, EY, NZ)
STRIPS = shape(6, EY, NZ)
ROWS = shape(128, NZ)
VMEM = pl.BlockSpec(memory_space=pltpu.VMEM)
SMEM = pl.BlockSpec(memory_space=pltpu.SMEM)
HBM = pl.BlockSpec(memory_space=pltpu.HBM)
LIMIT = 8 * 1024 * 1024


def call(kernel, outs, ins, scratch=(), name=None, specs=None, sems=0, aliases=None):
    return pl.pallas_call(
        kernel,
        out_shape=outs,
        in_specs=specs or [SMEM] + [VMEM] * (len(ins) - 1),
        out_specs=jax.tree.map(lambda _: VMEM, outs),
        scratch_shapes=list(scratch) + ([pltpu.SemaphoreType.DMA((sems,))] if sems else []),
        input_output_aliases=aliases or {},
        compiler_params=pltpu.CompilerParams(vmem_limit_bytes=LIMIT),
        name=name,
    )(*ins)


def local(cotangent, speed, coeff, dirs):
    nx, ny = lax.axis_size("gx"), lax.axis_size("gy")
    ix, iy = lax.axis_index("gx"), lax.axis_index("gy")
    hbm = [pltpu.with_memory_space_constraint(v, pltpu.HBM) for v in (cotangent, speed, coeff, dirs)]
    edge = jnp.stack([(ix < nx - 1).astype(jnp.int32), (iy < ny - 1).astype(jnp.int32)])

    strips = call(
        pack_kernel,
        [shape(NLOW, NY, NZ), shape(NHIGH, NY, NZ), shape(NX // GROUP, YROWS_LOW, NZ), shape(NX // GROUP, YROWS_HIGH, NZ)]
        + [shape(NLOW, T, NZ)] * 2 + [shape(NHIGH, T, NZ)] * 2,
        [edge, *hbm],
        specs=[SMEM] + [HBM] * 4,
        scratch=[pltpu.VMEM((3, NX, NY), jnp.int32)] + [pltpu.VMEM((7, NX, T, NZ), F32)] * 2,
        sems=29,
        name="pack",
    )

    def shifted(value, dx, dy):
        perm = []
        for i in range(nx):
            for j in range(ny):
                if 0 <= i + dx < nx and 0 <= j + dy < ny:
                    perm.append((i * ny + j, (i + dx) * ny + j + dy))
        return lax.ppermute(value, ("gx", "gy"), perm)

    def along_x(up, down):
        return shifted(up, 1, 0), shifted(down, -1, 0)

    def reduced(moments):
        return lax.all_to_all(moments, ("gx", "gy"), 0, 0, tiled=True)

    moves = ((1, 0), (-1, 0), (0, 1), (0, -1), (1, 1), (1, -1), (-1, 1), (-1, -1))
    received = [shifted(s, dx, dy) for s, (dx, dy) in zip(strips, moves)]
    e = call(center_kernel, EXT, [*hbm[:3], dirs], specs=[HBM] * 3 + [VMEM], sems=7, name="center")
    e, y, w, up, down = call(
        first_kernel, [EXT, FIELD, FIELD, STRIP, STRIP], [edge, e, *received], aliases={1: 0}, name="first"
    )
    inner = call(inner_kernel, [FIELD] * 4, [edge, e, y, w], name="inner")
    *basis, up, down, moments = call(
        basis_kernel,
        [FIELD] * 6 + [STRIPS, STRIPS, ROWS],
        [edge, e, y, w, *inner, *along_x(up, down)],
        scratch=SCRATCH * 2,
        aliases={n + 2: n for n in range(6)},
        name="basis",
    )
    low, high = along_x(up, down)
    nu4, nu3, y2, w2, moments = call(
        second_kernel,
        [FIELD] * 4 + [ROWS],
        [edge, e, *basis, low, high, reduced(moments)],
        scratch=SCRATCH * 2,
        name="second",
    )
    return call(
        last_kernel, shape(NX, NY, NZ), [e, nu4, nu3, y2, w2, reduced(moments)], scratch=SCRATCH * 3, specs=[VMEM] * 6, name="last"
    )


def solution(mesh):
    placed = (P("gx", "gy", None), P(None, "gx", "gy", None), P(None, "gx", "gy", None), P(None, "gx", "gy"))
    return jax.shard_map(local, mesh=mesh, in_specs=placed, out_specs=P("gx", "gy", None), check_vma=False)
```

```python
import jax
import jax.numpy as jnp
from jax import lax
from jax.experimental import pallas as pl
from jax.experimental.pallas import tpu as pltpu
from jax.sharding import PartitionSpec as P


NX, NY, NZ = 32, 64, 128
H = 3
T = 8
EX, EY = NX + 2 * H, NY + 2 * T
TILES = EY // T
AX, AY = EX + 1, EY + T
INNER = range(1, TILES - 1)
F32 = jnp.float32

C, K, U, K2B, U2B = 0, 1, 4, 7, 8
LOW = ((0, 3), (1, 3), (4, 3), (2, 2), (3, 2), (5, 2), (6, 2))
HIGH = ((0, 3), (1, 2), (4, 2), (2, 2), (3, 2), (5, 2), (6, 2))
NLOW = sum(n for _, n in LOW)
NHIGH = sum(n for _, n in HIGH)
YLOW = ((0, 7), (1, 6), (4, 6), (2, 7), (3, 6), (5, 7), (6, 6))
YHIGH = ((0, 7), (1, 6), (4, 6), (2, 6), (3, 6), (5, 6), (6, 6))
GROUP = 8
YROWS_LOW = GROUP * sum(n for _, n in YLOW)
YROWS_HIGH = GROUP * sum(n for _, n in YHIGH)
STEP = 9
CENTER_STEP = 8
THREE_STEP = 4
A0, B0 = 0.6, -0.083
PAIRS = ((0, 0), (0, 1), (0, 2), (1, 1), (1, 2), (2, 2))
BLOCK_STEP = 8


def rows(t):
    return slice(t * T, (t + 1) * T)


class Masks:
    def __init__(self):
        lane = lax.broadcasted_iota(jnp.int32, (T, NZ), 1)
        row = lax.broadcasted_iota(jnp.int32, (T, NZ), 0)
        self.first, self.last, self.top = lane == 0, lane == NZ - 1, row == 0


def back(v):
    return pltpu.roll(v, 1, 1)


class Tiles:
    def __init__(self, ref, masks):
        self.ref, self.masks, self.seen = ref, masks, {}

    def at(self, x, i, t):
        key = (i, t)
        if key not in self.seen:
            self.seen[key] = self.ref[x + i, rows(t), :]
        return self.seen[key]

    def dx(self, x, i, t):
        return self.at(x, i + 1, t) - self.at(x, i, t)

    def dy(self, x, i, t):
        v = self.at(x, i, t)
        if t + 1 < TILES:
            return self.ref[x + i, t * T + 1 : (t + 1) * T + 1, :] - v
        return pltpu.roll(v, T - 1, 0) - v

    def dz(self, x, i, t):
        v = self.at(x, i, t)
        return jnp.where(self.masks.last, 0.0, pltpu.roll(v, NZ - 1, 1)) - v

    def dz_below(self, x, i, t):
        v = self.at(x, i, t)
        return v - back(v)


def sweep(x0, x1, step, body, carry):
    count = (x1 - x0) // step
    assert count * step == x1 - x0
    return lax.fori_loop(0, count, lambda n, c: body(x0 + n * step, c), carry)


def fluxes(x0, tiles, masks, parts, emit):
    def plane(x, low_x, i, fetch):
        new_low = []
        before = jnp.zeros((T, NZ), F32)
        if tiles[0] > 0:
            before = pltpu.roll(parts(fetch, 1, x, i, tiles[0] - 1)[1], 1, 0)
        for n, t in enumerate(tiles):
            up_x, down_x = parts(fetch, 0, x, i, t)
            up_y, down_y = parts(fetch, 1, x, i, t)
            up_z, down_z = parts(fetch, 2, x, i, t)
            rolled = pltpu.roll(down_y, 1, 0)
            down_y = jnp.where(masks.top, before, rolled)
            before = rolled
            total = (up_x - low_x[n]) + (up_y - down_y) + (up_z - down_z)
            new_low.append(down_x)
            emit(fetch, x, i, t, total)
        return new_low

    return plane


def run(x0, x1, step, tiles, masks, fetch_of, parts, emit):
    plane = fluxes(x0, tiles, masks, parts, emit)
    fetch = fetch_of()
    low = [parts(fetch, 0, x0 - 1, 0, t)[1] for t in tiles]

    def body(x, low):
        fetch = fetch_of()
        for i in range(step):
            low = plane(x, low, i, fetch)
        return low

    sweep(x0, x1, step, body, low)


def m_pass(e, v_ref, w_ref, masks, x0=1, x1=NX + 2 * H - 1, step=None):
    def parts(v, d, x, i, t):
        if d == 2:
            return e[K + 2, x + i, rows(t), :] * v.dz(x, i, t), e[K2B, x + i, rows(t), :] * v.dz_below(x, i, t)
        flux = e[K + d, x + i, rows(t), :] * (v.dx, v.dy)[d](x, i, t)
        return flux, flux

    def emit(v, x, i, t, total):
        w_ref[x + i, rows(t), :] = v.at(x, i, t) - total

    run(x0, x1, step or STEP, range(TILES), masks, lambda: Tiles(v_ref, masks), parts, emit)


def s_pass(e, y_ref, masks):
    cot = e.at[C]

    def parts(v, d, x, i, t):
        k, u = e[K + d, x + i, rows(t), :], e[U + d, x + i, rows(t), :]
        delta = (v.dx, v.dy, v.dz)[d](x, i, t)
        up = (k + jnp.maximum(u, 0.0)) * delta
        if d == 2:
            k, u = e[K2B, x + i, rows(t), :], e[U2B, x + i, rows(t), :]
            delta = v.dz_below(x, i, t)
        return up, (k - jnp.minimum(u, 0.0)) * delta

    def emit(v, x, i, t, total):
        y_ref[x + i, rows(t), :] = total

    run(1, EX - 1, STEP, range(TILES), masks, lambda: Tiles(cot, masks), parts, emit)


def fd_pass(e, a_ref, d_ref, put, x0, x1, step, tiles, masks):
    def parts(both, d, x, i, t):
        a, b = both
        k, u = e[K + d, x + i, rows(t), :], e[U + d, x + i, rows(t), :]
        da, db = ((v.dx, v.dy, v.dz)[d](x, i, t) for v in (a, b))
        flux = k * db
        up = flux + jnp.maximum(u, 0.0) * da
        if d == 2:
            u = e[U2B, x + i, rows(t), :]
            flux = e[K2B, x + i, rows(t), :] * b.dz_below(x, i, t)
            da = a.dz_below(x, i, t)
        return up, flux - jnp.minimum(u, 0.0) * da

    def emit(both, x, i, t, total):
        put(x + i, t, total)

    run(x0, x1, step, tiles, masks, lambda: (Tiles(a_ref, masks), Tiles(d_ref, masks)), parts, emit)


def products(e, y_ref, w_ref, masks):
    zero = jnp.zeros((T, NZ), F32)

    def body(x, accs):
        yy, yw, ww, *energy = accs
        w = Tiles(w_ref, masks)
        for i in range(BLOCK_STEP):
            for t in INNER:
                v, y = w.at(x, i, t), y_ref[x + i, rows(t), :]
                yy, yw, ww = yy + y * y, yw + y * v, ww + v * v
                for d, delta in enumerate((w.dx, w.dy, w.dz)):
                    difference = delta(x, i, t)
                    energy[d] = energy[d] + e[K + d, x + i, rows(t), :] * (difference * difference)
        return yy, yw, ww, *energy

    yy, yw, ww, *energy = sweep(H, H + NX, BLOCK_STEP, body, (zero,) * 6)
    return yy, yw, ww, ww + (energy[0] + energy[1] + energy[2])


def outside_is_zero(edge, ref):
    @pl.when(edge[0] == 0)
    def _():
        ref[H + NX : EX - 1, :EY] = jnp.zeros((H - 1, EY, NZ), F32)

    @pl.when(edge[1] == 0)
    def _():
        ref[:, EY - T : EY, :] = jnp.zeros((EX, T, NZ), F32)


def finish(edge, e, y, w, up, down, moments, masks):
    outside_is_zero(edge, y)
    m_pass(e, y, w, masks)
    outside_is_zero(edge, w)
    if up is not None:
        up[0:1], up[1:3] = y[NX : NX + 1, :EY], w[NX : NX + 2, :EY]
        down[0:1], down[1:3] = y[H + 2 : H + 3, :EY], w[H + 1 : H + 3, :EY]
    if moments is None:
        return
    write_sums(moments, products(e, y, w, masks))


def write_sums(moments, sums):
    lane = lax.broadcasted_iota(jnp.int32, (1, NZ), 1)
    row = jnp.zeros((1, NZ), F32)
    for i, acc in enumerate(sums):
        total = jnp.sum(jnp.sum(acc, axis=0, keepdims=True), axis=1, keepdims=True)
        row = jnp.where(lane // 4 == i, total, row)
    moments[...] = jnp.broadcast_to(row, moments.shape)


def read_sums(moments_ref, count):
    sums = jnp.sum(moments_ref[...], axis=0, keepdims=True)
    lane = lax.broadcasted_iota(jnp.int32, (1, NZ), 1)
    return [jnp.sum(jnp.where(lane == 4 * i, sums, 0.0), axis=1, keepdims=True) for i in range(count)]


def coefficients(m0, m1, m2, m3):
    alpha0 = m0 / m1
    rr = alpha0 * alpha0 * m2 - m0
    product = m1 - 2.0 * alpha0 * m2 + alpha0 * alpha0 * m3
    ratio = rr / m0
    alpha1 = rr / (product - ratio * rr / alpha0)
    a = alpha0 + alpha1 * (1.0 + ratio)
    b = -(alpha1 * alpha0)
    return a, b


def full(*scalars):
    return tuple(jnp.broadcast_to(v, (T, NZ)) for v in scalars)


def two_sections(moments_ref):
    sums = read_sums(moments_ref, 4 * len(PAIRS))
    grams = [dict(zip(PAIRS, sums[len(PAIRS) * k : len(PAIRS) * (k + 1)])) for k in range(4)]

    def moments(a, b):
        return [
            g[0, 0]
            + 2.0 * (a * g[0, 1] + b * g[0, 2])
            + (a * a * g[1, 1] + 2.0 * a * b * g[1, 2] + b * b * g[2, 2])
            for g in grams
        ]

    a, b = coefficients(*moments(-A0, -B0))
    return full(a, b, *coefficients(*moments(a - A0, b - B0)))


def signs(dirs, d, x, first_rows):
    sign = (1 - 2 * dirs[d, pl.ds(x, 1), :]).astype(F32)
    count = T * len(first_rows)
    row = lax.broadcasted_iota(jnp.int32, (count, NY), 0)
    column = lax.broadcasted_iota(jnp.int32, (count, NY), 1)
    at = row
    for n, first in enumerate(first_rows):
        at = jnp.where(row // T == n, row - n * T + first, at)
    picked = jnp.where(at == column, jnp.broadcast_to(sign, (count, NY)), 0.0)
    ones = jnp.ones((NY, NZ), jnp.bfloat16)
    return jnp.dot(picked.astype(jnp.bfloat16), ones, preferred_element_type=F32)


def pack_kernel(edge, cot, speed, coeff, all_dirs, low, high, ylow, yhigh, cll, clh, chl, chh, dirs, tops, bottoms, sems):
    bottom, top, full = slice(0, T), slice(NY - T, NY), slice(0, NY)
    copies = [pltpu.make_async_copy(all_dirs, dirs, sems.at[0])]
    copies[0].start()

    def fetch(f, planes, rows, target):
        source = cot.at[planes, rows] if f == 0 else (coeff if f < 4 else speed).at[(f - 1) % 3, planes, rows]
        copy = pltpu.make_async_copy(source, target, sems.at[len(copies)])
        copy.start()
        copies.append(copy)

    for f in range(7):
        fetch(f, slice(0, NX), top, tops.at[f])
        fetch(f, slice(0, NX), bottom, bottoms.at[f])
    signed = []
    for fields, strip in ((LOW, low), (HIGH, high)):
        at = 0
        for f, n in fields:
            start = NX - n if fields is LOW else 0
            fetch(f, slice(start, start + n), full, strip.at[at : at + n])
            if f >= 4:
                signed += [(strip, at + i, f - 4, start + i) for i in range(n)]
            at += n
    for copy in copies:
        copy.wait()
    for group in range(NX // GROUP):
        at_low = at_high = 0
        for x in range(group * GROUP, (group + 1) * GROUP):
            sign = [signs(dirs, d, x, (NY - T, 0)) for d in range(3)]
            for (f, n), (_, m) in zip(YLOW, YHIGH):
                upper, lower = tops[f, x], bottoms[f, x]
                if f >= 4:
                    upper, lower = upper * sign[f - 4][:T], lower * sign[f - 4][T:]
                ylow[group, at_low : at_low + n, :] = upper[T - n :]
                yhigh[group, at_high : at_high + m, :] = lower[:m]
                at_low += n
                at_high += m
    for strip, at, d, x in signed:
        strip[at] = strip[at] * signs(dirs, d, x, tuple(range(0, NY, T)))
    cll[...] = low[:, top, :]
    clh[...] = low[:, bottom, :]
    chl[...] = high[:, top, :]
    chh[...] = high[:, bottom, :]


def place(e, f, x, rows, value):
    if f > 0:
        value = 0.25 * value
    e[f, x, rows, :] = value
    if f in (K + 2, U + 2):
        first = lax.broadcasted_iota(jnp.int32, value.shape, 1) == 0
        e[K2B if f == K + 2 else U2B, x, rows, :] = jnp.where(first, 0.0, back(value))


def shifted_tile(ref, group, start):
    inside = min(max(start, 0), ref.shape[1] - T)
    value = ref[group, inside : inside + T, :]
    return value if inside == start else pltpu.roll(value, (inside - start) % T, 0)


def center_kernel(cot, speed, coeff, dirs, e, sems):
    every = tuple(range(0, NY, T))
    middle = slice(T, T + NY)
    copies = []
    for f in range(7):
        source = cot if f == 0 else (coeff if f < 4 else speed).at[(f - 1) % 3]
        copies.append(pltpu.make_async_copy(source, e.at[f, H : H + NX, middle], sems.at[f]))
    for copy in copies:
        copy.start()
    for copy in copies:
        copy.wait()

    def body(n, _):
        for i in range(CENTER_STEP):
            x = CENTER_STEP * n + i
            for f in range(1, 7):
                value = e[f, H + x, middle, :]
                if f >= 4:
                    value = value * signs(dirs, f - 4, x, every)
                place(e, f, H + x, middle, value)
        return _

    lax.fori_loop(0, NX // CENTER_STEP, body, 0)


def first_kernel(edge, e_in, low, high, ylow, yhigh, cll, clh, chl, chh, e, y, w, up, down):
    masks = Masks()
    middle, below, above = slice(T, T + NY), slice(0, T), slice(T + NY, EY)
    for fields, base, middles, lows, highs in (
        (LOW, None, low, cll, clh),
        (HIGH, H + NX, high, chl, chh),
    ):
        at = 0
        for f, n in fields:
            for i in range(n):
                x = (H - n if base is None else base) + i
                place(e, f, x, middle, middles[at + i])
                place(e, f, x, below, lows[at + i])
                place(e, f, x, above, highs[at + i])
            at += n

    def body(group, _):
        at_low = at_high = 0
        for i in range(GROUP):
            x = H + group * GROUP + i
            for (f, n), (_, m) in zip(YLOW, YHIGH):
                place(e, f, x, below, shifted_tile(ylow, group, at_low + n - T))
                place(e, f, x, above, shifted_tile(yhigh, group, at_high))
                at_low += n
                at_high += m
        return _

    lax.fori_loop(0, NX // GROUP, body, 0)
    s_pass(e, y, masks)
    finish(edge, e, y, w, up, down, None, masks)


def combine(x0, x1, emit, tiles=range(TILES)):
    def body(n, _):
        for i in range(2):
            for t in tiles:
                emit(x0 + 2 * n + i, t)
        return _

    lax.fori_loop(0, (x1 - x0) // 2, body, 0)


def parts_pass(e, y_ref, w_ref, p1, p2, x0, x1, step, masks):
    zero = jnp.zeros((T, NZ), F32)
    tiles = range(TILES)

    def faces(both, d, x, i, t):
        y, w = both
        k, u = e[K + d, x + i, rows(t), :], e[U + d, x + i, rows(t), :]
        dy, dw = ((v.dx, v.dy, v.dz)[d](x, i, t) for v in both)
        ahead = 2.0 * jnp.maximum(u, 0.0)
        flux = k * dw
        up = (ahead * dy, ahead * dw + flux)
        if d == 2:
            k, u = e[K2B, x + i, rows(t), :], e[U2B, x + i, rows(t), :]
            dy, dw = y.dz_below(x, i, t), w.dz_below(x, i, t)
            flux = k * dw
        behind = 2.0 * jnp.minimum(u, 0.0)
        return up, (behind * dy, behind * dw - flux)

    first = (Tiles(y_ref, masks), Tiles(w_ref, masks))
    low_x = [faces(first, 0, x0 - 1, 0, t)[1] for t in tiles]

    def body(x, low_x):
        both = (Tiles(y_ref, masks), Tiles(w_ref, masks))
        for i in range(step):
            before = (zero, zero)
            next_low = []
            for t in tiles:
                (x_up, x_low), (y_up, y_low), (z_up, z_low) = (faces(both, d, x, i, t) for d in range(3))
                next_low.append(x_low)
                rolled = tuple(pltpu.roll(v, 1, 0) for v in y_low)
                y_below = [jnp.where(masks.top, old, new) for old, new in zip(before, rolled)]
                before = rolled
                totals = [
                    (x_up[j] + low_x[t][j]) + (y_up[j] + y_below[j]) + (z_up[j] + z_low[j]) for j in range(2)
                ]
                p1[x + i, rows(t), :] = totals[0] + (both[0].at(x, i, t) - both[1].at(x, i, t))
                p2[x + i, rows(t), :] = totals[1]
            low_x = next_low
        return low_x

    sweep(x0, x1, step, body, low_x)


def products_of_three(e, fields, images, masks):
    zero = jnp.zeros((T, NZ), F32)
    count = len(PAIRS)

    def body(x, accs):
        accs = list(accs)
        readers = [Tiles(ref, masks) for ref in images]
        for i in range(THREE_STEP):
            for t in INNER:
                q = [ref[x + i, rows(t), :] for ref in fields]
                m = [v.at(x, i, t) for v in readers]
                for n, (j, k) in enumerate(PAIRS):
                    accs[n] = accs[n] + q[j] * q[k]
                    accs[count + n] = accs[count + n] + q[j] * m[k]
                    accs[2 * count + n] = accs[2 * count + n] + m[j] * m[k]
                for d in range(3):
                    delta = [(v.dx, v.dy, v.dz)[d](x, i, t) for v in readers]
                    scaled = [e[K + d, x + i, rows(t), :] * v for v in delta]
                    for n, (j, k) in enumerate(PAIRS):
                        accs[3 * count + n] = accs[3 * count + n] + scaled[j] * delta[k]
        return tuple(accs)

    accs = sweep(H, H + NX, THREE_STEP, body, (zero,) * (4 * count))
    return accs[: 3 * count] + tuple(accs[3 * count + n] + accs[2 * count + n] for n in range(count))


def inner_kernel(edge, e, y, w, p1, p2, m1, m2):
    masks = Masks()
    parts_pass(e, y, w, p1, p2, H + 1, H + NX - 1, 10, masks)
    for p, m in ((p1, m1), (p2, m2)):
        outside_is_zero(edge, p)
        m_pass(e, p, m, masks, H + 2, H + NX - 2, 7)


def basis_kernel(
    edge, e, y_in, w_in, p1_in, p2_in, m1_in, m2_in, low, high, y4, w4, p1, p2, m1, m2, up, down, moments, q0, n0
):
    masks = Masks()
    y4[0:1, :EY], w4[0:2, :EY] = low[0:1], low[1:3]
    y4[EX - 1 :, :EY], w4[EX - 2 :, :EY] = high[0:1], high[1:3]
    for x0 in (1, H + NX - 1):
        parts_pass(e, y4, w4, p1, p2, x0, x0 + H, H, masks)
    for p, m in ((p1, m1), (p2, m2)):
        outside_is_zero(edge, p)
        m_pass(e, p, m, masks, H - 1, H + 2, 3)
        m_pass(e, p, m, masks, H + NX - 2, H + NX + 1, 3)
        outside_is_zero(edge, m)
    for n, (p, m) in enumerate(((p1, m1), (p2, m2))):
        up[n : n + 1], up[2 * n + 2 : 2 * n + 4] = p[NX : NX + 1, :EY], m[NX : NX + 2, :EY]
        down[n : n + 1], down[2 * n + 2 : 2 * n + 4] = p[H + 2 : H + 3, :EY], m[H + 1 : H + 3, :EY]

    def emit(x, t):
        at = (x, rows(t))
        q0[at] = y4[at] + A0 * p1[at] + B0 * p2[at]
        n0[at] = w4[at] + A0 * m1[at] + B0 * m2[at]

    combine(H, H + NX + 2, emit, range(1, TILES))
    write_sums(moments, products_of_three(e, (q0, p1, p2), (n0, m1, m2), masks))


def second_kernel(edge, e, y4, w4, p1, p2, m1, m2, low, high, sums, nu4, nu3, y, w, moments, adv, dif):
    masks = Masks()
    a4, b4, a3, b3 = two_sections(sums)

    def emit(x, t, parts):
        v, m = y4[x, rows(t), :], w4[x, rows(t), :]
        q1, q2, n1, n2 = parts
        c = 1.4 * e[C, x, rows(t), :]
        four = a4 * v + b4 * m
        three = a3 * (v + a4 * q1 + b4 * q2) + b3 * (m + a4 * n1 + b4 * n2)
        nu4[x, rows(t), :] = four
        nu3[x, rows(t), :] = three
        adv[x, rows(t), :] = c + 1.2 * four + 2.0 * three
        dif[x, rows(t), :] = c + 1.4 * four + three

    def read(ref, x, t):
        return ref[x, rows(t), :]

    combine(H - 1, H + NX + 1, lambda x, t: emit(x, t, [read(ref, x, t) for ref in (p1, p2, m1, m2)]))
    for x, strip, p_at, m_at in ((0, low, 0, 0), (1, low, None, 1), (EX - 2, high, None, 0), (EX - 1, high, 0, 1)):
        for t in range(TILES):
            ps = [read(ref, x, t) for ref in (p1, p2)] if p_at is None else [read(strip, n, t) for n in range(2)]
            emit(x, t, ps + [read(strip, 2 + 2 * n + m_at, t) for n in range(2)])

    def put(x, t, value):
        y[x, rows(t), :] = value

    fd_pass(e, adv, dif, put, 1, EX - 1, STEP, range(TILES), masks)
    finish(edge, e, y, w, None, None, moments, masks)


def last_kernel(e, nu4, nu3, y2, w2, sums, out, adv, dif, base):
    masks = Masks()
    a, b = full(*coefficients(*read_sums(sums, 4)))

    def emit(x, t):
        nu = a * y2[x, rows(t), :] + b * w2[x, rows(t), :]
        cot = e[C, x, rows(t), :]
        four, three = nu4[x, rows(t), :], nu3[x, rows(t), :]
        adv[x, rows(t), :] = 0.6 * cot + 0.8 * four + three + 2.0 * nu
        dif[x, rows(t), :] = 0.6 * (cot + four) + three + nu
        base[x, rows(t), :] = cot + four + three + nu

    combine(H - 1, H + NX + 1, emit)

    def put(x, t, value):
        out[x - H, rows(t - 1), :] = base[x, rows(t), :] + value

    fd_pass(e, adv, dif, put, H, H + NX, BLOCK_STEP, INNER, masks)


def shape(*dims):
    return jax.ShapeDtypeStruct(dims, F32)


FIELD = shape(EX, AY, NZ)
EXT = shape(9, AX, AY, NZ)
SCRATCH = [pltpu.VMEM((EX, AY, NZ), F32)]
STRIP = shape(3, EY, NZ)
STRIPS = shape(6, EY, NZ)
ROWS = shape(128, NZ)
VMEM = pl.BlockSpec(memory_space=pltpu.VMEM)
SMEM = pl.BlockSpec(memory_space=pltpu.SMEM)
HBM = pl.BlockSpec(memory_space=pltpu.HBM)
LIMIT = 8 * 1024 * 1024


def call(kernel, outs, ins, scratch=(), name=None, specs=None, sems=0, aliases=None):
    return pl.pallas_call(
        kernel,
        out_shape=outs,
        in_specs=specs or [SMEM] + [VMEM] * (len(ins) - 1),
        out_specs=jax.tree.map(lambda _: VMEM, outs),
        scratch_shapes=list(scratch) + ([pltpu.SemaphoreType.DMA((sems,))] if sems else []),
        input_output_aliases=aliases or {},
        compiler_params=pltpu.CompilerParams(vmem_limit_bytes=LIMIT),
        name=name,
    )(*ins)


def local(cotangent, speed, coeff, dirs):
    nx, ny = lax.axis_size("gx"), lax.axis_size("gy")
    ix, iy = lax.axis_index("gx"), lax.axis_index("gy")
    hbm = [pltpu.with_memory_space_constraint(v, pltpu.HBM) for v in (cotangent, speed, coeff, dirs)]
    edge = jnp.stack([(ix < nx - 1).astype(jnp.int32), (iy < ny - 1).astype(jnp.int32)])

    strips = call(
        pack_kernel,
        [shape(NLOW, NY, NZ), shape(NHIGH, NY, NZ), shape(NX // GROUP, YROWS_LOW, NZ), shape(NX // GROUP, YROWS_HIGH, NZ)]
        + [shape(NLOW, T, NZ)] * 2 + [shape(NHIGH, T, NZ)] * 2,
        [edge, *hbm],
        specs=[SMEM] + [HBM] * 4,
        scratch=[pltpu.VMEM((3, NX, NY), jnp.int32)] + [pltpu.VMEM((7, NX, T, NZ), F32)] * 2,
        sems=29,
        name="pack",
    )

    def shifted(value, dx, dy):
        perm = []
        for i in range(nx):
            for j in range(ny):
                if 0 <= i + dx < nx and 0 <= j + dy < ny:
                    perm.append((i * ny + j, (i + dx) * ny + j + dy))
        return lax.ppermute(value, ("gx", "gy"), perm)

    def along_x(up, down):
        return shifted(up, 1, 0), shifted(down, -1, 0)

    def reduced(moments):
        return lax.all_to_all(moments, ("gx", "gy"), 0, 0, tiled=True)

    moves = ((1, 0), (-1, 0), (0, 1), (0, -1), (1, 1), (1, -1), (-1, 1), (-1, -1))
    received = [shifted(s, dx, dy) for s, (dx, dy) in zip(strips, moves)]
    e = call(center_kernel, EXT, [*hbm[:3], dirs], specs=[HBM] * 3 + [VMEM], sems=7, name="center")
    e, y, w, up, down = call(
        first_kernel, [EXT, FIELD, FIELD, STRIP, STRIP], [edge, e, *received], aliases={1: 0}, name="first"
    )
    inner = call(inner_kernel, [FIELD] * 4, [edge, e, y, w], name="inner")
    *basis, up, down, moments = call(
        basis_kernel,
        [FIELD] * 6 + [STRIPS, STRIPS, ROWS],
        [edge, e, y, w, *inner, *along_x(up, down)],
        scratch=SCRATCH * 2,
        aliases={n + 2: n for n in range(6)},
        name="basis",
    )
    low, high = along_x(up, down)
    nu4, nu3, y2, w2, moments = call(
        second_kernel,
        [FIELD] * 4 + [ROWS],
        [edge, e, *basis, low, high, reduced(moments)],
        scratch=SCRATCH * 2,
        name="second",
    )
    return call(
        last_kernel, shape(NX, NY, NZ), [e, nu4, nu3, y2, w2, reduced(moments)], scratch=SCRATCH * 3, specs=[VMEM] * 6, name="last"
    )


def solution(mesh):
    placed = (P("gx", "gy", None), P(None, "gx", "gy", None), P(None, "gx", "gy", None), P(None, "gx", "gy"))
    return jax.shard_map(local, mesh=mesh, in_specs=placed, out_specs=P("gx", "gy", None), check_vma=False)
```
